256 devices in a mesh: lat: 64 (over z, x, core), depth: 4 (over y).
Axes of the slice: x: 4, y: 4, z: 8, core: 2. Of those that a mesh axis runs over, the one named last changes fastest.
Arguments:
- surface: float32 [1024, 4096], P('lat'), may hold values from -6 to 6
- velocity: float32 [2, 1024, 4096], P(None, 'lat'), may hold values from -6 to 6
- block_map: int32 [1024, 4096], P('lat'), may hold values from 0 to 15
- free_flags: int32 [1024, 4096], P('lat'), may hold values 0 or 1
- block_rates: float32 [16], replicated, may hold values from 0.2 to 2
- previous_mesh: float32 [1024, 64, 4096], P('lat', 'depth'), may hold values from -6 to 6
Outputs:
- new_surface: float32 [1024, 4096], P('lat')
- mesh_field: float32 [1024, 64, 4096], P('lat', 'depth')
- column_norm: float32 [1024], P('lat')
The draws below stay inside these ranges and needn't reach their ends.
All inputs are finite; a program needn't handle non-finite values. No bound on the sum of `free_flags` on one device may be relied on, other than what follows from the above.
Results may differ from the reference program's by a relative error of at most 0.00002.
Values sent between devices are 32-bit elements; how exact they have to be, the bound alone decides.
A program may use at most 64 MiB of HBM per device.

```python
import math
import jax
import jax.numpy as jnp
from jax import lax

NY = 4096
NB = 16
ITERS = 2
NX = 1024
NZ = 64


def touch_ends(result, key, least, top_value):
    place = [jax.random.randint(jax.random.fold_in(key, axis), (), 0, length) for axis, length in enumerate(result.shape)]
    main_axis = result.shape.index(max(result.shape))
    next_to = place[:main_axis] + [(place[main_axis] + 1) % result.shape[main_axis]] + place[main_axis + 1:]
    return result.at[tuple(place)].set(least).at[tuple(next_to)].set(top_value)


def shard_levels(stream_key, extent, cuts, low, largest):
    loudness = 1.0
    for position, parts in cuts:
        heights = jax.random.uniform(jax.random.fold_in(jax.random.fold_in(stream_key, 6), position), (parts,), jnp.float32, low / len(cuts), largest / len(cuts))
        loudness = loudness * jnp.repeat(jnp.exp(heights), extent[position] // parts).reshape((-1,) + (1,) * (len(extent) - 1 - position))
    return loudness


def bell_draw(key, extent, width, most, split=(), held_as=jnp.bfloat16):
    level = shard_levels(key, extent, split, -0.22, 0.18) if split else 1.0
    result = jax.random.normal(key, extent, jnp.float32) * width * level
    return jnp.minimum(jnp.maximum(result, -most), most).astype(held_as)


def setup_inputs(seed: int = 0) -> dict:
    keys = jax.random.split(jax.random.key(seed), 7)
    return {
        "surface": bell_draw(keys[0], (NX, NY), 1.0, 6.0, ((0, 64),), jnp.float32),
        "velocity": bell_draw(keys[1], (2, NX, NY), 1.0, 6.0, ((1, 64),), jnp.float32),
        "block_map": touch_ends(jax.random.randint(keys[2], (NX, NY), 0, NB), jax.random.fold_in(keys[2], 1), 0, NB - 1).astype(jnp.int32),
        "free_flags": touch_ends((jax.random.randint(keys[3], (NX, NY), 0, 4) < 3).astype(jnp.int32), jax.random.fold_in(keys[3], 1), 0, 1),
        "block_rates": jnp.clip(jnp.exp(jax.random.uniform(keys[4], (NB,), jnp.float32, math.log(0.2), math.log(2.0))), 0.2, 2.0),
        "previous_mesh": bell_draw(keys[5], (NX, NZ, NY), 1.0, 6.0, ((0, 64), (1, 4)), jnp.float32),
    }


TIME_STEP = 0.5
RELAX_WEIGHT = 0.8

def relax_once(field, surface_shift):
    padded_rows = jnp.pad(field, ((1, 1), (0, 0), (0, 0)))
    across_rows = padded_rows[2:] + padded_rows[:-2]
    padded_cols = jnp.pad(field, ((0, 0), (0, 0), (1, 1)))
    across_cols = padded_cols[:, :, 2:] + padded_cols[:, :, :-2]
    upper = jnp.concatenate([surface_shift[:, None, :], field[:, :-1, :]], axis=1)
    lower = jnp.concatenate([field[:, 1:, :], jnp.zeros_like(field[:, :1, :])], axis=1)
    neighbours = across_rows + across_cols + upper + lower
    return (1.0 - RELAX_WEIGHT) * field + RELAX_WEIGHT * neighbours / 6.0

def reference(surface, velocity, block_map, free_flags, block_rates, previous_mesh):
    padded = jnp.pad(surface, 1)
    grad_rows = (padded[2:, 1:-1] - padded[:-2, 1:-1]) * 0.5
    grad_cols = (padded[1:-1, 2:] - padded[1:-1, :-2]) * 0.5
    laplace = padded[2:, 1:-1] + padded[:-2, 1:-1] + padded[1:-1, 2:] + padded[1:-1, :-2] - 4.0 * surface
    diffusivity = block_rates[block_map]
    tendency = -velocity[0] * grad_rows - velocity[1] * grad_cols + diffusivity * laplace
    new_surface = surface + TIME_STEP * free_flags.astype(jnp.float32) * tendency
    surface_shift = new_surface - surface
    layers = jnp.arange(NZ, dtype=jnp.int32)
    profile = (NZ - layers).astype(jnp.float32) / NZ
    field = previous_mesh + surface_shift[:, None, :] * profile[None, :, None]
    for sweep_index in range(ITERS):
        field = relax_once(field, surface_shift)
    column_norm = jnp.sqrt(lax.optimization_barrier(jnp.sum(field * field, axis=(1, 2))) / (NZ * NY))
    return (new_surface, field, column_norm)
```

```python
import jax
import jax.numpy as jnp
from jax import lax
from jax.experimental import pallas as pl
from jax.experimental.pallas import tpu as pltpu
from jax.sharding import PartitionSpec as P

MESH = pl.DeviceIdType.MESH
TIME_STEP = 0.5
RELAX_WEIGHT = 0.8
KEEP = 1.0 - RELAX_WEIGHT
SHARE = RELAX_WEIGHT / 6.0
CENTRE = KEEP / SHARE
SCALE = SHARE * SHARE
SUB = 8
CHUNKS = 8


def iotas(width):
    lane = lax.broadcasted_iota(jnp.int32, (SUB, 128), 1)
    sub = lax.broadcasted_iota(jnp.int32, (SUB, 128), 0)
    return lane, sub


def before(v, masks):
    width = v.shape[-1]
    rolled = pltpu.roll(v, 1, 1)
    first = rolled[:, :128]
    carried = pltpu.roll(first, 1, 0)
    first = jnp.where(masks[0], jnp.where(masks[1], 0.0, carried), first)
    return jnp.concatenate([first, rolled[:, 128:]], axis=1)


def after(v, masks):
    width = v.shape[-1]
    rolled = pltpu.roll(v, width - 1, 1)
    last = rolled[:, width - 128:]
    carried = pltpu.roll(last, SUB - 1, 0)
    last = jnp.where(masks[2], jnp.where(masks[3], 0.0, carried), last)
    return jnp.concatenate([rolled[:, : width - 128], last], axis=1)


def relax_kernel(
    rows, layers, width, n_lat, n_depth,
    surface, velocity, block_map, free_flags, block_rates, previous,
    new_surface, mesh_out, norm_out,
    prev, once, above, below, surf, vel, bmap, flags, rates,
    shift, wide, widest, squares, totals,
    load_sem, up_send, up_recv, down_send, down_recv, side_send, side_recv,
    corner_send, corner_recv, sum_send, sum_recv,
):
    lat = lax.axis_index("lat")
    depth = lax.axis_index("depth")
    has_left, has_right = lat > 0, lat < n_lat - 1
    has_up, has_down = depth > 0, depth < n_depth - 1
    left, right = {"lat": lat - 1}, {"lat": lat + 1}
    up, down = {"depth": depth - 1}, {"depth": depth + 1}

    barrier = pltpu.get_barrier_semaphore()
    for k in (1, n_depth - 1):
        pl.semaphore_signal(
            barrier, inc=1, device_id={"depth": lax.rem(depth + k, n_depth)}, device_id_type=MESH)
    for have, target in ((has_left, left), (has_right, right)):
        @pl.when(have)
        def _():
            pl.semaphore_signal(barrier, inc=1, device_id=target, device_id_type=MESH)

    count = 0
    groups = {}

    def load(name, pairs):
        nonlocal count
        copies = []
        for src, dst in pairs:
            copy = pltpu.make_async_copy(src, dst, load_sem.at[count])
            copy.start()
            copies.append(copy)
            count += 1
        groups[name] = copies

    def loaded(name):
        for copy in groups[name]:
            copy.wait()

    cols = [slice(s * width, (s + 1) * width) for s in range(SUB)]
    own = slice(2, 2 + rows)
    load("outer", [
        (previous.at[:, part, cols[s]], prev.at[own, part, s, :])
        for part in (slice(layers - 2, layers), slice(0, 2)) for s in range(SUB)
    ])
    load("surface",
         [(surface.at[:, cols[s]], surf.at[slice(3, 3 + rows), s, :]) for s in range(SUB)]
         + [(velocity.at[:, :, cols[s]], vel.at[:, own, s, :]) for s in range(SUB)]
         + [(block_map.at[:, cols[s]], bmap.at[own, s, :]) for s in range(SUB)]
         + [(free_flags.at[:, cols[s]], flags.at[own, s, :]) for s in range(SUB)]
         + [(block_rates, rates)])
    load("inner", [
        (previous.at[:, part, cols[s]], prev.at[own, part, s, :])
        for part in (slice(2, SUB), slice(layers - SUB, layers - 2)) for s in range(SUB)
    ])

    def clear(ref):
        ref[...] = jnp.zeros(ref.shape, ref.dtype)

    @pl.when(jnp.logical_not(has_up))
    def _():
        clear(above)

    @pl.when(jnp.logical_not(has_down))
    def _():
        clear(below)

    for have, near, far, at in (
        (has_left, slice(0, 2), slice(0, 3), 0),
        (has_right, slice(rows + 2, rows + 4), slice(rows + 3, rows + 6), rows + 1),
    ):
        @pl.when(jnp.logical_not(have))
        def _():
            clear(prev.at[near])
            clear(surf.at[far])
            clear(vel.at[:, near])
            clear(bmap.at[near])
            clear(flags.at[near])
            clear(above.at[at])
            clear(below.at[at])
            clear(once.at[at])

    pl.semaphore_wait(barrier, 2 + has_left.astype(jnp.int32) + has_right.astype(jnp.int32))

    def remote(src, dst, send, recv, target):
        return pltpu.make_async_remote_copy(
            src_ref=src, dst_ref=dst, send_sem=send, recv_sem=recv,
            device_id=target, device_id_type=MESH,
        )

    step = rows // CHUNKS
    last_two, first_two = slice(layers - 2, layers), slice(0, 2)
    to_down, to_up = [], []
    for c in range(CHUNKS):
        mine = slice(2 + c * step, 2 + (c + 1) * step)
        theirs = slice(1 + c * step, 1 + (c + 1) * step)
        to_down.append(remote(prev.at[mine, last_two], above.at[theirs], down_send.at[c], down_recv.at[c], down))
        to_up.append(remote(prev.at[mine, first_two], below.at[theirs], up_send.at[c], up_recv.at[c], up))

    loaded("outer")

    @pl.when(has_down)
    def _():
        for copy in to_down:
            copy.start()

    @pl.when(has_up)
    def _():
        for copy in to_up:
            copy.start()

    def sides(mine3, theirs3, mine2, theirs2, row, target):
        return [
            remote(surf.at[mine3], surf.at[theirs3], side_send.at[row, 0], side_recv.at[row, 0], target),
            remote(vel.at[:, mine2], vel.at[:, theirs2], side_send.at[row, 1], side_recv.at[row, 1], target),
            remote(bmap.at[mine2], bmap.at[theirs2], side_send.at[row, 2], side_recv.at[row, 2], target),
            remote(flags.at[mine2], flags.at[theirs2], side_send.at[row, 3], side_recv.at[row, 3], target),
            remote(prev.at[mine2], prev.at[theirs2], side_send.at[row, 4], side_recv.at[row, 4], target),
        ]

    to_right = sides(slice(rows, rows + 3), slice(0, 3), slice(rows, rows + 2), slice(0, 2), 0, right)
    to_left = sides(slice(3, 6), slice(rows + 3, rows + 6), slice(2, 4), slice(rows + 2, rows + 4), 1, left)

    loaded("surface")

    @pl.when(has_right)
    def _():
        for copy in to_right[:4]:
            copy.start()

    @pl.when(has_left)
    def _():
        for copy in to_left[:4]:
            copy.start()

    loaded("inner")

    @pl.when(has_right)
    def _():
        to_right[4].start()

    @pl.when(has_left)
    def _():
        to_left[4].start()

    lane, sub = iotas(width)
    masks = (lane == 0, sub == 0, lane == 127, sub == SUB - 1)

    def neighbours(v):
        return before(v, masks) + after(v, masks)

    def sweep_once(i, carry):
        here = prev[i + 1, 0]
        earlier = None
        for z in range(layers):
            later = prev[i + 1, z + 1] if z < layers - 1 else None
            total = CENTRE * here + (prev[i, z] + prev[i + 2, z]) + neighbours(here)
            if earlier is not None:
                total = total + earlier
            if later is not None:
                total = total + later
            once[i, z] = total
            earlier, here = here, later
        return carry

    lax.fori_loop(2, rows, sweep_once, 0)

    @pl.when(has_left)
    def _():
        for copy in to_right[:4]:
            copy.wait_recv()

    @pl.when(has_right)
    def _():
        for copy in to_left[:4]:
            copy.wait_recv()

    corners = []
    for number, (src, dst, lat_to, depth_to, have_to, lat_from, depth_from) in enumerate((
        (prev.at[rows + 1, layers - 1], above.at[0, 1], lat + 1, depth + 1, (has_right, has_down), has_left, has_up),
        (prev.at[2, layers - 1], above.at[rows + 1, 1], lat - 1, depth + 1, (has_left, has_down), has_right, has_up),
        (prev.at[rows + 1, 0], below.at[0, 0], lat + 1, depth - 1, (has_right, has_up), has_left, has_down),
        (prev.at[2, 0], below.at[rows + 1, 0], lat - 1, depth - 1, (has_left, has_up), has_right, has_down),
    )):
        copy = remote(src, dst, corner_send.at[number], corner_recv.at[number], {"lat": lat_to, "depth": depth_to})
        goes = jnp.logical_and(*have_to)
        comes = jnp.logical_and(lat_from, depth_from)
        corners.append((copy, goes, comes))

        @pl.when(goes)
        def _():
            copy.start()

    rate = [rates[k] for k in range(16)]

    def lookup(index):
        level = rate
        for bit in range(4):
            odd = (index & (1 << bit)) != 0
            level = [jnp.where(odd, level[2 * k + 1], level[2 * k]) for k in range(len(level) // 2)]
        return level[0]

    def advect(i, store):
        low, middle, high = surf[i], surf[i + 1], surf[i + 2]
        west, east = before(middle, masks), after(middle, masks)
        grad_rows = (high - low) * 0.5
        grad_cols = (east - west) * 0.5
        laplace = high + low + east + west - 4.0 * middle
        tendency = -vel[0, i] * grad_rows - vel[1, i] * grad_cols + lookup(bmap[i]) * laplace
        new = middle + TIME_STEP * flags[i].astype(jnp.float32) * tendency
        if store:
            new_surface[i - 2] = new
        shift[i] = new - middle

    def advect_inner(i, carry):
        advect(i, True)
        return carry

    lax.fori_loop(2, rows + 2, advect_inner, 0)
    for i in (0, 1, rows + 2, rows + 3):
        advect(i, False)

    def widen(src, dst, i):
        here = src[i + 1]
        dst[i] = (CENTRE + 2.0) * here + (src[i] + src[i + 2]) + neighbours(here)

    def widen_once(i, carry):
        widen(shift, wide, i)
        return carry

    def widen_twice(i, carry):
        widen(wide, widest, i)
        return carry

    lax.fori_loop(0, rows + 2, widen_once, 0)

    @pl.when(jnp.logical_not(has_left))
    def _():
        clear(wide.at[0])

    @pl.when(jnp.logical_not(has_right))
    def _():
        clear(wide.at[rows + 1])

    lax.fori_loop(0, rows, widen_twice, 0)

    all_layers = layers * n_depth
    profile = [
        (all_layers - (depth * layers + z)).astype(jnp.float32) / all_layers * SCALE for z in range(layers)
    ]
    zero = jnp.float32(0.0)
    top = jnp.where(has_up, zero, jnp.float32(SCALE))
    upper = jnp.where(has_up, jnp.float32(SCALE), zero)
    lower = jnp.where(has_down, jnp.float32(SCALE), zero)

    def narrow(v):
        return sum(v[:, k * 128:(k + 1) * 128] for k in range(width // 128))

    def sweep_twice(i, carry):
        here = once[i + 1, 0]
        earlier = None
        part = widest[i]
        acc = None
        for z in range(layers):
            later = once[i + 1, z + 1] if z < layers - 1 else None
            total = CENTRE * here + (once[i, z] + once[i + 2, z]) + neighbours(here)
            if earlier is not None:
                total = total + earlier
            if later is not None:
                total = total + later
            total = SCALE * total + profile[z] * part
            if z == 0:
                total = total + upper * prev[i + 2, 0] + top * (
                    (1.0 / SHARE + 2.0 / all_layers) * shift[i + 2]
                    - (1.0 + 2.0 / all_layers) * wide[i + 1])
            elif z == 1:
                total = total - (top * (1.0 / all_layers)) * shift[i + 2]
            elif z == layers - 1:
                total = total + lower * prev[i + 2, layers - 1]
            elif z < layers - 2:
                acc = total * total if acc is None else acc + total * total
            mesh_out[i, z] = total
            earlier, here = here, later
        squares[i] = narrow(acc)
        return carry

    lax.fori_loop(2, rows - 2, sweep_twice, 0)

    @pl.when(has_left)
    def _():
        to_right[4].wait_recv()
        sweep_once(0, 0)

    @pl.when(has_right)
    def _():
        to_left[4].wait_recv()
        sweep_once(rows + 1, 0)

    sweep_once(1, 0)
    sweep_once(rows, 0)

    def at_edges(k, carry):
        sweep_twice(k, 0)
        sweep_twice(rows - 1 - k, 0)
        return carry

    lax.fori_loop(0, 2, at_edges, 0)

    def finish(i, carry):
        acc = None
        for ref, near, far, outer, inner in ((above, 1, 0, 0, 1), (below, 0, 1, layers - 1, layers - 2)):
            here = ref[i + 1, near]
            around = ref[i, near] + ref[i + 2, near] + neighbours(here)
            edge = mesh_out[i, outer] + SCALE * (2.0 * CENTRE * here + 2.0 * around + ref[i + 1, far])
            next_in = mesh_out[i, inner] + SCALE * here
            mesh_out[i, outer] = edge
            mesh_out[i, inner] = next_in
            both = edge * edge + next_in * next_in
            acc = both if acc is None else acc + both
        squares[i] = squares[i] + narrow(acc)
        return carry

    for copy, goes, comes in corners:
        @pl.when(comes)
        def _():
            copy.wait_recv()

    done = 0
    for c in range(CHUNKS):
        @pl.when(has_up)
        def _():
            to_down[c].wait_recv()

        @pl.when(has_down)
        def _():
            to_up[c].wait_recv()

        ready = rows if c == CHUNKS - 1 else (c + 1) * step - 1
        lax.fori_loop(done, ready, finish, 0)
        done = ready

    totals[depth] = jnp.sum(squares[...], axis=1)
    spread = []
    for k in range(1, n_depth):
        target = lax.rem(depth + k, n_depth)
        copy = remote(totals.at[depth], totals.at[depth], sum_send.at[k - 1], sum_recv.at[k - 1], {"depth": target})
        copy.start()
        spread.append(copy)
    for copy in spread:
        copy.wait_recv()
    total = totals[0]
    for k in range(1, n_depth):
        total = total + totals[k]
    norm = jnp.sqrt(jnp.sum(total, axis=1, keepdims=True) / (all_layers * SUB * width))
    spot = lax.broadcasted_iota(jnp.int32, (rows, 128), 0) == lax.broadcasted_iota(jnp.int32, (rows, 128), 1)
    norm_out[...] = jnp.sum(jnp.where(spot, norm, 0.0), axis=0, keepdims=True)

    @pl.when(has_down)
    def _():
        for copy in to_down:
            copy.wait_send()

    @pl.when(has_up)
    def _():
        for copy in to_up:
            copy.wait_send()

    @pl.when(has_right)
    def _():
        for copy in to_right:
            copy.wait_send()

    @pl.when(has_left)
    def _():
        for copy in to_left:
            copy.wait_send()

    for copy, goes, comes in corners:
        @pl.when(goes)
        def _():
            copy.wait_send()

    for copy in spread:
        copy.wait_send()


def store_kernel(rows, width, mesh_in, surface_in, norm_in, mesh_out, surface_out, norm_out, sem):
    copies = []
    for s in range(SUB):
        cols = slice(s * width, (s + 1) * width)
        copies.append(pltpu.make_async_copy(mesh_in.at[:, :, s, :], mesh_out.at[:, :, cols], sem.at[s]))
        copies.append(pltpu.make_async_copy(surface_in.at[:, s, :], surface_out.at[:, cols], sem.at[SUB + s]))
    for copy in copies:
        copy.start()
    norm_out[...] = norm_in[0, :rows]
    for copy in copies:
        copy.wait()


def solution(mesh):
    n_lat, n_depth = mesh.shape["lat"], mesh.shape["depth"]

    def per_device(surface, velocity, block_map, free_flags, block_rates, previous):
        rows, layers, columns = previous.shape
        width = columns // SUB
        f32 = jnp.float32

        def vmem(*shape, dtype=f32):
            return pltpu.VMEM(shape, dtype)

        def kernel(*refs):
            relax_kernel(rows, layers, width, n_lat, n_depth, *refs)

        hbm = pl.BlockSpec(memory_space=pl.ANY)
        inside = pl.BlockSpec(memory_space=pltpu.VMEM)
        dma = pltpu.SemaphoreType.DMA
        new_surface, field, norm = pl.pallas_call(
            kernel,
            out_shape=(
                jax.ShapeDtypeStruct((rows, SUB, width), f32),
                jax.ShapeDtypeStruct((rows, layers, SUB, width), f32),
                jax.ShapeDtypeStruct((1, 128), f32),
            ),
            in_specs=[hbm] * 6,
            out_specs=(inside, inside, inside),
            scratch_shapes=[
                vmem(rows + 4, layers, SUB, width),
                vmem(rows + 2, layers, SUB, width),
                vmem(rows + 2, 2, SUB, width),
                vmem(rows + 2, 2, SUB, width),
                vmem(rows + 6, SUB, width),
                vmem(2, rows + 4, SUB, width),
                vmem(rows + 4, SUB, width, dtype=jnp.int32),
                vmem(rows + 4, SUB, width, dtype=jnp.int32),
                pltpu.SMEM((16,), f32),
                vmem(rows + 4, SUB, width),
                vmem(rows + 2, SUB, width),
                vmem(rows, SUB, width),
                vmem(rows, SUB, 128),
                vmem(n_depth, rows, 128),
                dma((8 * SUB + 1,)),
                dma((CHUNKS,)), dma((CHUNKS,)), dma((CHUNKS,)), dma((CHUNKS,)),
                dma((2, 5)), dma((2, 5)),
                dma((4,)), dma((4,)),
                dma((n_depth - 1,)), dma((n_depth - 1,)),
            ],
            compiler_params=pltpu.CompilerParams(
                collective_id=0, has_side_effects=True, vmem_limit_bytes=VMEM_LIMIT
            ),
            name="relax",
        )(surface, velocity, block_map, free_flags, block_rates, previous)

        def store(*refs):
            store_kernel(rows, width, *refs)

        field, new_surface, norm = pl.pallas_call(
            store,
            out_shape=(
                jax.ShapeDtypeStruct(previous.shape, f32),
                jax.ShapeDtypeStruct(surface.shape, f32),
                jax.ShapeDtypeStruct((rows,), f32),
            ),
            in_specs=[inside, inside, inside],
            out_specs=(hbm, hbm, inside),
            scratch_shapes=[dma((2 * SUB,))],
            name="store",
        )(field, new_surface, norm)
        return new_surface, field, norm

    return jax.shard_map(
        per_device,
        mesh=mesh,
        in_specs=(
            P("lat", None), P(None, "lat", None), P("lat", None), P("lat", None), P(),
            P("lat", "depth", None),
        ),
        out_specs=(P("lat", None), P("lat", "depth", None), P("lat")),
        check_vma=False,
    )


VMEM_LIMIT = 58 * 1024 * 1024
```

```python
import jax
import jax.numpy as jnp
from jax import lax
from jax.experimental import pallas as pl
from jax.experimental.pallas import tpu as pltpu
from jax.sharding import PartitionSpec as P

MESH = pl.DeviceIdType.MESH
TIME_STEP = 0.5
RELAX_WEIGHT = 0.8
KEEP = 1.0 - RELAX_WEIGHT
SHARE = RELAX_WEIGHT / 6.0
CENTRE = KEEP / SHARE
SCALE = SHARE * SHARE
SUB = 8
CHUNKS = 8


def iotas(width):
    lane = lax.broadcasted_iota(jnp.int32, (SUB, 128), 1)
    sub = lax.broadcasted_iota(jnp.int32, (SUB, 128), 0)
    return lane, sub


def before(v, masks):
    width = v.shape[-1]
    rolled = pltpu.roll(v, 1, 1)
    first = rolled[:, :128]
    carried = pltpu.roll(first, 1, 0)
    first = jnp.where(masks[0], jnp.where(masks[1], 0.0, carried), first)
    return jnp.concatenate([first, rolled[:, 128:]], axis=1)


def after(v, masks):
    width = v.shape[-1]
    rolled = pltpu.roll(v, width - 1, 1)
    last = rolled[:, width - 128:]
    carried = pltpu.roll(last, SUB - 1, 0)
    last = jnp.where(masks[2], jnp.where(masks[3], 0.0, carried), last)
    return jnp.concatenate([rolled[:, : width - 128], last], axis=1)


def relax_kernel(
    rows, layers, width, n_lat, n_depth,
    surface, velocity, block_map, free_flags, block_rates, previous,
    new_surface, mesh_out, norm_out,
    prev, once, above, below, surf, vel, bmap, flags, rates,
    shift, wide, widest, squares, totals,
    load_sem, up_send, up_recv, down_send, down_recv, side_send, side_recv,
    corner_send, corner_recv, sum_send, sum_recv,
):
    lat = lax.axis_index("lat")
    depth = lax.axis_index("depth")
    has_left, has_right = lat > 0, lat < n_lat - 1
    has_up, has_down = depth > 0, depth < n_depth - 1
    left, right = {"lat": lat - 1}, {"lat": lat + 1}
    up, down = {"depth": depth - 1}, {"depth": depth + 1}

    barrier = pltpu.get_barrier_semaphore()
    for k in (1, n_depth - 1):
        pl.semaphore_signal(
            barrier, inc=1, device_id={"depth": lax.rem(depth + k, n_depth)}, device_id_type=MESH)
    for have, target in ((has_left, left), (has_right, right)):
        @pl.when(have)
        def _():
            pl.semaphore_signal(barrier, inc=1, device_id=target, device_id_type=MESH)

    count = 0
    groups = {}

    def load(name, pairs):
        nonlocal count
        copies = []
        for src, dst in pairs:
            copy = pltpu.make_async_copy(src, dst, load_sem.at[count])
            copy.start()
            copies.append(copy)
            count += 1
        groups[name] = copies

    def loaded(name):
        for copy in groups[name]:
            copy.wait()

    cols = [slice(s * width, (s + 1) * width) for s in range(SUB)]
    own = slice(2, 2 + rows)
    load("outer", [
        (previous.at[:, part, cols[s]], prev.at[own, part, s, :])
        for part in (slice(layers - 2, layers), slice(0, 2)) for s in range(SUB)
    ])
    load("surface",
         [(surface.at[:, cols[s]], surf.at[slice(3, 3 + rows), s, :]) for s in range(SUB)]
         + [(velocity.at[:, :, cols[s]], vel.at[:, own, s, :]) for s in range(SUB)]
         + [(block_map.at[:, cols[s]], bmap.at[own, s, :]) for s in range(SUB)]
         + [(free_flags.at[:, cols[s]], flags.at[own, s, :]) for s in range(SUB)]
         + [(block_rates, rates)])
    load("inner", [
        (previous.at[:, part, cols[s]], prev.at[own, part, s, :])
        for part in (slice(2, SUB), slice(layers - SUB, layers - 2)) for s in range(SUB)
    ])

    def clear(ref):
        ref[...] = jnp.zeros(ref.shape, ref.dtype)

    @pl.when(jnp.logical_not(has_up))
    def _():
        clear(above)

    @pl.when(jnp.logical_not(has_down))
    def _():
        clear(below)

    for have, near, far, at in (
        (has_left, slice(0, 2), slice(0, 3), 0),
        (has_right, slice(rows + 2, rows + 4), slice(rows + 3, rows + 6), rows + 1),
    ):
        @pl.when(jnp.logical_not(have))
        def _():
            clear(prev.at[near])
            clear(surf.at[far])
            clear(vel.at[:, near])
            clear(bmap.at[near])
            clear(flags.at[near])
            clear(above.at[at])
            clear(below.at[at])
            clear(once.at[at])

    pl.semaphore_wait(barrier, 2 + has_left.astype(jnp.int32) + has_right.astype(jnp.int32))

    def remote(src, dst, send, recv, target):
        return pltpu.make_async_remote_copy(
            src_ref=src, dst_ref=dst, send_sem=send, recv_sem=recv,
            device_id=target, device_id_type=MESH,
        )

    step = rows // CHUNKS
    last_two, first_two = slice(layers - 2, layers), slice(0, 2)
    to_down, to_up = [], []
    for c in range(CHUNKS):
        mine = slice(2 + c * step, 2 + (c + 1) * step)
        theirs = slice(1 + c * step, 1 + (c + 1) * step)
        to_down.append(remote(prev.at[mine, last_two], above.at[theirs], down_send.at[c], down_recv.at[c], down))
        to_up.append(remote(prev.at[mine, first_two], below.at[theirs], up_send.at[c], up_recv.at[c], up))

    loaded("outer")

    @pl.when(has_down)
    def _():
        for copy in to_down:
            copy.start()

    @pl.when(has_up)
    def _():
        for copy in to_up:
            copy.start()

    def sides(mine3, theirs3, mine2, theirs2, row, target):
        return [
            remote(surf.at[mine3], surf.at[theirs3], side_send.at[row, 0], side_recv.at[row, 0], target),
            remote(vel.at[:, mine2], vel.at[:, theirs2], side_send.at[row, 1], side_recv.at[row, 1], target),
            remote(bmap.at[mine2], bmap.at[theirs2], side_send.at[row, 2], side_recv.at[row, 2], target),
            remote(flags.at[mine2], flags.at[theirs2], side_send.at[row, 3], side_recv.at[row, 3], target),
            remote(prev.at[mine2], prev.at[theirs2], side_send.at[row, 4], side_recv.at[row, 4], target),
        ]

    to_right = sides(slice(rows, rows + 3), slice(0, 3), slice(rows, rows + 2), slice(0, 2), 0, right)
    to_left = sides(slice(3, 6), slice(rows + 3, rows + 6), slice(2, 4), slice(rows + 2, rows + 4), 1, left)

    loaded("surface")

    @pl.when(has_right)
    def _():
        for copy in to_right[:4]:
            copy.start()

    @pl.when(has_left)
    def _():
        for copy in to_left[:4]:
            copy.start()

    loaded("inner")

    @pl.when(has_right)
    def _():
        to_right[4].start()

    @pl.when(has_left)
    def _():
        to_left[4].start()

    lane, sub = iotas(width)
    masks = (lane == 0, sub == 0, lane == 127, sub == SUB - 1)

    def neighbours(v):
        return before(v, masks) + after(v, masks)

    def sweep_once(i, carry):
        here = prev[i + 1, 0]
        earlier = None
        for z in range(layers):
            later = prev[i + 1, z + 1] if z < layers - 1 else None
            total = CENTRE * here + (prev[i, z] + prev[i + 2, z]) + neighbours(here)
            if earlier is not None:
                total = total + earlier
            if later is not None:
                total = total + later
            once[i, z] = total
            earlier, here = here, later
        return carry

    lax.fori_loop(2, rows, sweep_once, 0)

    @pl.when(has_left)
    def _():
        for copy in to_right[:4]:
            copy.wait_recv()

    @pl.when(has_right)
    def _():
        for copy in to_left[:4]:
            copy.wait_recv()

    corners = []
    for number, (src, dst, lat_to, depth_to, have_to, lat_from, depth_from) in enumerate((
        (prev.at[rows + 1, layers - 1], above.at[0, 1], lat + 1, depth + 1, (has_right, has_down), has_left, has_up),
        (prev.at[2, layers - 1], above.at[rows + 1, 1], lat - 1, depth + 1, (has_left, has_down), has_right, has_up),
        (prev.at[rows + 1, 0], below.at[0, 0], lat + 1, depth - 1, (has_right, has_up), has_left, has_down),
        (prev.at[2, 0], below.at[rows + 1, 0], lat - 1, depth - 1, (has_left, has_up), has_right, has_down),
    )):
        copy = remote(src, dst, corner_send.at[number], corner_recv.at[number], {"lat": lat_to, "depth": depth_to})
        goes = jnp.logical_and(*have_to)
        comes = jnp.logical_and(lat_from, depth_from)
        corners.append((copy, goes, comes))

        @pl.when(goes)
        def _():
            copy.start()

    rate = [rates[k] for k in range(16)]

    def lookup(index):
        level = rate
        for bit in range(4):
            odd = (index & (1 << bit)) != 0
            level = [jnp.where(odd, level[2 * k + 1], level[2 * k]) for k in range(len(level) // 2)]
        return level[0]

    def advect(i, store):
        low, middle, high = surf[i], surf[i + 1], surf[i + 2]
        west, east = before(middle, masks), after(middle, masks)
        grad_rows = (high - low) * 0.5
        grad_cols = (east - west) * 0.5
        laplace = high + low + east + west - 4.0 * middle
        tendency = -vel[0, i] * grad_rows - vel[1, i] * grad_cols + lookup(bmap[i]) * laplace
        new = middle + TIME_STEP * flags[i].astype(jnp.float32) * tendency
        if store:
            new_surface[i - 2] = new
        shift[i] = new - middle

    def advect_inner(i, carry):
        advect(i, True)
        return carry

    lax.fori_loop(2, rows + 2, advect_inner, 0)
    for i in (0, 1, rows + 2, rows + 3):
        advect(i, False)

    def widen(src, dst, i):
        here = src[i + 1]
        dst[i] = (CENTRE + 2.0) * here + (src[i] + src[i + 2]) + neighbours(here)

    def widen_once(i, carry):
        widen(shift, wide, i)
        return carry

    def widen_twice(i, carry):
        widen(wide, widest, i)
        return carry

    lax.fori_loop(0, rows + 2, widen_once, 0)

    @pl.when(jnp.logical_not(has_left))
    def _():
        clear(wide.at[0])

    @pl.when(jnp.logical_not(has_right))
    def _():
        clear(wide.at[rows + 1])

    lax.fori_loop(0, rows, widen_twice, 0)

    all_layers = layers * n_depth
    profile = [
        (all_layers - (depth * layers + z)).astype(jnp.float32) / all_layers * SCALE for z in range(layers)
    ]
    zero = jnp.float32(0.0)
    top = jnp.where(has_up, zero, jnp.float32(SCALE))
    upper = jnp.where(has_up, jnp.float32(SCALE), zero)
    lower = jnp.where(has_down, jnp.float32(SCALE), zero)

    def narrow(v):
        return sum(v[:, k * 128:(k + 1) * 128] for k in range(width // 128))

    def sweep_twice(i, carry):
        here = once[i + 1, 0]
        earlier = None
        part = widest[i]
        acc = None
        for z in range(layers):
            later = once[i + 1, z + 1] if z < layers - 1 else None
            total = CENTRE * here + (once[i, z] + once[i + 2, z]) + neighbours(here)
            if earlier is not None:
                total = total + earlier
            if later is not None:
                total = total + later
            total = SCALE * total + profile[z] * part
            if z == 0:
                total = total + upper * prev[i + 2, 0] + top * (
                    (1.0 / SHARE + 2.0 / all_layers) * shift[i + 2]
                    - (1.0 + 2.0 / all_layers) * wide[i + 1])
            elif z == 1:
                total = total - (top * (1.0 / all_layers)) * shift[i + 2]
            elif z == layers - 1:
                total = total + lower * prev[i + 2, layers - 1]
            elif z < layers - 2:
                acc = total * total if acc is None else acc + total * total
            mesh_out[i, z] = total
            earlier, here = here, later
        squares[i] = narrow(acc)
        return carry

    lax.fori_loop(2, rows - 2, sweep_twice, 0)

    @pl.when(has_left)
    def _():
        to_right[4].wait_recv()
        sweep_once(0, 0)

    @pl.when(has_right)
    def _():
        to_left[4].wait_recv()
        sweep_once(rows + 1, 0)

    sweep_once(1, 0)
    sweep_once(rows, 0)

    def at_edges(k, carry):
        sweep_twice(k, 0)
        sweep_twice(rows - 1 - k, 0)
        return carry

    lax.fori_loop(0, 2, at_edges, 0)

    def finish(i, carry):
        acc = None
        for ref, near, far, outer, inner in ((above, 1, 0, 0, 1), (below, 0, 1, layers - 1, layers - 2)):
            here = ref[i + 1, near]
            around = ref[i, near] + ref[i + 2, near] + neighbours(here)
            edge = mesh_out[i, outer] + SCALE * (2.0 * CENTRE * here + 2.0 * around + ref[i + 1, far])
            next_in = mesh_out[i, inner] + SCALE * here
            mesh_out[i, outer] = edge
            mesh_out[i, inner] = next_in
            both = edge * edge + next_in * next_in
            acc = both if acc is None else acc + both
        squares[i] = squares[i] + narrow(acc)
        return carry

    for copy, goes, comes in corners:
        @pl.when(comes)
        def _():
            copy.wait_recv()

    done = 0
    for c in range(CHUNKS):
        @pl.when(has_up)
        def _():
            to_down[c].wait_recv()

        @pl.when(has_down)
        def _():
            to_up[c].wait_recv()

        ready = rows if c == CHUNKS - 1 else (c + 1) * step - 1
        lax.fori_loop(done, ready, finish, 0)
        done = ready

    totals[depth] = jnp.sum(squares[...], axis=1)
    spread = []
    for k in range(1, n_depth):
        target = lax.rem(depth + k, n_depth)
        copy = remote(totals.at[depth], totals.at[depth], sum_send.at[k - 1], sum_recv.at[k - 1], {"depth": target})
        copy.start()
        spread.append(copy)
    for copy in spread:
        copy.wait_recv()
    total = totals[0]
    for k in range(1, n_depth):
        total = total + totals[k]
    norm = jnp.sqrt(jnp.sum(total, axis=1, keepdims=True) / (all_layers * SUB * width))
    spot = lax.broadcasted_iota(jnp.int32, (rows, 128), 0) == lax.broadcasted_iota(jnp.int32, (rows, 128), 1)
    norm_out[...] = jnp.sum(jnp.where(spot, norm, 0.0), axis=0, keepdims=True)

    @pl.when(has_down)
    def _():
        for copy in to_down:
            copy.wait_send()

    @pl.when(has_up)
    def _():
        for copy in to_up:
            copy.wait_send()

    @pl.when(has_right)
    def _():
        for copy in to_right:
            copy.wait_send()

    @pl.when(has_left)
    def _():
        for copy in to_left:
            copy.wait_send()

    for copy, goes, comes in corners:
        @pl.when(goes)
        def _():
            copy.wait_send()

    for copy in spread:
        copy.wait_send()


def store_kernel(rows, width, mesh_in, surface_in, norm_in, mesh_out, surface_out, norm_out, sem):
    copies = []
    for s in range(SUB):
        cols = slice(s * width, (s + 1) * width)
        copies.append(pltpu.make_async_copy(mesh_in.at[:, :, s, :], mesh_out.at[:, :, cols], sem.at[s]))
        copies.append(pltpu.make_async_copy(surface_in.at[:, s, :], surface_out.at[:, cols], sem.at[SUB + s]))
    for copy in copies:
        copy.start()
    norm_out[...] = norm_in[0, :rows]
    for copy in copies:
        copy.wait()


def solution(mesh):
    n_lat, n_depth = mesh.shape["lat"], mesh.shape["depth"]

    def per_device(surface, velocity, block_map, free_flags, block_rates, previous):
        rows, layers, columns = previous.shape
        width = columns // SUB
        f32 = jnp.float32

        def vmem(*shape, dtype=f32):
            return pltpu.VMEM(shape, dtype)

        def kernel(*refs):
            relax_kernel(rows, layers, width, n_lat, n_depth, *refs)

        hbm = pl.BlockSpec(memory_space=pl.ANY)
        inside = pl.BlockSpec(memory_space=pltpu.VMEM)
        dma = pltpu.SemaphoreType.DMA
        new_surface, field, norm = pl.pallas_call(
            kernel,
            out_shape=(
                jax.ShapeDtypeStruct((rows, SUB, width), f32),
                jax.ShapeDtypeStruct((rows, layers, SUB, width), f32),
                jax.ShapeDtypeStruct((1, 128), f32),
            ),
            in_specs=[hbm] * 6,
            out_specs=(inside, inside, inside),
            scratch_shapes=[
                vmem(rows + 4, layers, SUB, width),
                vmem(rows + 2, layers, SUB, width),
                vmem(rows + 2, 2, SUB, width),
                vmem(rows + 2, 2, SUB, width),
                vmem(rows + 6, SUB, width),
                vmem(2, rows + 4, SUB, width),
                vmem(rows + 4, SUB, width, dtype=jnp.int32),
                vmem(rows + 4, SUB, width, dtype=jnp.int32),
                pltpu.SMEM((16,), f32),
                vmem(rows + 4, SUB, width),
                vmem(rows + 2, SUB, width),
                vmem(rows, SUB, width),
                vmem(rows, SUB, 128),
                vmem(n_depth, rows, 128),
                dma((8 * SUB + 1,)),
                dma((CHUNKS,)), dma((CHUNKS,)), dma((CHUNKS,)), dma((CHUNKS,)),
                dma((2, 5)), dma((2, 5)),
                dma((4,)), dma((4,)),
                dma((n_depth - 1,)), dma((n_depth - 1,)),
            ],
            compiler_params=pltpu.CompilerParams(
                collective_id=0, has_side_effects=True, vmem_limit_bytes=VMEM_LIMIT
            ),
            name="relax",
        )(*(
            pltpu.with_memory_space_constraint(value, pltpu.HBM)
            for value in (surface, velocity, block_map, free_flags, block_rates, previous)
        ))

        def store(*refs):
            store_kernel(rows, width, *refs)

        field, new_surface, norm = pl.pallas_call(
            store,
            out_shape=(
                jax.ShapeDtypeStruct(previous.shape, f32),
                jax.ShapeDtypeStruct(surface.shape, f32),
                jax.ShapeDtypeStruct((rows,), f32),
            ),
            in_specs=[inside, inside, inside],
            out_specs=(hbm, hbm, inside),
            scratch_shapes=[dma((2 * SUB,))],
            compiler_params=pltpu.CompilerParams(vmem_limit_bytes=1024 * 1024),
            name="store",
        )(field, new_surface, norm)
        return new_surface, field, norm

    return jax.shard_map(
        per_device,
        mesh=mesh,
        in_specs=(
            P("lat", None), P(None, "lat", None), P("lat", None), P("lat", None), P(),
            P("lat", "depth", None),
        ),
        out_specs=(P("lat", None), P("lat", "depth", None), P("lat")),
        check_vma=False,
    )


VMEM_LIMIT = 40 * 1024 * 1024
```

```python
import jax
import jax.numpy as jnp
from jax import lax
from jax.experimental import pallas as pl
from jax.experimental.pallas import tpu as pltpu
from jax.sharding import PartitionSpec as P

MESH = pl.DeviceIdType.MESH
TIME_STEP = 0.5
RELAX_WEIGHT = 0.8
KEEP = 1.0 - RELAX_WEIGHT
SHARE = RELAX_WEIGHT / 6.0
CENTRE = KEEP / SHARE
SCALE = SHARE * SHARE
SUB = 8
CHUNKS = 8


def iotas(width):
    lane = lax.broadcasted_iota(jnp.int32, (SUB, 128), 1)
    sub = lax.broadcasted_iota(jnp.int32, (SUB, 128), 0)
    return lane, sub


def before(v, masks):
    width = v.shape[-1]
    rolled = pltpu.roll(v, 1, 1)
    first = rolled[:, :128]
    carried = pltpu.roll(first, 1, 0)
    first = jnp.where(masks[0], jnp.where(masks[1], 0.0, carried), first)
    return jnp.concatenate([first, rolled[:, 128:]], axis=1)


def after(v, masks):
    width = v.shape[-1]
    rolled = pltpu.roll(v, width - 1, 1)
    last = rolled[:, width - 128:]
    carried = pltpu.roll(last, SUB - 1, 0)
    last = jnp.where(masks[2], jnp.where(masks[3], 0.0, carried), last)
    return jnp.concatenate([rolled[:, : width - 128], last], axis=1)


def relax_kernel(
    rows, layers, width, n_lat, n_depth,
    surface, velocity, block_map, free_flags, block_rates, previous,
    new_surface, mesh_out, norm_out,
    prev, once, above, below, surf, vel, bmap, flags, rates,
    shift, wide, widest, squares, totals,
    load_sem, up_send, up_recv, down_send, down_recv, side_send, side_recv,
    corner_send, corner_recv, sum_send, sum_recv, relay_sem,
):
    lat = lax.axis_index("lat")
    depth = lax.axis_index("depth")
    has_left, has_right = lat > 0, lat < n_lat - 1
    has_up, has_down = depth > 0, depth < n_depth - 1
    left, right = {"lat": lat - 1}, {"lat": lat + 1}
    up, down = {"depth": depth - 1}, {"depth": depth + 1}

    barrier = pltpu.get_barrier_semaphore()
    around = ((has_up, up), (has_down, down), (has_left, left), (has_right, right))
    for have, target in around:
        @pl.when(have)
        def _():
            pl.semaphore_signal(barrier, inc=1, device_id=target, device_id_type=MESH)

    count = 0
    groups = {}

    def load(name, pairs):
        nonlocal count
        copies = []
        for src, dst in pairs:
            copy = pltpu.make_async_copy(src, dst, load_sem.at[count])
            copy.start()
            copies.append(copy)
            count += 1
        groups[name] = copies

    def loaded(name):
        for copy in groups[name]:
            copy.wait()

    cols = [slice(s * width, (s + 1) * width) for s in range(SUB)]
    own = slice(2, 2 + rows)
    load("outer", [
        (previous.at[:, part, cols[s]], prev.at[own, part, s, :])
        for part in (slice(layers - 2, layers), slice(0, 2)) for s in range(SUB)
    ])
    load("surface",
         [(surface.at[:, cols[s]], surf.at[slice(3, 3 + rows), s, :]) for s in range(SUB)]
         + [(velocity.at[:, :, cols[s]], vel.at[:, own, s, :]) for s in range(SUB)]
         + [(block_map.at[:, cols[s]], bmap.at[own, s, :]) for s in range(SUB)]
         + [(free_flags.at[:, cols[s]], flags.at[own, s, :]) for s in range(SUB)]
         + [(block_rates, rates)])
    load("inner", [
        (previous.at[:, part, cols[s]], prev.at[own, part, s, :])
        for part in (slice(2, SUB), slice(layers - SUB, layers - 2)) for s in range(SUB)
    ])

    def clear(ref):
        ref[...] = jnp.zeros(ref.shape, ref.dtype)

    @pl.when(jnp.logical_not(has_up))
    def _():
        clear(above)

    @pl.when(jnp.logical_not(has_down))
    def _():
        clear(below)

    for have, near, far, at in (
        (has_left, slice(0, 2), slice(0, 3), 0),
        (has_right, slice(rows + 2, rows + 4), slice(rows + 3, rows + 6), rows + 1),
    ):
        @pl.when(jnp.logical_not(have))
        def _():
            clear(prev.at[near])
            clear(surf.at[far])
            clear(vel.at[:, near])
            clear(bmap.at[near])
            clear(flags.at[near])
            clear(above.at[at])
            clear(below.at[at])
            clear(once.at[at])

    pl.semaphore_wait(barrier, sum(have.astype(jnp.int32) for have, _ in around))

    def remote(src, dst, send, recv, target):
        return pltpu.make_async_remote_copy(
            src_ref=src, dst_ref=dst, send_sem=send, recv_sem=recv,
            device_id=target, device_id_type=MESH,
        )

    step = rows // CHUNKS
    last_two, first_two = slice(layers - 2, layers), slice(0, 2)
    to_down, to_up = [], []
    for c in range(CHUNKS):
        mine = slice(2 + c * step, 2 + (c + 1) * step)
        theirs = slice(1 + c * step, 1 + (c + 1) * step)
        to_down.append(remote(prev.at[mine, last_two], above.at[theirs], down_send.at[c], down_recv.at[c], down))
        to_up.append(remote(prev.at[mine, first_two], below.at[theirs], up_send.at[c], up_recv.at[c], up))

    loaded("outer")

    @pl.when(has_down)
    def _():
        for copy in to_down:
            copy.start()

    @pl.when(has_up)
    def _():
        for copy in to_up:
            copy.start()

    def sides(mine3, theirs3, mine2, theirs2, near, far, row, target):
        return [
            remote(surf.at[mine3], surf.at[theirs3], side_send.at[row, 0], side_recv.at[row, 0], target),
            remote(vel.at[:, mine2], vel.at[:, theirs2], side_send.at[row, 1], side_recv.at[row, 1], target),
            remote(bmap.at[mine2], bmap.at[theirs2], side_send.at[row, 2], side_recv.at[row, 2], target),
            remote(flags.at[mine2], flags.at[theirs2], side_send.at[row, 3], side_recv.at[row, 3], target),
            remote(prev.at[near[0]], prev.at[near[1]], side_send.at[row, 4], side_recv.at[row, 4], target),
            remote(prev.at[far[0]], prev.at[far[1]], side_send.at[row, 5], side_recv.at[row, 5], target),
        ]

    to_right = sides(slice(rows, rows + 3), slice(0, 3), slice(rows, rows + 2), slice(0, 2),
                     (rows + 1, 1), (rows, 0), 0, right)
    to_left = sides(slice(3, 6), slice(rows + 3, rows + 6), slice(2, 4), slice(rows + 2, rows + 4),
                    (2, rows + 2), (3, rows + 3), 1, left)

    loaded("surface")

    @pl.when(has_right)
    def _():
        for copy in to_right[:4]:
            copy.start()

    @pl.when(has_left)
    def _():
        for copy in to_left[:4]:
            copy.start()

    loaded("inner")

    @pl.when(has_right)
    def _():
        for copy in to_right[4:]:
            copy.start()

    @pl.when(has_left)
    def _():
        for copy in to_left[4:]:
            copy.start()

    lane, sub = iotas(width)
    masks = (lane == 0, sub == 0, lane == 127, sub == SUB - 1)

    def neighbours(v):
        return before(v, masks) + after(v, masks)

    def sweep_once(i, carry):
        here = prev[i + 1, 0]
        earlier = None
        for z in range(layers):
            later = prev[i + 1, z + 1] if z < layers - 1 else None
            total = CENTRE * here + (prev[i, z] + prev[i + 2, z]) + neighbours(here)
            if earlier is not None:
                total = total + earlier
            if later is not None:
                total = total + later
            once[i, z] = total
            earlier, here = here, later
        return carry

    lax.fori_loop(2, rows, sweep_once, 0)

    rate = [rates[k] for k in range(16)]

    def lookup(index):
        level = rate
        for bit in range(4):
            odd = (index & (1 << bit)) != 0
            level = [jnp.where(odd, level[2 * k + 1], level[2 * k]) for k in range(len(level) // 2)]
        return level[0]

    def advect(i, store):
        low, middle, high = surf[i], surf[i + 1], surf[i + 2]
        west, east = before(middle, masks), after(middle, masks)
        grad_rows = (high - low) * 0.5
        grad_cols = (east - west) * 0.5
        laplace = high + low + east + west - 4.0 * middle
        tendency = -vel[0, i] * grad_rows - vel[1, i] * grad_cols + lookup(bmap[i]) * laplace
        new = middle + TIME_STEP * flags[i].astype(jnp.float32) * tendency
        if store:
            new_surface[i - 2] = new
        shift[i] = new - middle

    def widen(src, dst, i):
        here = src[i + 1]
        dst[i] = (CENTRE + 2.0) * here + (src[i] + src[i + 2]) + neighbours(here)

    all_layers = layers * n_depth
    profile = [
        (all_layers - (depth * layers + z)).astype(jnp.float32) / all_layers * SCALE for z in range(layers)
    ]
    zero = jnp.float32(0.0)
    top = jnp.where(has_up, zero, jnp.float32(SCALE))
    upper = jnp.where(has_up, jnp.float32(SCALE), zero)
    lower = jnp.where(has_down, jnp.float32(SCALE), zero)

    def narrow(v):
        return sum(v[:, k * 128:(k + 1) * 128] for k in range(width // 128))

    def sweep_twice(i, carry):
        here = once[i + 1, 0]
        earlier = None
        part = widest[i]
        acc = None
        for z in range(layers):
            later = once[i + 1, z + 1] if z < layers - 1 else None
            total = CENTRE * here + (once[i, z] + once[i + 2, z]) + neighbours(here)
            if earlier is not None:
                total = total + earlier
            if later is not None:
                total = total + later
            total = SCALE * total + profile[z] * part
            if z == 0:
                total = total + upper * prev[i + 2, 0] + top * (
                    (1.0 / SHARE + 2.0 / all_layers) * shift[i + 2]
                    - (1.0 + 2.0 / all_layers) * wide[i + 1])
            elif z == 1:
                total = total - (top * (1.0 / all_layers)) * shift[i + 2]
            elif z == layers - 1:
                total = total + lower * prev[i + 2, layers - 1]
            elif z < layers - 2:
                acc = total * total if acc is None else acc + total * total
            mesh_out[i, z] = total
            earlier, here = here, later
        squares[i] = narrow(acc)
        return carry

    def grouped(first, last, size, what):
        def some(g, carry):
            for k in range(size):
                what(first + g * size + k)
            return carry

        count = (last - first) // size
        if count:
            lax.fori_loop(0, count, some, 0)
        for i in range(first + count * size, last):
            what(i)

    grouped(3, rows + 1, 5, lambda i: advect(i, True))
    grouped(3, rows - 1, 5, lambda i: widen(shift, wide, i))
    grouped(3, rows - 3, 5, lambda i: widen(wide, widest, i))
    lax.fori_loop(3, rows - 3, sweep_twice, 0)

    @pl.when(has_left)
    def _():
        for copy in to_right[:4]:
            copy.wait_recv()

    @pl.when(has_right)
    def _():
        for copy in to_left[:4]:
            copy.wait_recv()

    corners = []
    for number, (src, dst, lat_to, depth_to, have_to, lat_from, depth_from) in enumerate((
        (prev.at[rows + 1, layers - 1], above.at[0, 1], lat + 1, depth + 1, (has_right, has_down), has_left, has_up),
        (prev.at[2, layers - 1], above.at[rows + 1, 1], lat - 1, depth + 1, (has_left, has_down), has_right, has_up),
        (prev.at[rows + 1, 0], below.at[0, 0], lat + 1, depth - 1, (has_right, has_up), has_left, has_down),
        (prev.at[2, 0], below.at[rows + 1, 0], lat - 1, depth - 1, (has_left, has_up), has_right, has_down),
    )):
        copy = remote(src, dst, corner_send.at[number], corner_recv.at[number], {"lat": lat_to, "depth": depth_to})
        goes = jnp.logical_and(*have_to)
        comes = jnp.logical_and(lat_from, depth_from)
        corners.append((copy, goes, comes))

        @pl.when(goes)
        def _():
            copy.start()

    for i in (0, 1, rows + 2, rows + 3):
        advect(i, False)
    for i in (2, rows + 1):
        advect(i, True)
    for i in (0, 1, 2, rows - 1, rows, rows + 1):
        widen(shift, wide, i)

    @pl.when(jnp.logical_not(has_left))
    def _():
        clear(wide.at[0])

    @pl.when(jnp.logical_not(has_right))
    def _():
        clear(wide.at[rows + 1])

    for i in (0, 1, 2, rows - 3, rows - 2, rows - 1):
        widen(wide, widest, i)

    @pl.when(has_left)
    def _():
        to_right[4].wait_recv()

    @pl.when(has_right)
    def _():
        to_left[4].wait_recv()

    def one_each_side(k, carry):
        sweep_once(1 + k * (rows - 1), 0)
        return carry

    def second_rows(k, carry):
        sweep_twice(lax.select(k < 2, k + 1, rows - 5 + k), 0)
        return carry

    lax.fori_loop(0, 2, one_each_side, 0)
    lax.fori_loop(0, 4, second_rows, 0)

    def finish(first, last):
        parts, values = {}, []
        for i in range(first, last):
            acc = None
            for ref, near, far, outer, inner in ((above, 1, 0, 0, 1), (below, 0, 1, layers - 1, layers - 2)):
                here = ref[i + 1, near]
                around = ref[i, near] + ref[i + 2, near] + neighbours(here)
                edge = mesh_out[i, outer] + SCALE * (2.0 * CENTRE * here + 2.0 * around + ref[i + 1, far])
                next_in = mesh_out[i, inner] + SCALE * here
                values += [(i, outer, edge), (i, inner, next_in)]
                both = edge * edge + next_in * next_in
                acc = both if acc is None else acc + both
            parts[i] = squares[i] + narrow(acc)
        for i, z, value in values:
            mesh_out[i, z] = value
        for i, value in parts.items():
            squares[i] = value

    def arrived(chunk):
        @pl.when(has_up)
        def _():
            to_down[chunk].wait_recv()

        @pl.when(has_down)
        def _():
            to_up[chunk].wait_recv()

    early = 3 * CHUNKS // 4
    for c in range(early):
        arrived(c)

    for have, target in ((has_up, up), (has_down, down)):
        @pl.when(have)
        def _():
            pl.semaphore_signal(relay_sem, inc=1, device_id=target, device_id_type=MESH)

    middle = early * step - 1
    for first in range(3, middle, 4):
        finish(first, min(first + 4, middle))

    @pl.when(has_left)
    def _():
        to_right[5].wait_recv()
        sweep_once(0, 0)

    @pl.when(has_right)
    def _():
        to_left[5].wait_recv()
        sweep_once(rows + 1, 0)

    def edge_rows(k, carry):
        sweep_twice(k * (rows - 1), 0)
        return carry

    lax.fori_loop(0, 2, edge_rows, 0)

    for copy, goes, comes in corners:
        @pl.when(comes)
        def _():
            copy.wait_recv()

    finish(0, 3)
    done = middle
    for c in range(early, CHUNKS):
        arrived(c)
        ready = rows if c == CHUNKS - 1 else (c + 1) * step - 1
        finish(done, ready)
        done = ready

    pl.semaphore_wait(relay_sem, has_up.astype(jnp.int32) + has_down.astype(jnp.int32))
    totals[depth] = jnp.sum(squares[...], axis=1)
    spread = []
    for k in range(1, n_depth):
        target = lax.rem(depth + k, n_depth)
        copy = remote(totals.at[depth], totals.at[depth], sum_send.at[k - 1], sum_recv.at[k - 1], {"depth": target})
        copy.start()
        spread.append(copy)
    for copy in spread:
        copy.wait_recv()
    total = totals[0]
    for k in range(1, n_depth):
        total = total + totals[k]
    norm = jnp.sqrt(jnp.sum(total, axis=1, keepdims=True) / (all_layers * SUB * width))
    spot = lax.broadcasted_iota(jnp.int32, (rows, 128), 0) == lax.broadcasted_iota(jnp.int32, (rows, 128), 1)
    norm_out[...] = jnp.sum(jnp.where(spot, norm, 0.0), axis=0, keepdims=True)

    @pl.when(has_down)
    def _():
        for copy in to_down:
            copy.wait_send()

    @pl.when(has_up)
    def _():
        for copy in to_up:
            copy.wait_send()

    @pl.when(has_right)
    def _():
        for copy in to_right:
            copy.wait_send()

    @pl.when(has_left)
    def _():
        for copy in to_left:
            copy.wait_send()

    for copy, goes, comes in corners:
        @pl.when(goes)
        def _():
            copy.wait_send()

    for copy in spread:
        copy.wait_send()


def store_kernel(rows, width, mesh_in, surface_in, norm_in, mesh_out, surface_out, norm_out, norm, sem):
    copies = []
    for s in range(SUB):
        cols = slice(s * width, (s + 1) * width)
        copies.append(pltpu.make_async_copy(mesh_in.at[:, :, s, :], mesh_out.at[:, :, cols], sem.at[s]))
        copies.append(pltpu.make_async_copy(surface_in.at[:, s, :], surface_out.at[:, cols], sem.at[SUB + s]))
    for copy in copies:
        copy.start()
    norm[...] = norm_in[0, :rows]
    last = pltpu.make_async_copy(norm, norm_out, sem.at[2 * SUB])
    last.start()
    copies.append(last)
    for copy in copies:
        copy.wait()


def solution(mesh):
    n_lat, n_depth = mesh.shape["lat"], mesh.shape["depth"]

    def per_device(surface, velocity, block_map, free_flags, block_rates, previous):
        rows, layers, columns = previous.shape
        width = columns // SUB
        f32 = jnp.float32

        def vmem(*shape, dtype=f32):
            return pltpu.VMEM(shape, dtype)

        def kernel(*refs):
            relax_kernel(rows, layers, width, n_lat, n_depth, *refs)

        hbm = pl.BlockSpec(memory_space=pl.ANY)
        inside = pl.BlockSpec(memory_space=pltpu.VMEM)
        dma = pltpu.SemaphoreType.DMA
        new_surface, field, norm = pl.pallas_call(
            kernel,
            out_shape=(
                jax.ShapeDtypeStruct((rows, SUB, width), f32),
                jax.ShapeDtypeStruct((rows, layers, SUB, width), f32),
                jax.ShapeDtypeStruct((1, 128), f32),
            ),
            in_specs=[hbm] * 6,
            out_specs=(inside, inside, inside),
            scratch_shapes=[
                vmem(rows + 4, layers, SUB, width),
                vmem(rows + 2, layers, SUB, width),
                vmem(rows + 2, 2, SUB, width),
                vmem(rows + 2, 2, SUB, width),
                vmem(rows + 6, SUB, width),
                vmem(2, rows + 4, SUB, width),
                vmem(rows + 4, SUB, width, dtype=jnp.int32),
                vmem(rows + 4, SUB, width, dtype=jnp.int32),
                pltpu.SMEM((16,), f32),
                vmem(rows + 4, SUB, width),
                vmem(rows + 2, SUB, width),
                vmem(rows, SUB, width),
                vmem(rows, SUB, 128),
                vmem(n_depth, rows, 128),
                dma((8 * SUB + 1,)),
                dma((CHUNKS,)), dma((CHUNKS,)), dma((CHUNKS,)), dma((CHUNKS,)),
                dma((2, 6)), dma((2, 6)),
                dma((4,)), dma((4,)),
                dma((n_depth - 1,)), dma((n_depth - 1,)),
                pltpu.SemaphoreType.REGULAR,
            ],
            compiler_params=pltpu.CompilerParams(
                collective_id=0, has_side_effects=True, vmem_limit_bytes=VMEM_LIMIT
            ),
            name="relax",
        )(*(
            pltpu.with_memory_space_constraint(value, pltpu.HBM)
            for value in (surface, velocity, block_map, free_flags, block_rates, previous)
        ))

        def store(*refs):
            store_kernel(rows, width, *refs)

        field, new_surface, norm = pl.pallas_call(
            store,
            out_shape=(
                jax.ShapeDtypeStruct(previous.shape, f32),
                jax.ShapeDtypeStruct(surface.shape, f32),
                jax.ShapeDtypeStruct((rows,), f32),
            ),
            in_specs=[inside, inside, inside],
            out_specs=(hbm, hbm, hbm),
            scratch_shapes=[vmem(rows), dma((2 * SUB + 1,))],
            compiler_params=pltpu.CompilerParams(vmem_limit_bytes=1024 * 1024),
            name="store",
        )(field, new_surface, norm)
        return new_surface, field, norm

    return jax.shard_map(
        per_device,
        mesh=mesh,
        in_specs=(
            P("lat", None), P(None, "lat", None), P("lat", None), P("lat", None), P(),
            P("lat", "depth", None),
        ),
        out_specs=(P("lat", None), P("lat", "depth", None), P("lat")),
        check_vma=False,
    )


VMEM_LIMIT = 40 * 1024 * 1024
```

```python
import jax
import jax.numpy as jnp
from jax import lax
from jax.experimental import pallas as pl
from jax.experimental.pallas import tpu as pltpu
from jax.sharding import PartitionSpec as P

MESH = pl.DeviceIdType.MESH
TIME_STEP = 0.5
RELAX_WEIGHT = 0.8
KEEP = 1.0 - RELAX_WEIGHT
SHARE = RELAX_WEIGHT / 6.0
CENTRE = KEEP / SHARE
SCALE = SHARE * SHARE
SUB = 8


def iotas(width):
    lane = lax.broadcasted_iota(jnp.int32, (SUB, 128), 1)
    sub = lax.broadcasted_iota(jnp.int32, (SUB, 128), 0)
    return lane, sub


def before(v, masks):
    width = v.shape[-1]
    rolled = pltpu.roll(v, 1, 1)
    first = rolled[:, :128]
    carried = pltpu.roll(first, 1, 0)
    first = jnp.where(masks[0], jnp.where(masks[1], 0.0, carried), first)
    return jnp.concatenate([first, rolled[:, 128:]], axis=1)


def after(v, masks):
    width = v.shape[-1]
    rolled = pltpu.roll(v, width - 1, 1)
    last = rolled[:, width - 128:]
    carried = pltpu.roll(last, SUB - 1, 0)
    last = jnp.where(masks[2], jnp.where(masks[3], 0.0, carried), last)
    return jnp.concatenate([rolled[:, : width - 128], last], axis=1)


def relax_kernel(
    rows, layers, width, n_lat, n_depth,
    surface, velocity, block_map, free_flags, block_rates, previous,
    new_surface, mesh_out, totals,
    prev, once, above, below, surf, vel, bmap, flags, rates,
    shift, wide, widest, squares,
    load_sem, up_send, up_recv, down_send, down_recv, side_send, side_recv,
    corner_send, corner_recv, sum_send, sum_recv, relay_sem,
):
    lat = lax.axis_index("lat")
    depth = lax.axis_index("depth")
    has_left, has_right = lat > 0, lat < n_lat - 1
    has_up, has_down = depth > 0, depth < n_depth - 1
    left, right = {"lat": lat - 1}, {"lat": lat + 1}
    up, down = {"depth": depth - 1}, {"depth": depth + 1}

    barrier = pltpu.get_barrier_semaphore()
    around = ((has_up, up), (has_down, down), (has_left, left), (has_right, right))
    for have, target in around:
        @pl.when(have)
        def _():
            pl.semaphore_signal(barrier, inc=1, device_id=target, device_id_type=MESH)

    count = 0
    groups = {}

    def load(name, pairs):
        nonlocal count
        copies = []
        for src, dst in pairs:
            copy = pltpu.make_async_copy(src, dst, load_sem.at[count])
            copy.start()
            copies.append(copy)
            count += 1
        groups[name] = copies

    def loaded(name):
        for copy in groups[name]:
            copy.wait()

    pieces = [(0, 1), (rows - 1, rows)] + [(r, r + 2) for r in range(1, rows - 3, 2)]
    pieces += [(rows - 3, rows - 2), (rows - 2, rows - 1)]

    cols = [slice(s * width, (s + 1) * width) for s in range(SUB)]
    own = slice(2, 2 + rows)
    load("outer", [
        (previous.at[:, part, cols[s]], prev.at[own, part, s, :])
        for part in (slice(layers - 2, layers), slice(0, 2)) for s in range(SUB)
    ])
    load("surface",
         [(surface.at[:, cols[s]], surf.at[slice(3, 3 + rows), s, :]) for s in range(SUB)]
         + [(velocity.at[:, :, cols[s]], vel.at[:, own, s, :]) for s in range(SUB)]
         + [(block_map.at[:, cols[s]], bmap.at[own, s, :]) for s in range(SUB)]
         + [(free_flags.at[:, cols[s]], flags.at[own, s, :]) for s in range(SUB)]
         + [(block_rates, rates)])
    load("inner", [
        (previous.at[:, part, cols[s]], prev.at[own, part, s, :])
        for part in (slice(2, SUB), slice(layers - SUB, layers - 2)) for s in range(SUB)
    ])

    def clear(ref):
        ref[...] = jnp.zeros(ref.shape, ref.dtype)

    @pl.when(jnp.logical_not(has_up))
    def _():
        clear(above)

    @pl.when(jnp.logical_not(has_down))
    def _():
        clear(below)

    for have, near, far, at in (
        (has_left, slice(0, 2), slice(0, 3), 0),
        (has_right, slice(rows + 2, rows + 4), slice(rows + 3, rows + 6), rows + 1),
    ):
        @pl.when(jnp.logical_not(have))
        def _():
            clear(prev.at[near])
            clear(surf.at[far])
            clear(vel.at[:, near])
            clear(bmap.at[near])
            clear(flags.at[near])
            clear(above.at[at])
            clear(below.at[at])
            clear(once.at[at])

    pl.semaphore_wait(barrier, sum(have.astype(jnp.int32) for have, _ in around))

    def remote(src, dst, send, recv, target):
        return pltpu.make_async_remote_copy(
            src_ref=src, dst_ref=dst, send_sem=send, recv_sem=recv,
            device_id=target, device_id_type=MESH,
        )

    last_two, first_two = slice(layers - 2, layers), slice(0, 2)
    to_down, to_up = [], []
    for c, (first, last) in enumerate(pieces):
        mine, theirs = slice(2 + first, 2 + last), slice(1 + first, 1 + last)
        to_down.append(remote(prev.at[mine, last_two], above.at[theirs], down_send.at[c], down_recv.at[c], down))
        to_up.append(remote(prev.at[mine, first_two], below.at[theirs], up_send.at[c], up_recv.at[c], up))

    loaded("outer")

    @pl.when(has_down)
    def _():
        for copy in to_down:
            copy.start()

    @pl.when(has_up)
    def _():
        for copy in to_up:
            copy.start()

    def sides(mine3, theirs3, mine2, theirs2, near, far, row, target):
        return [
            remote(surf.at[mine3], surf.at[theirs3], side_send.at[row, 0], side_recv.at[row, 0], target),
            remote(vel.at[:, mine2], vel.at[:, theirs2], side_send.at[row, 1], side_recv.at[row, 1], target),
            remote(bmap.at[mine2], bmap.at[theirs2], side_send.at[row, 2], side_recv.at[row, 2], target),
            remote(flags.at[mine2], flags.at[theirs2], side_send.at[row, 3], side_recv.at[row, 3], target),
            remote(prev.at[near[0]], prev.at[near[1]], side_send.at[row, 4], side_recv.at[row, 4], target),
            remote(prev.at[far[0]], prev.at[far[1]], side_send.at[row, 5], side_recv.at[row, 5], target),
        ]

    to_right = sides(slice(rows, rows + 3), slice(0, 3), slice(rows, rows + 2), slice(0, 2),
                     (rows + 1, 1), (rows, 0), 0, right)
    to_left = sides(slice(3, 6), slice(rows + 3, rows + 6), slice(2, 4), slice(rows + 2, rows + 4),
                    (2, rows + 2), (3, rows + 3), 1, left)

    loaded("surface")

    @pl.when(has_right)
    def _():
        for copy in to_right[:4]:
            copy.start()

    @pl.when(has_left)
    def _():
        for copy in to_left[:4]:
            copy.start()

    loaded("inner")

    @pl.when(has_right)
    def _():
        for copy in to_right[4:]:
            copy.start()

    @pl.when(has_left)
    def _():
        for copy in to_left[4:]:
            copy.start()

    lane, sub = iotas(width)
    masks = (lane == 0, sub == 0, lane == 127, sub == SUB - 1)

    def neighbours(v):
        return before(v, masks) + after(v, masks)

    def sweep_once(i, carry):
        here = prev[i + 1, 0]
        earlier = None
        for z in range(layers):
            later = prev[i + 1, z + 1] if z < layers - 1 else None
            total = CENTRE * here + (prev[i, z] + prev[i + 2, z]) + neighbours(here)
            if earlier is not None:
                total = total + earlier
            if later is not None:
                total = total + later
            once[i, z] = total
            earlier, here = here, later
        return carry

    lax.fori_loop(2, rows, sweep_once, 0)

    rate = [rates[k] for k in range(16)]

    def lookup(index):
        level = rate
        for bit in range(4):
            odd = (index & (1 << bit)) != 0
            level = [jnp.where(odd, level[2 * k + 1], level[2 * k]) for k in range(len(level) // 2)]
        return level[0]

    def advect(i, store):
        low, middle, high = surf[i], surf[i + 1], surf[i + 2]
        west, east = before(middle, masks), after(middle, masks)
        grad_rows = (high - low) * 0.5
        grad_cols = (east - west) * 0.5
        laplace = high + low + east + west - 4.0 * middle
        tendency = -vel[0, i] * grad_rows - vel[1, i] * grad_cols + lookup(bmap[i]) * laplace
        new = middle + TIME_STEP * flags[i].astype(jnp.float32) * tendency
        if store:
            new_surface[i - 2] = new
        shift[i] = new - middle

    def widen(src, dst, i):
        here = src[i + 1]
        dst[i] = (CENTRE + 2.0) * here + (src[i] + src[i + 2]) + neighbours(here)

    all_layers = layers * n_depth
    profile = [
        (all_layers - (depth * layers + z)).astype(jnp.float32) / all_layers * SCALE for z in range(layers)
    ]
    zero = jnp.float32(0.0)
    top = jnp.where(has_up, zero, jnp.float32(SCALE))
    upper = jnp.where(has_up, jnp.float32(SCALE), zero)
    lower = jnp.where(has_down, jnp.float32(SCALE), zero)

    def narrow(v):
        return sum(v[:, k * 128:(k + 1) * 128] for k in range(width // 128))

    def sweep_twice(i, carry):
        here = once[i + 1, 0]
        earlier = None
        part = widest[i]
        acc = None
        for z in range(layers):
            later = once[i + 1, z + 1] if z < layers - 1 else None
            total = CENTRE * here + (once[i, z] + once[i + 2, z]) + neighbours(here)
            if earlier is not None:
                total = total + earlier
            if later is not None:
                total = total + later
            total = SCALE * total + profile[z] * part
            if z == 0:
                total = total + upper * prev[i + 2, 0] + top * (
                    (1.0 / SHARE + 2.0 / all_layers) * shift[i + 2]
                    - (1.0 + 2.0 / all_layers) * wide[i + 1])
            elif z == 1:
                total = total - (top * (1.0 / all_layers)) * shift[i + 2]
            elif z == layers - 1:
                total = total + lower * prev[i + 2, layers - 1]
            elif z < layers - 2:
                acc = total * total if acc is None else acc + total * total
            mesh_out[i, z] = total
            earlier, here = here, later
        squares[i] = narrow(acc)
        return carry

    def arrived(chunk):
        @pl.when(has_up)
        def _():
            to_down[chunk].wait_recv()

        @pl.when(has_down)
        def _():
            to_up[chunk].wait_recv()

    arrived(0)
    arrived(1)
    corners = []
    for number, (ref, near, depth_from) in enumerate(((above, 1, has_up), (below, 0, has_down))):
        for side, (src, dst, goes, comes, target) in enumerate((
            (rows, 0, has_right, has_left, right),
            (1, rows + 1, has_left, has_right, left),
        )):
            copy = remote(
                ref.at[src, near], ref.at[dst, near],
                corner_send.at[2 * number + side], corner_recv.at[2 * number + side], target)
            goes, comes = jnp.logical_and(goes, depth_from), jnp.logical_and(comes, depth_from)
            corners.append((copy, goes, comes))

            @pl.when(goes)
            def _():
                copy.start()

    def grouped(first, last, size, what):
        def some(g, carry):
            for k in range(size):
                what(first + g * size + k)
            return carry

        count = (last - first) // size
        if count:
            lax.fori_loop(0, count, some, 0)
        for i in range(first + count * size, last):
            what(i)

    grouped(3, rows + 1, 5, lambda i: advect(i, True))
    grouped(3, rows - 1, 5, lambda i: widen(shift, wide, i))
    grouped(3, rows - 3, 5, lambda i: widen(wide, widest, i))
    lax.fori_loop(3, rows - 3, sweep_twice, 0)

    @pl.when(has_left)
    def _():
        for copy in to_right[:4]:
            copy.wait_recv()

    @pl.when(has_right)
    def _():
        for copy in to_left[:4]:
            copy.wait_recv()

    for i in (0, 1, rows + 2, rows + 3):
        advect(i, False)
    for i in (2, rows + 1):
        advect(i, True)
    for i in (0, 1, 2, rows - 1, rows, rows + 1):
        widen(shift, wide, i)

    @pl.when(jnp.logical_not(has_left))
    def _():
        clear(wide.at[0])

    @pl.when(jnp.logical_not(has_right))
    def _():
        clear(wide.at[rows + 1])

    for i in (0, 1, 2, rows - 3, rows - 2, rows - 1):
        widen(wide, widest, i)

    @pl.when(has_left)
    def _():
        to_right[4].wait_recv()

    @pl.when(has_right)
    def _():
        to_left[4].wait_recv()

    def one_each_side(k, carry):
        sweep_once(1 + k * (rows - 1), 0)
        return carry

    def second_rows(k, carry):
        sweep_twice(lax.select(k < 2, k + 1, rows - 5 + k), 0)
        return carry

    lax.fori_loop(0, 2, one_each_side, 0)
    lax.fori_loop(0, 4, second_rows, 0)

    def finish(first, last):
        parts, values = {}, []
        for i in range(first, last):
            acc = None
            for ref, near, far, outer, inner in ((above, 1, 0, 0, 1), (below, 0, 1, layers - 1, layers - 2)):
                here = ref[i + 1, near]
                around = ref[i, near] + ref[i + 2, near] + neighbours(here)
                edge = mesh_out[i, outer] + SCALE * (2.0 * CENTRE * here + 2.0 * around + ref[i + 1, far])
                next_in = mesh_out[i, inner] + SCALE * here
                values += [(i, outer, edge), (i, inner, next_in)]
                both = edge * edge + next_in * next_in
                acc = both if acc is None else acc + both
            parts[i] = squares[i] + narrow(acc)
        for i, z, value in values:
            mesh_out[i, z] = value
        for i, value in parts.items():
            squares[i] = value

    early = 7
    for c in range(2, early):
        arrived(c)

    for have, target in ((has_up, up), (has_down, down)):
        @pl.when(have)
        def _():
            pl.semaphore_signal(relay_sem, inc=1, device_id=target, device_id_type=MESH)

    middle = pieces[early - 1][1] - 1
    for first in range(3, middle, 4):
        finish(first, min(first + 4, middle))

    @pl.when(has_left)
    def _():
        to_right[5].wait_recv()
        sweep_once(0, 0)

    @pl.when(has_right)
    def _():
        to_left[5].wait_recv()
        sweep_once(rows + 1, 0)

    def edge_rows(k, carry):
        sweep_twice(k * (rows - 1), 0)
        return carry

    lax.fori_loop(0, 2, edge_rows, 0)

    for copy, goes, comes in corners:
        @pl.when(comes)
        def _():
            copy.wait_recv()

    finish(0, 3)
    done = middle
    for c in range(early, len(pieces)):
        arrived(c)
        ready = rows if c == len(pieces) - 1 else pieces[c][1] - 1
        finish(done, ready)
        done = ready

    pl.semaphore_wait(relay_sem, has_up.astype(jnp.int32) + has_down.astype(jnp.int32))
    totals[depth] = jnp.sum(squares[...], axis=1)
    spread = []
    for k in range(1, n_depth):
        target = lax.rem(depth + k, n_depth)
        copy = remote(totals.at[depth], totals.at[depth], sum_send.at[k - 1], sum_recv.at[k - 1], {"depth": target})
        copy.start()
        spread.append(copy)
    for copy in spread:
        copy.wait_recv()

    @pl.when(has_down)
    def _():
        for copy in to_down:
            copy.wait_send()

    @pl.when(has_up)
    def _():
        for copy in to_up:
            copy.wait_send()

    @pl.when(has_right)
    def _():
        for copy in to_right:
            copy.wait_send()

    @pl.when(has_left)
    def _():
        for copy in to_left:
            copy.wait_send()

    for copy, goes, comes in corners:
        @pl.when(goes)
        def _():
            copy.wait_send()

    for copy in spread:
        copy.wait_send()


def store_kernel(rows, width, mesh_in, surface_in, totals, mesh_out, surface_out, norm_out, norm, sem):
    copies = []
    for s in range(SUB):
        cols = slice(s * width, (s + 1) * width)
        copies.append(pltpu.make_async_copy(mesh_in.at[:, :, s, :], mesh_out.at[:, :, cols], sem.at[s]))
        copies.append(pltpu.make_async_copy(surface_in.at[:, s, :], surface_out.at[:, cols], sem.at[SUB + s]))
    for copy in copies:
        copy.start()
    total = totals[0]
    for k in range(1, totals.shape[0]):
        total = total + totals[k]
    nodes = mesh_in.shape[1] * totals.shape[0] * SUB * width
    root = jnp.sqrt(jnp.sum(total, axis=1, keepdims=True) / nodes)
    spot = lax.broadcasted_iota(jnp.int32, (rows, 128), 0) == lax.broadcasted_iota(jnp.int32, (rows, 128), 1)
    norm[...] = jnp.sum(jnp.where(spot, root, 0.0), axis=0)[:rows]
    last = pltpu.make_async_copy(norm, norm_out, sem.at[2 * SUB])
    last.start()
    copies.append(last)
    for copy in copies:
        copy.wait()


def solution(mesh):
    n_lat, n_depth = mesh.shape["lat"], mesh.shape["depth"]

    def per_device(surface, velocity, block_map, free_flags, block_rates, previous):
        rows, layers, columns = previous.shape
        width = columns // SUB
        f32 = jnp.float32

        def vmem(*shape, dtype=f32):
            return pltpu.VMEM(shape, dtype)

        def kernel(*refs):
            relax_kernel(rows, layers, width, n_lat, n_depth, *refs)

        hbm = pl.BlockSpec(memory_space=pl.ANY)
        inside = pl.BlockSpec(memory_space=pltpu.VMEM)
        dma = pltpu.SemaphoreType.DMA
        new_surface, field, norm = pl.pallas_call(
            kernel,
            out_shape=(
                jax.ShapeDtypeStruct((rows, SUB, width), f32),
                jax.ShapeDtypeStruct((rows, layers, SUB, width), f32),
                jax.ShapeDtypeStruct((n_depth, rows, 128), f32),
            ),
            in_specs=[hbm] * 6,
            out_specs=(inside, inside, inside),
            scratch_shapes=[
                vmem(rows + 4, layers, SUB, width),
                vmem(rows + 2, layers, SUB, width),
                vmem(rows + 2, 2, SUB, width),
                vmem(rows + 2, 2, SUB, width),
                vmem(rows + 6, SUB, width),
                vmem(2, rows + 4, SUB, width),
                vmem(rows + 4, SUB, width, dtype=jnp.int32),
                vmem(rows + 4, SUB, width, dtype=jnp.int32),
                pltpu.SMEM((16,), f32),
                vmem(rows + 4, SUB, width),
                vmem(rows + 2, SUB, width),
                vmem(rows, SUB, width),
                vmem(rows, SUB, 128),
                dma((8 * SUB + 1,)),
                dma((rows,)), dma((rows,)), dma((rows,)), dma((rows,)),
                dma((2, 6)), dma((2, 6)),
                dma((4,)), dma((4,)),
                dma((n_depth - 1,)), dma((n_depth - 1,)),
                pltpu.SemaphoreType.REGULAR,
            ],
            compiler_params=pltpu.CompilerParams(
                collective_id=0, has_side_effects=True, vmem_limit_bytes=VMEM_LIMIT
            ),
            name="relax",
        )(*(
            pltpu.with_memory_space_constraint(value, pltpu.HBM)
            for value in (surface, velocity, block_map, free_flags, block_rates, previous)
        ))

        def store(*refs):
            store_kernel(rows, width, *refs)

        field, new_surface, norm = pl.pallas_call(
            store,
            out_shape=(
                jax.ShapeDtypeStruct(previous.shape, f32),
                jax.ShapeDtypeStruct(surface.shape, f32),
                jax.ShapeDtypeStruct((rows,), f32),
            ),
            in_specs=[inside, inside, inside],
            out_specs=(hbm, hbm, hbm),
            scratch_shapes=[vmem(rows), dma((2 * SUB + 1,))],
            compiler_params=pltpu.CompilerParams(vmem_limit_bytes=1024 * 1024),
            name="store",
        )(field, new_surface, norm)
        return new_surface, field, norm

    return jax.shard_map(
        per_device,
        mesh=mesh,
        in_specs=(
            P("lat", None), P(None, "lat", None), P("lat", None), P("lat", None), P(),
            P("lat", "depth", None),
        ),
        out_specs=(P("lat", None), P("lat", "depth", None), P("lat")),
        check_vma=False,
    )


VMEM_LIMIT = 40 * 1024 * 1024
```

```python
import jax
import jax.numpy as jnp
from jax import lax
from jax.experimental import pallas as pl
from jax.experimental.pallas import tpu as pltpu
from jax.sharding import PartitionSpec as P

MESH = pl.DeviceIdType.MESH
TIME_STEP = 0.5
RELAX_WEIGHT = 0.8
KEEP = 1.0 - RELAX_WEIGHT
SHARE = RELAX_WEIGHT / 6.0
CENTRE = KEEP / SHARE
SCALE = SHARE * SHARE
SUB = 8


def iotas(width):
    lane = lax.broadcasted_iota(jnp.int32, (SUB, 128), 1)
    sub = lax.broadcasted_iota(jnp.int32, (SUB, 128), 0)
    return lane, sub


def before(v, masks):
    width = v.shape[-1]
    rolled = pltpu.roll(v, 1, 1)
    first = rolled[:, :128]
    carried = pltpu.roll(first, 1, 0)
    first = jnp.where(masks[0], jnp.where(masks[1], 0.0, carried), first)
    return jnp.concatenate([first, rolled[:, 128:]], axis=1)


def after(v, masks):
    width = v.shape[-1]
    rolled = pltpu.roll(v, width - 1, 1)
    last = rolled[:, width - 128:]
    carried = pltpu.roll(last, SUB - 1, 0)
    last = jnp.where(masks[2], jnp.where(masks[3], 0.0, carried), last)
    return jnp.concatenate([rolled[:, : width - 128], last], axis=1)


def relax_kernel(
    rows, layers, width, n_lat, n_depth,
    surface, velocity, block_map, free_flags, block_rates, previous,
    new_surface, mesh_out, totals,
    prev, once, above, below, surf, vel, bmap, flags, rates,
    shift, wide, widest, squares,
    load_sem, z_send, up_recv, down_recv, side_send, side_recv,
    corner_send, corner_recv, sum_sem, relay_sem,
):
    lat = lax.axis_index("lat")
    depth = lax.axis_index("depth")
    has_left, has_right = lat > 0, lat < n_lat - 1
    has_up, has_down = depth > 0, depth < n_depth - 1
    left, right = {"lat": lat - 1}, {"lat": lat + 1}
    up, down = {"depth": depth - 1}, {"depth": depth + 1}

    barrier = pltpu.get_barrier_semaphore()
    around = ((has_up, up), (has_down, down), (has_left, left), (has_right, right))
    for have, target in around:
        @pl.when(have)
        def _():
            pl.semaphore_signal(barrier, inc=1, device_id=target, device_id_type=MESH)

    def settled(ref, sem):
        pltpu.make_async_copy(ref, ref, sem).wait()

    def load(sem, pairs):
        for src, dst in pairs:
            pltpu.make_async_copy(src, dst, sem).start()

    pieces = [
        (0, 1, 0), (rows - 1, rows, 0), (1, rows - 5, 1), (rows - 5, rows - 3, 2),
        (rows - 3, rows - 2, 3), (rows - 2, rows - 1, 4),
    ]

    cols = [slice(s * width, (s + 1) * width) for s in range(SUB)]
    own = slice(2, 2 + rows)
    load(load_sem.at[0], [
        (previous.at[:, part, cols[s]], prev.at[own, part, s, :])
        for part in (slice(layers - 2, layers), slice(0, 2)) for s in range(SUB)
    ])
    load(load_sem.at[1],
         [(surface.at[:, cols[s]], surf.at[slice(3, 3 + rows), s, :]) for s in range(SUB)]
         + [(velocity.at[:, :, cols[s]], vel.at[:, own, s, :]) for s in range(SUB)]
         + [(block_map.at[:, cols[s]], bmap.at[own, s, :]) for s in range(SUB)]
         + [(free_flags.at[:, cols[s]], flags.at[own, s, :]) for s in range(SUB)])
    load(load_sem.at[2], [
        (previous.at[:, part, cols[s]], prev.at[own, part, s, :])
        for part in (slice(2, SUB), slice(layers - SUB, layers - 2)) for s in range(SUB)
    ])
    rates_copy = pltpu.make_async_copy(block_rates, rates, load_sem.at[3])
    rates_copy.start()

    def clear(ref):
        ref[...] = jnp.zeros(ref.shape, ref.dtype)

    @pl.when(jnp.logical_not(has_up))
    def _():
        clear(above)

    @pl.when(jnp.logical_not(has_down))
    def _():
        clear(below)

    for have, near, far, at in (
        (has_left, slice(0, 2), slice(0, 3), 0),
        (has_right, slice(rows + 2, rows + 4), slice(rows + 3, rows + 6), rows + 1),
    ):
        @pl.when(jnp.logical_not(have))
        def _():
            clear(prev.at[near])
            clear(surf.at[far])
            clear(vel.at[:, near])
            clear(bmap.at[near])
            clear(flags.at[near])
            clear(above.at[at])
            clear(below.at[at])
            clear(once.at[at])

    pl.semaphore_wait(barrier, sum(have.astype(jnp.int32) for have, _ in around))

    def remote(src, dst, send, recv, target):
        return pltpu.make_async_remote_copy(
            src_ref=src, dst_ref=dst, send_sem=send, recv_sem=recv,
            device_id=target, device_id_type=MESH,
        )

    last_two, first_two = slice(layers - 2, layers), slice(0, 2)
    to_down, to_up = [], []
    for first, last, c in pieces:
        mine, theirs = slice(2 + first, 2 + last), slice(1 + first, 1 + last)
        to_down.append(remote(prev.at[mine, last_two], above.at[theirs], z_send.at[0], down_recv.at[c], down))
        to_up.append(remote(prev.at[mine, first_two], below.at[theirs], z_send.at[1], up_recv.at[c], up))

    settled(prev.at[own, slice(0, 4)], load_sem.at[0])

    @pl.when(has_down)
    def _():
        for copy in to_down:
            copy.start()

    @pl.when(has_up)
    def _():
        for copy in to_up:
            copy.start()

    def sides(mine3, theirs3, mine2, theirs2, near, far, row, target):
        return [
            remote(surf.at[mine3], surf.at[theirs3], side_send.at[row, 0], side_recv.at[row, 0], target),
            remote(vel.at[:, mine2], vel.at[:, theirs2], side_send.at[row, 0], side_recv.at[row, 0], target),
            remote(bmap.at[mine2], bmap.at[theirs2], side_send.at[row, 0], side_recv.at[row, 0], target),
            remote(flags.at[mine2], flags.at[theirs2], side_send.at[row, 0], side_recv.at[row, 0], target),
            remote(prev.at[near[0]], prev.at[near[1]], side_send.at[row, 1], side_recv.at[row, 1], target),
            remote(prev.at[far[0]], prev.at[far[1]], side_send.at[row, 1], side_recv.at[row, 2], target),
        ]

    edge_bytes = surf.at[slice(0, 3 + 4 * 2)]

    to_right = sides(slice(rows, rows + 3), slice(0, 3), slice(rows, rows + 2), slice(0, 2),
                     (rows + 1, 1), (rows, 0), 0, right)
    to_left = sides(slice(3, 6), slice(rows + 3, rows + 6), slice(2, 4), slice(rows + 2, rows + 4),
                    (2, rows + 2), (3, rows + 3), 1, left)

    settled(prev.at[own, slice(0, 5)], load_sem.at[1])
    rates_copy.wait()

    @pl.when(has_right)
    def _():
        for copy in to_right[:4]:
            copy.start()

    @pl.when(has_left)
    def _():
        for copy in to_left[:4]:
            copy.start()

    settled(prev.at[own, slice(2, layers - 2)], load_sem.at[2])

    @pl.when(has_right)
    def _():
        for copy in to_right[4:]:
            copy.start()

    @pl.when(has_left)
    def _():
        for copy in to_left[4:]:
            copy.start()

    lane, sub = iotas(width)
    masks = (lane == 0, sub == 0, lane == 127, sub == SUB - 1)

    def neighbours(v):
        return before(v, masks) + after(v, masks)

    def sweep_once(i, carry):
        here = prev[i + 1, 0]
        earlier = None
        for z in range(layers):
            later = prev[i + 1, z + 1] if z < layers - 1 else None
            total = CENTRE * here + (prev[i, z] + prev[i + 2, z]) + neighbours(here)
            if earlier is not None:
                total = total + earlier
            if later is not None:
                total = total + later
            once[i, z] = total
            earlier, here = here, later
        return carry

    lax.fori_loop(2, rows, sweep_once, 0)

    rate = [rates[k] for k in range(16)]

    def lookup(index):
        level = rate
        for bit in range(4):
            odd = (index & (1 << bit)) != 0
            level = [jnp.where(odd, level[2 * k + 1], level[2 * k]) for k in range(len(level) // 2)]
        return level[0]

    def advect(i, store):
        low, middle, high = surf[i], surf[i + 1], surf[i + 2]
        west, east = before(middle, masks), after(middle, masks)
        grad_rows = (high - low) * 0.5
        grad_cols = (east - west) * 0.5
        laplace = high + low + east + west - 4.0 * middle
        tendency = -vel[0, i] * grad_rows - vel[1, i] * grad_cols + lookup(bmap[i]) * laplace
        new = middle + TIME_STEP * flags[i].astype(jnp.float32) * tendency
        if store:
            new_surface[i - 2] = new
        shift[i] = new - middle

    def widen(src, dst, i):
        here = src[i + 1]
        dst[i] = (CENTRE + 2.0) * here + (src[i] + src[i + 2]) + neighbours(here)

    all_layers = layers * n_depth
    profile = [
        (all_layers - (depth * layers + z)).astype(jnp.float32) / all_layers * SCALE for z in range(layers)
    ]
    zero = jnp.float32(0.0)
    top = jnp.where(has_up, zero, jnp.float32(SCALE))
    upper = jnp.where(has_up, jnp.float32(SCALE), zero)
    lower = jnp.where(has_down, jnp.float32(SCALE), zero)

    def narrow(v):
        return sum(v[:, k * 128:(k + 1) * 128] for k in range(width // 128))

    def sweep_twice(i, carry):
        here = once[i + 1, 0]
        earlier = None
        part = widest[i]
        acc = None
        for z in range(layers):
            later = once[i + 1, z + 1] if z < layers - 1 else None
            total = CENTRE * here + (once[i, z] + once[i + 2, z]) + neighbours(here)
            if earlier is not None:
                total = total + earlier
            if later is not None:
                total = total + later
            total = SCALE * total + profile[z] * part
            if z == 0:
                total = total + upper * prev[i + 2, 0] + top * (
                    (1.0 / SHARE + 2.0 / all_layers) * shift[i + 2]
                    - (1.0 + 2.0 / all_layers) * wide[i + 1])
            elif z == 1:
                total = total - (top * (1.0 / all_layers)) * shift[i + 2]
            elif z == layers - 1:
                total = total + lower * prev[i + 2, layers - 1]
            elif z < layers - 2:
                acc = total * total if acc is None else acc + total * total
            mesh_out[i, z] = total
            earlier, here = here, later
        squares[i] = narrow(acc)
        return carry

    def arrived(c):
        size = sum(last - first for first, last, sem in pieces if sem == c)

        @pl.when(has_up)
        def _():
            settled(above.at[slice(0, size)], down_recv.at[c])

        @pl.when(has_down)
        def _():
            settled(below.at[slice(0, size)], up_recv.at[c])

    arrived(0)
    corners = []
    for number, (ref, near, depth_from) in enumerate(((above, 1, has_up), (below, 0, has_down))):
        for side, (src, dst, goes, comes, target) in enumerate((
            (rows, 0, has_right, has_left, right),
            (1, rows + 1, has_left, has_right, left),
        )):
            copy = remote(
                ref.at[src, near], ref.at[dst, near],
                corner_send.at[2 * number + side], corner_recv.at[2 * number + side], target)
            goes, comes = jnp.logical_and(goes, depth_from), jnp.logical_and(comes, depth_from)
            corners.append((copy, goes, comes))

            @pl.when(goes)
            def _():
                copy.start()

    def grouped(first, last, size, what):
        def some(g, carry):
            for k in range(size):
                what(first + g * size + k)
            return carry

        count = (last - first) // size
        if count:
            lax.fori_loop(0, count, some, 0)
        for i in range(first + count * size, last):
            what(i)

    grouped(3, rows + 1, 5, lambda i: advect(i, True))
    grouped(3, rows - 1, 5, lambda i: widen(shift, wide, i))
    grouped(3, rows - 3, 5, lambda i: widen(wide, widest, i))
    lax.fori_loop(3, rows - 3, sweep_twice, 0)

    @pl.when(has_left)
    def _():
        settled(edge_bytes, side_recv.at[0, 0])

    @pl.when(has_right)
    def _():
        settled(edge_bytes, side_recv.at[1, 0])

    for i in (0, 1, rows + 2, rows + 3):
        advect(i, False)
    for i in (2, rows + 1):
        advect(i, True)
    for i in (0, 1, 2, rows - 1, rows, rows + 1):
        widen(shift, wide, i)

    @pl.when(jnp.logical_not(has_left))
    def _():
        clear(wide.at[0])

    @pl.when(jnp.logical_not(has_right))
    def _():
        clear(wide.at[rows + 1])

    for i in (0, 1, 2, rows - 3, rows - 2, rows - 1):
        widen(wide, widest, i)

    @pl.when(has_left)
    def _():
        to_right[4].wait_recv()

    @pl.when(has_right)
    def _():
        to_left[4].wait_recv()

    def one_each_side(k, carry):
        sweep_once(1 + k * (rows - 1), 0)
        return carry

    def second_rows(k, carry):
        sweep_twice(lax.select(k < 2, k + 1, rows - 5 + k), 0)
        return carry

    lax.fori_loop(0, 2, one_each_side, 0)
    lax.fori_loop(0, 4, second_rows, 0)

    def finish(first, last):
        parts, values = {}, []
        for i in range(first, last):
            acc = None
            for ref, near, far, outer, inner in ((above, 1, 0, 0, 1), (below, 0, 1, layers - 1, layers - 2)):
                here = ref[i + 1, near]
                around = ref[i, near] + ref[i + 2, near] + neighbours(here)
                edge = mesh_out[i, outer] + SCALE * (2.0 * CENTRE * here + 2.0 * around + ref[i + 1, far])
                next_in = mesh_out[i, inner] + SCALE * here
                values += [(i, outer, edge), (i, inner, next_in)]
                both = edge * edge + next_in * next_in
                acc = both if acc is None else acc + both
            parts[i] = squares[i] + narrow(acc)
        for i, z, value in values:
            mesh_out[i, z] = value
        for i, value in parts.items():
            squares[i] = value

    arrived(1)

    for have, target in ((has_up, up), (has_down, down)):
        @pl.when(have)
        def _():
            pl.semaphore_signal(relay_sem, inc=1, device_id=target, device_id_type=MESH)

    middle = rows - 6
    for first in range(3, middle, 4):
        finish(first, min(first + 4, middle))

    @pl.when(has_left)
    def _():
        to_right[5].wait_recv()
        sweep_once(0, 0)

    @pl.when(has_right)
    def _():
        to_left[5].wait_recv()
        sweep_once(rows + 1, 0)

    def edge_rows(k, carry):
        sweep_twice(k * (rows - 1), 0)
        return carry

    lax.fori_loop(0, 2, edge_rows, 0)

    for copy, goes, comes in corners:
        @pl.when(comes)
        def _():
            copy.wait_recv()

    finish(0, 3)
    done = middle
    for c, ready in ((2, rows - 4), (3, rows - 3), (4, rows)):
        arrived(c)
        finish(done, ready)
        done = ready

    pl.semaphore_wait(relay_sem, has_up.astype(jnp.int32) + has_down.astype(jnp.int32))
    totals[depth] = jnp.sum(squares[...], axis=1)
    for k in range(1, n_depth):
        target = lax.rem(depth + k, n_depth)
        copy = remote(totals.at[depth], totals.at[depth], sum_sem.at[0], sum_sem.at[1], {"depth": target})
        copy.start()
    everyone_else = totals.at[slice(0, n_depth - 1)]
    settled(everyone_else, sum_sem.at[1])

    for have, sem in ((has_down, z_send.at[0]), (has_up, z_send.at[1])):
        @pl.when(have)
        def _():
            settled(prev.at[own, slice(0, 2)], sem)

    for have, row in ((has_right, 0), (has_left, 1)):
        @pl.when(have)
        def _():
            settled(edge_bytes, side_send.at[row, 0])
            settled(prev.at[slice(0, 2)], side_send.at[row, 1])

    for copy, goes, comes in corners:
        @pl.when(goes)
        def _():
            copy.wait_send()

    settled(everyone_else, sum_sem.at[0])


def store_kernel(rows, width, mesh_in, surface_in, totals, mesh_out, surface_out, norm_out, norm, sem):
    copies = []
    for s in range(SUB):
        cols = slice(s * width, (s + 1) * width)
        copies.append(pltpu.make_async_copy(mesh_in.at[:, :, s, :], mesh_out.at[:, :, cols], sem.at[0]))
        copies.append(pltpu.make_async_copy(surface_in.at[:, s, :], surface_out.at[:, cols], sem.at[1]))
    for copy in copies:
        copy.start()
    total = totals[0]
    for k in range(1, totals.shape[0]):
        total = total + totals[k]
    nodes = mesh_in.shape[1] * totals.shape[0] * SUB * width
    root = jnp.sqrt(jnp.sum(total, axis=1, keepdims=True) / nodes)
    spot = lax.broadcasted_iota(jnp.int32, (rows, 128), 0) == lax.broadcasted_iota(jnp.int32, (rows, 128), 1)
    norm[...] = jnp.sum(jnp.where(spot, root, 0.0), axis=0)[:rows]
    last = pltpu.make_async_copy(norm, norm_out, sem.at[2])
    last.start()
    last.wait()
    for ref, k in ((mesh_in, 0), (surface_in, 1)):
        pltpu.make_async_copy(ref, ref, sem.at[k]).wait()


def solution(mesh):
    n_lat, n_depth = mesh.shape["lat"], mesh.shape["depth"]

    def per_device(surface, velocity, block_map, free_flags, block_rates, previous):
        rows, layers, columns = previous.shape
        width = columns // SUB
        f32 = jnp.float32

        def vmem(*shape, dtype=f32):
            return pltpu.VMEM(shape, dtype)

        def kernel(*refs):
            relax_kernel(rows, layers, width, n_lat, n_depth, *refs)

        hbm = pl.BlockSpec(memory_space=pl.ANY)
        inside = pl.BlockSpec(memory_space=pltpu.VMEM)
        dma = pltpu.SemaphoreType.DMA
        new_surface, field, norm = pl.pallas_call(
            kernel,
            out_shape=(
                jax.ShapeDtypeStruct((rows, SUB, width), f32),
                jax.ShapeDtypeStruct((rows, layers, SUB, width), f32),
                jax.ShapeDtypeStruct((n_depth, rows, 128), f32),
            ),
            in_specs=[hbm] * 6,
            out_specs=(inside, inside, inside),
            scratch_shapes=[
                vmem(rows + 4, layers, SUB, width),
                vmem(rows + 2, layers, SUB, width),
                vmem(rows + 2, 2, SUB, width),
                vmem(rows + 2, 2, SUB, width),
                vmem(rows + 6, SUB, width),
                vmem(2, rows + 4, SUB, width),
                vmem(rows + 4, SUB, width, dtype=jnp.int32),
                vmem(rows + 4, SUB, width, dtype=jnp.int32),
                pltpu.SMEM((16,), f32),
                vmem(rows + 4, SUB, width),
                vmem(rows + 2, SUB, width),
                vmem(rows, SUB, width),
                vmem(rows, SUB, 128),
                dma((4,)),
                dma((2,)), dma((5,)), dma((5,)),
                dma((2, 2)), dma((2, 3)),
                dma((4,)), dma((4,)),
                dma((2,)),
                pltpu.SemaphoreType.REGULAR,
            ],
            compiler_params=pltpu.CompilerParams(
                collective_id=0, has_side_effects=True, vmem_limit_bytes=VMEM_LIMIT
            ),
            name="relax",
        )(*(
            pltpu.with_memory_space_constraint(value, pltpu.HBM)
            for value in (surface, velocity, block_map, free_flags, block_rates, previous)
        ))

        def store(*refs):
            store_kernel(rows, width, *refs)

        field, new_surface, norm = pl.pallas_call(
            store,
            out_shape=(
                jax.ShapeDtypeStruct(previous.shape, f32),
                jax.ShapeDtypeStruct(surface.shape, f32),
                jax.ShapeDtypeStruct((rows,), f32),
            ),
            in_specs=[inside, inside, inside],
            out_specs=(hbm, hbm, hbm),
            scratch_shapes=[vmem(rows), dma((3,))],
            compiler_params=pltpu.CompilerParams(vmem_limit_bytes=1024 * 1024),
            name="store",
        )(field, new_surface, norm)
        return new_surface, field, norm

    return jax.shard_map(
        per_device,
        mesh=mesh,
        in_specs=(
            P("lat", None), P(None, "lat", None), P("lat", None), P("lat", None), P(),
            P("lat", "depth", None),
        ),
        out_specs=(P("lat", None), P("lat", "depth", None), P("lat")),
        check_vma=False,
    )


VMEM_LIMIT = 40 * 1024 * 1024
```

```python
import jax
import jax.numpy as jnp
from jax import lax
from jax.experimental import pallas as pl
from jax.experimental.pallas import tpu as pltpu
from jax.sharding import PartitionSpec as P

MESH = pl.DeviceIdType.MESH
TIME_STEP = 0.5
RELAX_WEIGHT = 0.8
KEEP = 1.0 - RELAX_WEIGHT
SHARE = RELAX_WEIGHT / 6.0
CENTRE = KEEP / SHARE
SCALE = SHARE * SHARE
SUB = 8
FIRST = 9


def iotas(width):
    lane = lax.broadcasted_iota(jnp.int32, (SUB, 128), 1)
    sub = lax.broadcasted_iota(jnp.int32, (SUB, 128), 0)
    return lane, sub


def before(v, masks):
    width = v.shape[-1]
    rolled = pltpu.roll(v, 1, 1)
    first = rolled[:, :128]
    carried = pltpu.roll(first, 1, 0)
    first = jnp.where(masks[0], jnp.where(masks[1], 0.0, carried), first)
    return jnp.concatenate([first, rolled[:, 128:]], axis=1)


def after(v, masks):
    width = v.shape[-1]
    rolled = pltpu.roll(v, width - 1, 1)
    last = rolled[:, width - 128:]
    carried = pltpu.roll(last, SUB - 1, 0)
    last = jnp.where(masks[2], jnp.where(masks[3], 0.0, carried), last)
    return jnp.concatenate([rolled[:, : width - 128], last], axis=1)


def relax_kernel(
    rows, layers, width, n_lat, n_depth,
    surface, velocity, block_map, free_flags, block_rates, previous,
    new_surface, mesh_out, totals,
    prev, once, above, below, surf, vel, bmap, flags, rates,
    shift, wide, widest, squares,
    load_sem, z_send, up_recv, down_recv, side_send, side_recv,
    corner_send, corner_recv, sum_sem, relay_sem,
):
    lat = lax.axis_index("lat")
    depth = lax.axis_index("depth")
    has_left, has_right = lat > 0, lat < n_lat - 1
    has_up, has_down = depth > 0, depth < n_depth - 1
    left, right = {"lat": lat - 1}, {"lat": lat + 1}
    up, down = {"depth": depth - 1}, {"depth": depth + 1}

    barrier = pltpu.get_barrier_semaphore()
    around = ((has_up, up), (has_down, down), (has_left, left), (has_right, right))
    for have, target in around:
        @pl.when(have)
        def _():
            pl.semaphore_signal(barrier, inc=1, device_id=target, device_id_type=MESH)

    def settled(ref, sem):
        pltpu.make_async_copy(ref, ref, sem).wait()

    def load(sem, pairs):
        for src, dst in pairs:
            pltpu.make_async_copy(src, dst, sem).start()

    pieces = [
        (0, 1, 0), (rows - 1, rows, 0), (1, FIRST, 1), (FIRST, rows - 4, 2),
        (rows - 4, rows - 2, 3), (rows - 2, rows - 1, 4),
    ]

    cols = [slice(s * width, (s + 1) * width) for s in range(SUB)]
    own = slice(2, 2 + rows)
    load(load_sem.at[0], [
        (previous.at[:, part, cols[s]], prev.at[own, part, s, :])
        for part in (slice(layers - 2, layers), slice(0, 2)) for s in range(SUB)
    ])
    load(load_sem.at[1],
         [(surface.at[:, cols[s]], surf.at[slice(3, 3 + rows), s, :]) for s in range(SUB)]
         + [(velocity.at[:, :, cols[s]], vel.at[:, own, s, :]) for s in range(SUB)]
         + [(block_map.at[:, cols[s]], bmap.at[own, s, :]) for s in range(SUB)]
         + [(free_flags.at[:, cols[s]], flags.at[own, s, :]) for s in range(SUB)])
    load(load_sem.at[2], [
        (previous.at[:, part, cols[s]], prev.at[own, part, s, :])
        for part in (slice(2, SUB), slice(layers - SUB, layers - 2)) for s in range(SUB)
    ])
    rates_copy = pltpu.make_async_copy(block_rates, rates, load_sem.at[3])
    rates_copy.start()

    def clear(ref):
        ref[...] = jnp.zeros(ref.shape, ref.dtype)

    @pl.when(jnp.logical_not(has_up))
    def _():
        clear(above)

    @pl.when(jnp.logical_not(has_down))
    def _():
        clear(below)

    for have, near, far, at in (
        (has_left, slice(0, 2), slice(0, 3), 0),
        (has_right, slice(rows + 2, rows + 4), slice(rows + 3, rows + 6), rows + 1),
    ):
        @pl.when(jnp.logical_not(have))
        def _():
            clear(prev.at[near])
            clear(surf.at[far])
            clear(vel.at[:, near])
            clear(bmap.at[near])
            clear(flags.at[near])
            clear(above.at[at])
            clear(below.at[at])
            clear(once.at[at])

    pl.semaphore_wait(barrier, sum(have.astype(jnp.int32) for have, _ in around))

    def remote(src, dst, send, recv, target):
        return pltpu.make_async_remote_copy(
            src_ref=src, dst_ref=dst, send_sem=send, recv_sem=recv,
            device_id=target, device_id_type=MESH,
        )

    last_two, first_two = slice(layers - 2, layers), slice(0, 2)
    to_down, to_up = [], []
    for first, last, c in pieces:
        mine, theirs = slice(2 + first, 2 + last), slice(1 + first, 1 + last)
        to_down.append(remote(prev.at[mine, last_two], above.at[theirs], z_send.at[0], down_recv.at[c], down))
        to_up.append(remote(prev.at[mine, first_two], below.at[theirs], z_send.at[1], up_recv.at[c], up))

    settled(prev.at[own, slice(0, 4)], load_sem.at[0])

    def send_layers(turn, part):
        @pl.when(jnp.logical_and(has_down, turn))
        def _():
            for copy in to_down[part]:
                copy.start()

        @pl.when(jnp.logical_and(has_up, turn))
        def _():
            for copy in to_up[part]:
                copy.start()

    odd = lax.rem(lat, 2) == 1
    held = jnp.logical_and(odd, lat != n_lat // 2 - 1)
    send_layers(True, slice(0, 3))
    send_layers(jnp.logical_not(held), slice(3, None))

    def sides(mine3, theirs3, mine2, theirs2, near, far, row, target):
        return [
            remote(surf.at[mine3], surf.at[theirs3], side_send.at[row, 0], side_recv.at[row, 0], target),
            remote(vel.at[:, mine2], vel.at[:, theirs2], side_send.at[row, 0], side_recv.at[row, 0], target),
            remote(bmap.at[mine2], bmap.at[theirs2], side_send.at[row, 0], side_recv.at[row, 0], target),
            remote(flags.at[mine2], flags.at[theirs2], side_send.at[row, 0], side_recv.at[row, 0], target),
            remote(prev.at[near[0]], prev.at[near[1]], side_send.at[row, 1], side_recv.at[row, 1], target),
            remote(prev.at[far[0]], prev.at[far[1]], side_send.at[row, 1], side_recv.at[row, 2], target),
        ]

    edge_bytes = surf.at[slice(0, 3 + 4 * 2)]

    to_right = sides(slice(rows, rows + 3), slice(0, 3), slice(rows, rows + 2), slice(0, 2),
                     (rows + 1, 1), (rows, 0), 0, right)
    to_left = sides(slice(3, 6), slice(rows + 3, rows + 6), slice(2, 4), slice(rows + 2, rows + 4),
                    (2, rows + 2), (3, rows + 3), 1, left)

    settled(prev.at[own, slice(0, 5)], load_sem.at[1])
    rates_copy.wait()

    @pl.when(has_right)
    def _():
        for copy in to_right[:4]:
            copy.start()

    @pl.when(has_left)
    def _():
        for copy in to_left[:4]:
            copy.start()

    settled(prev.at[own, slice(2, layers - 2)], load_sem.at[2])

    @pl.when(has_right)
    def _():
        for copy in to_right[4:]:
            copy.start()

    @pl.when(has_left)
    def _():
        for copy in to_left[4:]:
            copy.start()

    lane, sub = iotas(width)
    masks = (lane == 0, sub == 0, lane == 127, sub == SUB - 1)

    def neighbours(v):
        return before(v, masks) + after(v, masks)

    def sweep_once(i, carry):
        here = prev[i + 1, 0]
        earlier = None
        for z in range(layers):
            later = prev[i + 1, z + 1] if z < layers - 1 else None
            total = CENTRE * here + (prev[i, z] + prev[i + 2, z]) + neighbours(here)
            if earlier is not None:
                total = total + earlier
            if later is not None:
                total = total + later
            once[i, z] = total
            earlier, here = here, later
        return carry

    lax.fori_loop(2, rows, sweep_once, 0)

    rate = [rates[k] for k in range(16)]

    def lookup(index):
        level = rate
        for bit in range(4):
            odd = (index & (1 << bit)) != 0
            level = [jnp.where(odd, level[2 * k + 1], level[2 * k]) for k in range(len(level) // 2)]
        return level[0]

    def advect(i, store):
        low, middle, high = surf[i], surf[i + 1], surf[i + 2]
        west, east = before(middle, masks), after(middle, masks)
        grad_rows = (high - low) * 0.5
        grad_cols = (east - west) * 0.5
        laplace = high + low + east + west - 4.0 * middle
        tendency = -vel[0, i] * grad_rows - vel[1, i] * grad_cols + lookup(bmap[i]) * laplace
        new = middle + TIME_STEP * flags[i].astype(jnp.float32) * tendency
        if store:
            new_surface[i - 2] = new
        shift[i] = new - middle

    def widen(src, dst, i):
        here = src[i + 1]
        dst[i] = (CENTRE + 2.0) * here + (src[i] + src[i + 2]) + neighbours(here)

    all_layers = layers * n_depth
    profile = [
        (all_layers - (depth * layers + z)).astype(jnp.float32) / all_layers * SCALE for z in range(layers)
    ]
    zero = jnp.float32(0.0)
    top = jnp.where(has_up, zero, jnp.float32(SCALE))
    upper = jnp.where(has_up, jnp.float32(SCALE), zero)
    lower = jnp.where(has_down, jnp.float32(SCALE), zero)

    def narrow(v):
        return sum(v[:, k * 128:(k + 1) * 128] for k in range(width // 128))

    def sweep_twice(i, carry):
        here = once[i + 1, 0]
        earlier = None
        part = widest[i]
        acc = None
        for z in range(layers):
            later = once[i + 1, z + 1] if z < layers - 1 else None
            total = CENTRE * here + (once[i, z] + once[i + 2, z]) + neighbours(here)
            if earlier is not None:
                total = total + earlier
            if later is not None:
                total = total + later
            total = SCALE * total + profile[z] * part
            if z == 0:
                total = total + upper * prev[i + 2, 0] + top * (
                    (1.0 / SHARE + 2.0 / all_layers) * shift[i + 2]
                    - (1.0 + 2.0 / all_layers) * wide[i + 1])
            elif z == 1:
                total = total - (top * (1.0 / all_layers)) * shift[i + 2]
            elif z == layers - 1:
                total = total + lower * prev[i + 2, layers - 1]
            elif z < layers - 2:
                acc = total * total if acc is None else acc + total * total
            mesh_out[i, z] = total
            earlier, here = here, later
        squares[i] = narrow(acc)
        return carry

    def arrived(c):
        size = sum(last - first for first, last, sem in pieces if sem == c)

        @pl.when(has_up)
        def _():
            settled(above.at[slice(0, size)], down_recv.at[c])

        @pl.when(has_down)
        def _():
            settled(below.at[slice(0, size)], up_recv.at[c])

    arrived(0)

    for have, target in ((has_up, up), (has_down, down)):
        @pl.when(have)
        def _():
            pl.semaphore_signal(relay_sem, inc=1, device_id=target, device_id_type=MESH)

    corners = []
    for number, (ref, near, depth_from) in enumerate(((above, 1, has_up), (below, 0, has_down))):
        for side, (src, dst, goes, comes, target) in enumerate((
            (rows, 0, has_right, has_left, right),
            (1, rows + 1, has_left, has_right, left),
        )):
            copy = remote(
                ref.at[src, near], ref.at[dst, near],
                corner_send.at[2 * number + side], corner_recv.at[2 * number + side], target)
            goes, comes = jnp.logical_and(goes, depth_from), jnp.logical_and(comes, depth_from)
            corners.append((copy, goes, comes))

            @pl.when(goes)
            def _():
                copy.start()

    def grouped(first, last, size, what):
        def some(g, carry):
            for k in range(size):
                what(first + g * size + k)
            return carry

        count = (last - first) // size
        if count:
            lax.fori_loop(0, count, some, 0)
        for i in range(first + count * size, last):
            what(i)

    grouped(3, rows + 1, 5, lambda i: advect(i, True))
    grouped(3, rows - 1, 5, lambda i: widen(shift, wide, i))
    grouped(3, rows - 3, 5, lambda i: widen(wide, widest, i))
    lax.fori_loop(3, rows - 3, sweep_twice, 0)

    @pl.when(has_left)
    def _():
        settled(edge_bytes, side_recv.at[0, 0])

    @pl.when(has_right)
    def _():
        settled(edge_bytes, side_recv.at[1, 0])

    for i in (0, 1, rows + 2, rows + 3):
        advect(i, False)
    for i in (2, rows + 1):
        advect(i, True)
    for i in (0, 1, 2, rows - 1, rows, rows + 1):
        widen(shift, wide, i)

    @pl.when(jnp.logical_not(has_left))
    def _():
        clear(wide.at[0])

    @pl.when(jnp.logical_not(has_right))
    def _():
        clear(wide.at[rows + 1])

    for i in (0, 1, 2, rows - 3, rows - 2, rows - 1):
        widen(wide, widest, i)

    even = jnp.logical_not(odd)
    far_side = jnp.logical_or(jnp.logical_and(odd, has_right), jnp.logical_and(even, has_left))

    def side_rows(at_left, kind):
        first = lax.select(at_left, 0, rows - 1)
        inward = lax.select(at_left, 1, -1)

        def wait():
            @pl.when(at_left)
            def _():
                to_right[kind].wait_recv()

            @pl.when(jnp.logical_not(at_left))
            def _():
                to_left[kind].wait_recv()

        return first, inward, wait

    def near_rows(at_left, have):
        first, inward, wait = side_rows(at_left, 4)
        pl.when(have)(wait)
        sweep_once(first + 1, 0)

        def body(k, carry):
            return sweep_twice(first + k * inward, 0)

        lax.fori_loop(1, 3, body, 0)

    def edge_row(at_left, have):
        first, inward, wait = side_rows(at_left, 5)

        @pl.when(have)
        def _():
            wait()
            sweep_once(first + 1 - inward, 0)

        sweep_twice(first, 0)

    near_rows(odd, True)
    edge_row(odd, True)
    near_rows(even, far_side)
    send_layers(held, slice(3, None))

    def finish(first, last):
        parts, values = {}, []
        for i in range(first, last):
            acc = None
            for ref, near, far, outer, inner in ((above, 1, 0, 0, 1), (below, 0, 1, layers - 1, layers - 2)):
                here = ref[i + 1, near]
                around = ref[i, near] + ref[i + 2, near] + neighbours(here)
                edge = mesh_out[i, outer] + SCALE * (2.0 * CENTRE * here + 2.0 * around + ref[i + 1, far])
                next_in = mesh_out[i, inner] + SCALE * here
                values += [(i, outer, edge), (i, inner, next_in)]
                both = edge * edge + next_in * next_in
                acc = both if acc is None else acc + both
            parts[i] = squares[i] + narrow(acc)
        for i, z, value in values:
            mesh_out[i, z] = value
        for i, value in parts.items():
            squares[i] = value

    edge_row(even, far_side)

    arrived(1)
    finish(3, 6)
    finish(6, FIRST - 1)

    for copy, goes, comes in corners:
        @pl.when(comes)
        def _():
            copy.wait_recv()

    finish(0, 3)
    arrived(2)
    finish(FIRST - 1, rows - 5)

    arrived(3)
    finish(rows - 5, rows - 3)
    arrived(4)
    finish(rows - 3, rows)

    pl.semaphore_wait(relay_sem, has_up.astype(jnp.int32) + has_down.astype(jnp.int32))
    totals[depth] = jnp.sum(squares[...], axis=1)
    for k in sorted(range(1, n_depth), key=lambda k: abs(2 * k - n_depth)):
        target = lax.rem(depth + k, n_depth)
        copy = remote(totals.at[depth], totals.at[depth], sum_sem.at[0], sum_sem.at[1], {"depth": target})
        copy.start()
    everyone_else = totals.at[slice(0, n_depth - 1)]
    settled(everyone_else, sum_sem.at[1])

    for have, sem in ((has_down, z_send.at[0]), (has_up, z_send.at[1])):
        @pl.when(have)
        def _():
            settled(prev.at[own, slice(0, 2)], sem)

    for have, row in ((has_right, 0), (has_left, 1)):
        @pl.when(have)
        def _():
            settled(edge_bytes, side_send.at[row, 0])
            settled(prev.at[slice(0, 2)], side_send.at[row, 1])

    for copy, goes, comes in corners:
        @pl.when(goes)
        def _():
            copy.wait_send()

    settled(everyone_else, sum_sem.at[0])


def store_kernel(rows, width, mesh_in, surface_in, totals, mesh_out, surface_out, norm_out, norm, sem):
    copies = []
    for s in range(SUB):
        cols = slice(s * width, (s + 1) * width)
        copies.append(pltpu.make_async_copy(mesh_in.at[:, :, s, :], mesh_out.at[:, :, cols], sem.at[0]))
        copies.append(pltpu.make_async_copy(surface_in.at[:, s, :], surface_out.at[:, cols], sem.at[1]))
    for copy in copies:
        copy.start()
    total = totals[0]
    for k in range(1, totals.shape[0]):
        total = total + totals[k]
    nodes = mesh_in.shape[1] * totals.shape[0] * SUB * width
    root = jnp.sqrt(jnp.sum(total, axis=1, keepdims=True) / nodes)
    spot = lax.broadcasted_iota(jnp.int32, (rows, 128), 0) == lax.broadcasted_iota(jnp.int32, (rows, 128), 1)
    norm[...] = jnp.sum(jnp.where(spot, root, 0.0), axis=0)[:rows]
    last = pltpu.make_async_copy(norm, norm_out, sem.at[2])
    last.start()
    last.wait()
    for ref, k in ((mesh_in, 0), (surface_in, 1)):
        pltpu.make_async_copy(ref, ref, sem.at[k]).wait()


def solution(mesh):
    n_lat, n_depth = mesh.shape["lat"], mesh.shape["depth"]

    def per_device(surface, velocity, block_map, free_flags, block_rates, previous):
        rows, layers, columns = previous.shape
        width = columns // SUB
        f32 = jnp.float32

        def vmem(*shape, dtype=f32):
            return pltpu.VMEM(shape, dtype)

        def kernel(*refs):
            relax_kernel(rows, layers, width, n_lat, n_depth, *refs)

        hbm = pl.BlockSpec(memory_space=pl.ANY)
        inside = pl.BlockSpec(memory_space=pltpu.VMEM)
        dma = pltpu.SemaphoreType.DMA
        new_surface, field, norm = pl.pallas_call(
            kernel,
            out_shape=(
                jax.ShapeDtypeStruct((rows, SUB, width), f32),
                jax.ShapeDtypeStruct((rows, layers, SUB, width), f32),
                jax.ShapeDtypeStruct((n_depth, rows, 128), f32),
            ),
            in_specs=[hbm] * 6,
            out_specs=(inside, inside, inside),
            scratch_shapes=[
                vmem(rows + 4, layers, SUB, width),
                vmem(rows + 2, layers, SUB, width),
                vmem(rows + 2, 2, SUB, width),
                vmem(rows + 2, 2, SUB, width),
                vmem(rows + 6, SUB, width),
                vmem(2, rows + 4, SUB, width),
                vmem(rows + 4, SUB, width, dtype=jnp.int32),
                vmem(rows + 4, SUB, width, dtype=jnp.int32),
                pltpu.SMEM((16,), f32),
                vmem(rows + 4, SUB, width),
                vmem(rows + 2, SUB, width),
                vmem(rows, SUB, width),
                vmem(rows, SUB, 128),
                dma((4,)),
                dma((2,)), dma((5,)), dma((5,)),
                dma((2, 2)), dma((2, 3)),
                dma((4,)), dma((4,)),
                dma((2,)),
                pltpu.SemaphoreType.REGULAR,
            ],
            compiler_params=pltpu.CompilerParams(
                collective_id=0, has_side_effects=True, vmem_limit_bytes=VMEM_LIMIT
            ),
            name="relax",
        )(*(
            pltpu.with_memory_space_constraint(value, pltpu.HBM)
            for value in (surface, velocity, block_map, free_flags, block_rates, previous)
        ))

        def store(*refs):
            store_kernel(rows, width, *refs)

        field, new_surface, norm = pl.pallas_call(
            store,
            out_shape=(
                jax.ShapeDtypeStruct(previous.shape, f32),
                jax.ShapeDtypeStruct(surface.shape, f32),
                jax.ShapeDtypeStruct((rows,), f32),
            ),
            in_specs=[inside, inside, inside],
            out_specs=(hbm, hbm, hbm),
            scratch_shapes=[vmem(rows), dma((3,))],
            compiler_params=pltpu.CompilerParams(vmem_limit_bytes=1024 * 1024),
            name="store",
        )(field, new_surface, norm)
        return new_surface, field, norm

    return jax.shard_map(
        per_device,
        mesh=mesh,
        in_specs=(
            P("lat", None), P(None, "lat", None), P("lat", None), P("lat", None), P(),
            P("lat", "depth", None),
        ),
        out_specs=(P("lat", None), P("lat", "depth", None), P("lat")),
        check_vma=False,
    )


VMEM_LIMIT = 40 * 1024 * 1024
```

```python
import jax
import jax.numpy as jnp
from jax import lax
from jax.experimental import pallas as pl
from jax.experimental.pallas import tpu as pltpu
from jax.sharding import PartitionSpec as P

MESH = pl.DeviceIdType.MESH
TIME_STEP = 0.5
RELAX_WEIGHT = 0.8
KEEP = 1.0 - RELAX_WEIGHT
SHARE = RELAX_WEIGHT / 6.0
CENTRE = KEEP / SHARE
SCALE = SHARE * SHARE
SUB = 8
FIRST = 10


def iotas(width):
    lane = lax.broadcasted_iota(jnp.int32, (SUB, 128), 1)
    sub = lax.broadcasted_iota(jnp.int32, (SUB, 128), 0)
    return lane, sub


def before(v, masks):
    width = v.shape[-1]
    rolled = pltpu.roll(v, 1, 1)
    first = rolled[:, :128]
    carried = pltpu.roll(first, 1, 0)
    first = jnp.where(masks[0], jnp.where(masks[1], 0.0, carried), first)
    return jnp.concatenate([first, rolled[:, 128:]], axis=1)


def after(v, masks):
    width = v.shape[-1]
    rolled = pltpu.roll(v, width - 1, 1)
    last = rolled[:, width - 128:]
    carried = pltpu.roll(last, SUB - 1, 0)
    last = jnp.where(masks[2], jnp.where(masks[3], 0.0, carried), last)
    return jnp.concatenate([rolled[:, : width - 128], last], axis=1)


def relax_kernel(
    rows, layers, width, n_lat, n_depth,
    surface, velocity, block_map, free_flags, block_rates, previous,
    new_surface, mesh_out, totals,
    prev, once, above, below, surf, vel, bmap, flags, rates,
    shift, wide, widest, squares,
    load_sem, z_send, up_recv, down_recv, side_send, side_recv,
    corner_send, corner_recv, sum_sem, relay_sem,
):
    lat = lax.axis_index("lat")
    depth = lax.axis_index("depth")
    has_left, has_right = lat > 0, lat < n_lat - 1
    has_up, has_down = depth > 0, depth < n_depth - 1
    left, right = {"lat": lat - 1}, {"lat": lat + 1}
    up, down = {"depth": depth - 1}, {"depth": depth + 1}

    barrier = pltpu.get_barrier_semaphore()
    around = ((has_up, up), (has_down, down), (has_left, left), (has_right, right))
    for have, target in around:
        @pl.when(have)
        def _():
            pl.semaphore_signal(barrier, inc=1, device_id=target, device_id_type=MESH)

    def settled(ref, sem):
        pltpu.make_async_copy(ref, ref, sem).wait()

    def load(sem, pairs):
        for src, dst in pairs:
            pltpu.make_async_copy(src, dst, sem).start()

    pieces = [
        (0, 1, 0), (rows - 1, rows, 0), (1, FIRST, 1), (FIRST, rows - 4, 2),
        (rows - 4, rows - 2, 3), (rows - 2, rows - 1, 4),
    ]

    cols = [slice(s * width, (s + 1) * width) for s in range(SUB)]
    own = slice(2, 2 + rows)
    load(load_sem.at[0], [
        (previous.at[:, part, cols[s]], prev.at[own, part, s, :])
        for part in (slice(layers - 2, layers), slice(0, 2)) for s in range(SUB)
    ])
    load(load_sem.at[1],
         [(surface.at[:, cols[s]], surf.at[slice(3, 3 + rows), s, :]) for s in range(SUB)]
         + [(velocity.at[:, :, cols[s]], vel.at[:, own, s, :]) for s in range(SUB)]
         + [(block_map.at[:, cols[s]], bmap.at[own, s, :]) for s in range(SUB)]
         + [(free_flags.at[:, cols[s]], flags.at[own, s, :]) for s in range(SUB)])
    load(load_sem.at[2], [
        (previous.at[:, part, cols[s]], prev.at[own, part, s, :])
        for part in (slice(2, SUB), slice(layers - SUB, layers - 2)) for s in range(SUB)
    ])
    rates_copy = pltpu.make_async_copy(block_rates, rates, load_sem.at[3])
    rates_copy.start()

    def clear(ref):
        ref[...] = jnp.zeros(ref.shape, ref.dtype)

    @pl.when(jnp.logical_not(has_up))
    def _():
        clear(above)

    @pl.when(jnp.logical_not(has_down))
    def _():
        clear(below)

    for have, near, far, at in (
        (has_left, slice(0, 2), slice(0, 3), 0),
        (has_right, slice(rows + 2, rows + 4), slice(rows + 3, rows + 6), rows + 1),
    ):
        @pl.when(jnp.logical_not(have))
        def _():
            clear(prev.at[near])
            clear(surf.at[far])
            clear(vel.at[:, near])
            clear(bmap.at[near])
            clear(flags.at[near])
            clear(above.at[at])
            clear(below.at[at])
            clear(once.at[at])

    pl.semaphore_wait(barrier, sum(have.astype(jnp.int32) for have, _ in around))

    def remote(src, dst, send, recv, target):
        return pltpu.make_async_remote_copy(
            src_ref=src, dst_ref=dst, send_sem=send, recv_sem=recv,
            device_id=target, device_id_type=MESH,
        )

    last_two, first_two = slice(layers - 2, layers), slice(0, 2)
    to_down, to_up = [], []
    for first, last, c in pieces:
        mine, theirs = slice(2 + first, 2 + last), slice(1 + first, 1 + last)
        to_down.append(remote(prev.at[mine, last_two], above.at[theirs], z_send.at[0], down_recv.at[c], down))
        to_up.append(remote(prev.at[mine, first_two], below.at[theirs], z_send.at[1], up_recv.at[c], up))

    settled(prev.at[own, slice(0, 4)], load_sem.at[0])

    def send_layers(turn, part):
        @pl.when(jnp.logical_and(has_down, turn))
        def _():
            for copy in to_down[part]:
                copy.start()

        @pl.when(jnp.logical_and(has_up, turn))
        def _():
            for copy in to_up[part]:
                copy.start()

    odd = lax.rem(lat, 2) == 1
    half = n_lat // 2
    late = jnp.logical_or(lat == 1, lat == half - 1)
    held = jnp.logical_and(odd, jnp.logical_not(late))
    send_layers(True, slice(0, 3))
    send_layers(jnp.logical_not(held), slice(3, None))

    def sides(mine3, theirs3, mine2, theirs2, near, far, row, target):
        return [
            remote(surf.at[mine3], surf.at[theirs3], side_send.at[row, 0], side_recv.at[row, 0], target),
            remote(vel.at[:, mine2], vel.at[:, theirs2], side_send.at[row, 0], side_recv.at[row, 0], target),
            remote(bmap.at[mine2], bmap.at[theirs2], side_send.at[row, 0], side_recv.at[row, 0], target),
            remote(flags.at[mine2], flags.at[theirs2], side_send.at[row, 0], side_recv.at[row, 0], target),
            remote(prev.at[near[0]], prev.at[near[1]], side_send.at[row, 1], side_recv.at[row, 1], target),
            remote(prev.at[far[0]], prev.at[far[1]], side_send.at[row, 1], side_recv.at[row, 2], target),
        ]

    edge_bytes = surf.at[slice(0, 3 + 4 * 2)]

    to_right = sides(slice(rows, rows + 3), slice(0, 3), slice(rows, rows + 2), slice(0, 2),
                     (rows + 1, 1), (rows, 0), 0, right)
    to_left = sides(slice(3, 6), slice(rows + 3, rows + 6), slice(2, 4), slice(rows + 2, rows + 4),
                    (2, rows + 2), (3, rows + 3), 1, left)

    settled(prev.at[own, slice(0, 5)], load_sem.at[1])
    rates_copy.wait()

    @pl.when(has_right)
    def _():
        for copy in to_right[:4]:
            copy.start()

    @pl.when(has_left)
    def _():
        for copy in to_left[:4]:
            copy.start()

    settled(prev.at[own, slice(2, layers - 2)], load_sem.at[2])

    @pl.when(has_right)
    def _():
        for copy in to_right[4:]:
            copy.start()

    @pl.when(has_left)
    def _():
        for copy in to_left[4:]:
            copy.start()

    lane, sub = iotas(width)
    masks = (lane == 0, sub == 0, lane == 127, sub == SUB - 1)

    def neighbours(v):
        return before(v, masks) + after(v, masks)

    def sweep_once(i, carry):
        here = prev[i + 1, 0]
        earlier = None
        for z in range(layers):
            later = prev[i + 1, z + 1] if z < layers - 1 else None
            total = CENTRE * here + (prev[i, z] + prev[i + 2, z]) + neighbours(here)
            if earlier is not None:
                total = total + earlier
            if later is not None:
                total = total + later
            once[i, z] = total
            earlier, here = here, later
        return carry

    lax.fori_loop(2, rows, sweep_once, 0)

    rate = [rates[k] for k in range(16)]

    def lookup(index):
        level = rate
        for bit in range(4):
            odd = (index & (1 << bit)) != 0
            level = [jnp.where(odd, level[2 * k + 1], level[2 * k]) for k in range(len(level) // 2)]
        return level[0]

    def advect(i, store):
        low, middle, high = surf[i], surf[i + 1], surf[i + 2]
        west, east = before(middle, masks), after(middle, masks)
        grad_rows = (high - low) * 0.5
        grad_cols = (east - west) * 0.5
        laplace = high + low + east + west - 4.0 * middle
        tendency = -vel[0, i] * grad_rows - vel[1, i] * grad_cols + lookup(bmap[i]) * laplace
        new = middle + TIME_STEP * flags[i].astype(jnp.float32) * tendency
        if store:
            new_surface[i - 2] = new
        shift[i] = new - middle

    def widen(src, dst, i):
        here = src[i + 1]
        dst[i] = (CENTRE + 2.0) * here + (src[i] + src[i + 2]) + neighbours(here)

    all_layers = layers * n_depth
    profile = [
        (all_layers - (depth * layers + z)).astype(jnp.float32) / all_layers * SCALE for z in range(layers)
    ]
    zero = jnp.float32(0.0)
    top = jnp.where(has_up, zero, jnp.float32(SCALE))
    upper = jnp.where(has_up, jnp.float32(SCALE), zero)
    lower = jnp.where(has_down, jnp.float32(SCALE), zero)

    def narrow(v):
        return sum(v[:, k * 128:(k + 1) * 128] for k in range(width // 128))

    def sweep_twice(i, carry):
        here = once[i + 1, 0]
        earlier = None
        part = widest[i]
        acc = None
        for z in range(layers):
            later = once[i + 1, z + 1] if z < layers - 1 else None
            total = CENTRE * here + (once[i, z] + once[i + 2, z]) + neighbours(here)
            if earlier is not None:
                total = total + earlier
            if later is not None:
                total = total + later
            total = SCALE * total + profile[z] * part
            if z == 0:
                total = total + upper * prev[i + 2, 0] + top * (
                    (1.0 / SHARE + 2.0 / all_layers) * shift[i + 2]
                    - (1.0 + 2.0 / all_layers) * wide[i + 1])
            elif z == 1:
                total = total - (top * (1.0 / all_layers)) * shift[i + 2]
            elif z == layers - 1:
                total = total + lower * prev[i + 2, layers - 1]
            elif z < layers - 2:
                acc = total * total if acc is None else acc + total * total
            mesh_out[i, z] = total
            earlier, here = here, later
        squares[i] = narrow(acc)
        return carry

    def arrived(c):
        size = sum(last - first for first, last, sem in pieces if sem == c)

        @pl.when(has_up)
        def _():
            settled(above.at[slice(0, size)], down_recv.at[c])

        @pl.when(has_down)
        def _():
            settled(below.at[slice(0, size)], up_recv.at[c])

    arrived(0)

    for have, target in ((has_up, up), (has_down, down)):
        @pl.when(have)
        def _():
            pl.semaphore_signal(relay_sem, inc=1, device_id=target, device_id_type=MESH)

    corners = []
    for number, (ref, near, depth_from) in enumerate(((above, 1, has_up), (below, 0, has_down))):
        for side, (src, dst, goes, comes, target) in enumerate((
            (rows, 0, has_right, has_left, right),
            (1, rows + 1, has_left, has_right, left),
        )):
            copy = remote(
                ref.at[src, near], ref.at[dst, near],
                corner_send.at[2 * number + side], corner_recv.at[2 * number + side], target)
            goes, comes = jnp.logical_and(goes, depth_from), jnp.logical_and(comes, depth_from)
            corners.append((copy, goes, comes))

            @pl.when(goes)
            def _():
                copy.start()

    def grouped(first, last, size, what):
        def some(g, carry):
            for k in range(size):
                what(first + g * size + k)
            return carry

        count = (last - first) // size
        if count:
            lax.fori_loop(0, count, some, 0)
        for i in range(first + count * size, last):
            what(i)

    grouped(3, rows + 1, 5, lambda i: advect(i, True))
    grouped(3, rows - 1, 5, lambda i: widen(shift, wide, i))
    grouped(3, rows - 3, 5, lambda i: widen(wide, widest, i))
    lax.fori_loop(3, rows - 3, sweep_twice, 0)

    @pl.when(has_left)
    def _():
        settled(edge_bytes, side_recv.at[0, 0])

    @pl.when(has_right)
    def _():
        settled(edge_bytes, side_recv.at[1, 0])

    for i in (0, 1, rows + 2, rows + 3):
        advect(i, False)
    for i in (2, rows + 1):
        advect(i, True)
    for i in (0, 1, 2, rows - 1, rows, rows + 1):
        widen(shift, wide, i)

    @pl.when(jnp.logical_not(has_left))
    def _():
        clear(wide.at[0])

    @pl.when(jnp.logical_not(has_right))
    def _():
        clear(wide.at[rows + 1])

    for i in (0, 1, 2, rows - 3, rows - 2, rows - 1):
        widen(wide, widest, i)

    even = jnp.logical_not(odd)
    far_side = jnp.logical_or(jnp.logical_and(odd, has_right), jnp.logical_and(even, has_left))

    def side_rows(at_left, kind):
        first = lax.select(at_left, 0, rows - 1)
        inward = lax.select(at_left, 1, -1)

        def wait():
            @pl.when(at_left)
            def _():
                to_right[kind].wait_recv()

            @pl.when(jnp.logical_not(at_left))
            def _():
                to_left[kind].wait_recv()

        return first, inward, wait

    def near_rows(at_left, have):
        first, inward, wait = side_rows(at_left, 4)
        pl.when(have)(wait)
        sweep_once(first + 1, 0)

        def body(k, carry):
            return sweep_twice(first + k * inward, 0)

        lax.fori_loop(1, 3, body, 0)

    def edge_row(at_left, have):
        first, inward, wait = side_rows(at_left, 5)

        @pl.when(have)
        def _():
            wait()
            sweep_once(first + 1 - inward, 0)

        sweep_twice(first, 0)

    near_rows(odd, True)
    edge_row(odd, True)
    near_rows(even, far_side)
    send_layers(held, slice(3, None))

    def finish(first, last):
        parts, values = {}, []
        for i in range(first, last):
            acc = None
            for ref, near, far, outer, inner in ((above, 1, 0, 0, 1), (below, 0, 1, layers - 1, layers - 2)):
                here = ref[i + 1, near]
                around = ref[i, near] + ref[i + 2, near] + neighbours(here)
                edge = mesh_out[i, outer] + SCALE * (2.0 * CENTRE * here + 2.0 * around + ref[i + 1, far])
                next_in = mesh_out[i, inner] + SCALE * here
                values += [(i, outer, edge), (i, inner, next_in)]
                both = edge * edge + next_in * next_in
                acc = both if acc is None else acc + both
            parts[i] = squares[i] + narrow(acc)
        for i, z, value in values:
            mesh_out[i, z] = value
        for i, value in parts.items():
            squares[i] = value

    def middle():
        arrived(2)
        finish(FIRST - 1, rows - 5)

    arrived(1)
    for first in range(1, FIRST - 1, 4):
        finish(first, min(first + 4, FIRST - 1))
    pl.when(even)(middle)
    edge_row(even, far_side)

    for copy, goes, comes in corners:
        @pl.when(comes)
        def _():
            copy.wait_recv()

    finish(0, 1)
    pl.when(odd)(middle)
    arrived(3)
    finish(rows - 5, rows - 3)
    arrived(4)
    finish(rows - 3, rows)

    pl.semaphore_wait(relay_sem, has_up.astype(jnp.int32) + has_down.astype(jnp.int32))
    totals[depth] = jnp.sum(squares[...], axis=1)
    for k in sorted(range(1, n_depth), key=lambda k: abs(2 * k - n_depth)):
        target = lax.rem(depth + k, n_depth)
        copy = remote(totals.at[depth], totals.at[depth], sum_sem.at[0], sum_sem.at[1], {"depth": target})
        copy.start()
    everyone_else = totals.at[slice(0, n_depth - 1)]
    settled(everyone_else, sum_sem.at[1])

    for have, sem in ((has_down, z_send.at[0]), (has_up, z_send.at[1])):
        @pl.when(have)
        def _():
            settled(prev.at[own, slice(0, 2)], sem)

    for have, row in ((has_right, 0), (has_left, 1)):
        @pl.when(have)
        def _():
            settled(edge_bytes, side_send.at[row, 0])
            settled(prev.at[slice(0, 2)], side_send.at[row, 1])

    for copy, goes, comes in corners:
        @pl.when(goes)
        def _():
            copy.wait_send()

    settled(everyone_else, sum_sem.at[0])


def store_kernel(rows, width, mesh_in, surface_in, totals, mesh_out, surface_out, norm_out, norm, sem):
    copies = []
    for s in range(SUB):
        cols = slice(s * width, (s + 1) * width)
        copies.append(pltpu.make_async_copy(mesh_in.at[:, :, s, :], mesh_out.at[:, :, cols], sem.at[0]))
        copies.append(pltpu.make_async_copy(surface_in.at[:, s, :], surface_out.at[:, cols], sem.at[1]))
    for copy in copies:
        copy.start()
    total = totals[0]
    for k in range(1, totals.shape[0]):
        total = total + totals[k]
    nodes = mesh_in.shape[1] * totals.shape[0] * SUB * width
    root = jnp.sqrt(jnp.sum(total, axis=1, keepdims=True) / nodes)
    spot = lax.broadcasted_iota(jnp.int32, (rows, 128), 0) == lax.broadcasted_iota(jnp.int32, (rows, 128), 1)
    norm[...] = jnp.sum(jnp.where(spot, root, 0.0), axis=0)[:rows]
    last = pltpu.make_async_copy(norm, norm_out, sem.at[2])
    last.start()
    last.wait()
    for ref, k in ((mesh_in, 0), (surface_in, 1)):
        pltpu.make_async_copy(ref, ref, sem.at[k]).wait()


def solution(mesh):
    n_lat, n_depth = mesh.shape["lat"], mesh.shape["depth"]

    def per_device(surface, velocity, block_map, free_flags, block_rates, previous):
        rows, layers, columns = previous.shape
        width = columns // SUB
        f32 = jnp.float32

        def vmem(*shape, dtype=f32):
            return pltpu.VMEM(shape, dtype)

        def kernel(*refs):
            relax_kernel(rows, layers, width, n_lat, n_depth, *refs)

        hbm = pl.BlockSpec(memory_space=pl.ANY)
        inside = pl.BlockSpec(memory_space=pltpu.VMEM)
        dma = pltpu.SemaphoreType.DMA
        new_surface, field, norm = pl.pallas_call(
            kernel,
            out_shape=(
                jax.ShapeDtypeStruct((rows, SUB, width), f32),
                jax.ShapeDtypeStruct((rows, layers, SUB, width), f32),
                jax.ShapeDtypeStruct((n_depth, rows, 128), f32),
            ),
            in_specs=[hbm] * 6,
            out_specs=(inside, inside, inside),
            scratch_shapes=[
                vmem(rows + 4, layers, SUB, width),
                vmem(rows + 2, layers, SUB, width),
                vmem(rows + 2, 2, SUB, width),
                vmem(rows + 2, 2, SUB, width),
                vmem(rows + 6, SUB, width),
                vmem(2, rows + 4, SUB, width),
                vmem(rows + 4, SUB, width, dtype=jnp.int32),
                vmem(rows + 4, SUB, width, dtype=jnp.int32),
                pltpu.SMEM((16,), f32),
                vmem(rows + 4, SUB, width),
                vmem(rows + 2, SUB, width),
                vmem(rows, SUB, width),
                vmem(rows, SUB, 128),
                dma((4,)),
                dma((2,)), dma((5,)), dma((5,)),
                dma((2, 2)), dma((2, 3)),
                dma((4,)), dma((4,)),
                dma((2,)),
                pltpu.SemaphoreType.REGULAR,
            ],
            compiler_params=pltpu.CompilerParams(
                collective_id=0, has_side_effects=True, vmem_limit_bytes=VMEM_LIMIT
            ),
            name="relax",
        )(*(
            pltpu.with_memory_space_constraint(value, pltpu.HBM)
            for value in (surface, velocity, block_map, free_flags, block_rates, previous)
        ))

        def store(*refs):
            store_kernel(rows, width, *refs)

        field, new_surface, norm = pl.pallas_call(
            store,
            out_shape=(
                jax.ShapeDtypeStruct(previous.shape, f32),
                jax.ShapeDtypeStruct(surface.shape, f32),
                jax.ShapeDtypeStruct((rows,), f32),
            ),
            in_specs=[inside, inside, inside],
            out_specs=(hbm, hbm, hbm),
            scratch_shapes=[vmem(rows), dma((3,))],
            compiler_params=pltpu.CompilerParams(vmem_limit_bytes=1024 * 1024),
            name="store",
        )(field, new_surface, norm)
        return new_surface, field, norm

    return jax.shard_map(
        per_device,
        mesh=mesh,
        in_specs=(
            P("lat", None), P(None, "lat", None), P("lat", None), P("lat", None), P(),
            P("lat", "depth", None),
        ),
        out_specs=(P("lat", None), P("lat", "depth", None), P("lat")),
        check_vma=False,
    )


VMEM_LIMIT = 40 * 1024 * 1024
```

```python
import jax
import jax.numpy as jnp
from jax import lax
from jax.experimental import pallas as pl
from jax.experimental.pallas import tpu as pltpu
from jax.sharding import PartitionSpec as P

MESH = pl.DeviceIdType.MESH
TIME_STEP = 0.5
RELAX_WEIGHT = 0.8
KEEP = 1.0 - RELAX_WEIGHT
SHARE = RELAX_WEIGHT / 6.0
CENTRE = KEEP / SHARE
SCALE = SHARE * SHARE
SUB = 8
FIRST = 10


def iotas(width):
    lane = lax.broadcasted_iota(jnp.int32, (SUB, 128), 1)
    sub = lax.broadcasted_iota(jnp.int32, (SUB, 128), 0)
    return lane, sub


def before(v, masks):
    width = v.shape[-1]
    rolled = pltpu.roll(v, 1, 1)
    first = rolled[:, :128]
    carried = pltpu.roll(first, 1, 0)
    first = jnp.where(masks[0], jnp.where(masks[1], 0.0, carried), first)
    return jnp.concatenate([first, rolled[:, 128:]], axis=1)


def after(v, masks):
    width = v.shape[-1]
    rolled = pltpu.roll(v, width - 1, 1)
    last = rolled[:, width - 128:]
    carried = pltpu.roll(last, SUB - 1, 0)
    last = jnp.where(masks[2], jnp.where(masks[3], 0.0, carried), last)
    return jnp.concatenate([rolled[:, : width - 128], last], axis=1)


def relax_kernel(
    rows, layers, width, n_lat, n_depth,
    surface, velocity, block_map, free_flags, block_rates, previous,
    new_surface, mesh_out, totals,
    prev, once, above, below, surf, vel, bmap, flags, rates,
    shift, wide, widest, squares,
    load_sem, z_send, up_recv, down_recv, side_send, side_recv,
    corner_send, corner_recv, sum_sem, relay_sem,
):
    lat = lax.axis_index("lat")
    depth = lax.axis_index("depth")
    has_left, has_right = lat > 0, lat < n_lat - 1
    has_up, has_down = depth > 0, depth < n_depth - 1
    left, right = {"lat": lat - 1}, {"lat": lat + 1}
    up, down = {"depth": depth - 1}, {"depth": depth + 1}

    barrier = pltpu.get_barrier_semaphore()
    around = ((has_up, up), (has_down, down), (has_left, left), (has_right, right))
    for have, target in around:
        @pl.when(have)
        def _():
            pl.semaphore_signal(barrier, inc=1, device_id=target, device_id_type=MESH)

    def settled(ref, sem):
        pltpu.make_async_copy(ref, ref, sem).wait()

    def load(sem, pairs):
        for src, dst in pairs:
            pltpu.make_async_copy(src, dst, sem).start()

    pieces = [
        (0, 1, 0), (rows - 1, rows, 0), (1, FIRST, 1), (FIRST, rows - 4, 2),
        (rows - 4, rows - 2, 3), (rows - 2, rows - 1, 4),
    ]

    cols = [slice(s * width, (s + 1) * width) for s in range(SUB)]
    own = slice(2, 2 + rows)
    load(load_sem.at[0], [
        (previous.at[:, part, cols[s]], prev.at[own, part, s, :])
        for part in (slice(layers - 2, layers), slice(0, 2)) for s in range(SUB)
    ])
    load(load_sem.at[1],
         [(surface.at[:, cols[s]], surf.at[slice(3, 3 + rows), s, :]) for s in range(SUB)]
         + [(velocity.at[:, :, cols[s]], vel.at[:, own, s, :]) for s in range(SUB)]
         + [(block_map.at[:, cols[s]], bmap.at[own, s, :]) for s in range(SUB)]
         + [(free_flags.at[:, cols[s]], flags.at[own, s, :]) for s in range(SUB)])
    load(load_sem.at[2], [
        (previous.at[:, part, cols[s]], prev.at[own, part, s, :])
        for part in (slice(2, SUB), slice(layers - SUB, layers - 2)) for s in range(SUB)
    ])
    rates_copy = pltpu.make_async_copy(block_rates, rates, load_sem.at[3])
    rates_copy.start()

    def clear(ref):
        ref[...] = jnp.zeros(ref.shape, ref.dtype)

    @pl.when(jnp.logical_not(has_up))
    def _():
        clear(above)

    @pl.when(jnp.logical_not(has_down))
    def _():
        clear(below)

    for have, near, far, at in (
        (has_left, slice(0, 2), slice(0, 3), 0),
        (has_right, slice(rows + 2, rows + 4), slice(rows + 3, rows + 6), rows + 1),
    ):
        @pl.when(jnp.logical_not(have))
        def _():
            clear(prev.at[near])
            clear(surf.at[far])
            clear(vel.at[:, near])
            clear(bmap.at[near])
            clear(flags.at[near])
            clear(above.at[at])
            clear(below.at[at])
            clear(once.at[at])

    pl.semaphore_wait(barrier, sum(have.astype(jnp.int32) for have, _ in around))

    def remote(src, dst, send, recv, target):
        return pltpu.make_async_remote_copy(
            src_ref=src, dst_ref=dst, send_sem=send, recv_sem=recv,
            device_id=target, device_id_type=MESH,
        )

    last_two, first_two = slice(layers - 2, layers), slice(0, 2)
    to_down, to_up = [], []
    for first, last, c in pieces:
        mine, theirs = slice(2 + first, 2 + last), slice(1 + first, 1 + last)
        to_down.append(remote(prev.at[mine, last_two], above.at[theirs], z_send.at[0], down_recv.at[c], down))
        to_up.append(remote(prev.at[mine, first_two], below.at[theirs], z_send.at[1], up_recv.at[c], up))

    settled(prev.at[own, slice(0, 4)], load_sem.at[0])

    def send_layers(turn, part):
        @pl.when(jnp.logical_and(has_down, turn))
        def _():
            for copy in to_down[part]:
                copy.start()

        @pl.when(jnp.logical_and(has_up, turn))
        def _():
            for copy in to_up[part]:
                copy.start()

    odd = lax.rem(lat, 2) == 1
    half = n_lat // 2
    late = jnp.logical_or(lat == 1, lat == half - 1)
    held = jnp.logical_or(jnp.logical_and(odd, jnp.logical_not(late)), lat == 0)
    send_layers(True, slice(0, 3))
    send_layers(jnp.logical_not(held), slice(3, None))

    def sides(mine3, theirs3, mine2, theirs2, near, far, row, target):
        return [
            remote(surf.at[mine3], surf.at[theirs3], side_send.at[row, 0], side_recv.at[row, 0], target),
            remote(vel.at[:, mine2], vel.at[:, theirs2], side_send.at[row, 0], side_recv.at[row, 0], target),
            remote(bmap.at[mine2], bmap.at[theirs2], side_send.at[row, 0], side_recv.at[row, 0], target),
            remote(flags.at[mine2], flags.at[theirs2], side_send.at[row, 0], side_recv.at[row, 0], target),
            remote(prev.at[near[0]], prev.at[near[1]], side_send.at[row, 1], side_recv.at[row, 1], target),
            remote(prev.at[far[0]], prev.at[far[1]], side_send.at[row, 1], side_recv.at[row, 2], target),
        ]

    edge_bytes = surf.at[slice(0, 3 + 4 * 2)]

    to_right = sides(slice(rows, rows + 3), slice(0, 3), slice(rows, rows + 2), slice(0, 2),
                     (rows + 1, 1), (rows, 0), 0, right)
    to_left = sides(slice(3, 6), slice(rows + 3, rows + 6), slice(2, 4), slice(rows + 2, rows + 4),
                    (2, rows + 2), (3, rows + 3), 1, left)

    settled(prev.at[own, slice(0, 5)], load_sem.at[1])
    rates_copy.wait()

    @pl.when(has_right)
    def _():
        for copy in to_right[:4]:
            copy.start()

    @pl.when(has_left)
    def _():
        for copy in to_left[:4]:
            copy.start()

    settled(prev.at[own, slice(2, layers - 2)], load_sem.at[2])

    @pl.when(has_right)
    def _():
        for copy in to_right[4:]:
            copy.start()

    @pl.when(has_left)
    def _():
        for copy in to_left[4:]:
            copy.start()

    lane, sub = iotas(width)
    masks = (lane == 0, sub == 0, lane == 127, sub == SUB - 1)

    def neighbours(v):
        return before(v, masks) + after(v, masks)

    def sweep_once(i, carry):
        here = prev[i + 1, 0]
        earlier = None
        for z in range(layers):
            later = prev[i + 1, z + 1] if z < layers - 1 else None
            total = CENTRE * here + (prev[i, z] + prev[i + 2, z]) + neighbours(here)
            if earlier is not None:
                total = total + earlier
            if later is not None:
                total = total + later
            once[i, z] = total
            earlier, here = here, later
        return carry

    lax.fori_loop(2, rows, sweep_once, 0)

    rate = [rates[k] for k in range(16)]

    def lookup(index):
        level = rate
        for bit in range(4):
            odd = (index & (1 << bit)) != 0
            level = [jnp.where(odd, level[2 * k + 1], level[2 * k]) for k in range(len(level) // 2)]
        return level[0]

    def advect(i, store):
        low, middle, high = surf[i], surf[i + 1], surf[i + 2]
        west, east = before(middle, masks), after(middle, masks)
        grad_rows = (high - low) * 0.5
        grad_cols = (east - west) * 0.5
        laplace = high + low + east + west - 4.0 * middle
        tendency = -vel[0, i] * grad_rows - vel[1, i] * grad_cols + lookup(bmap[i]) * laplace
        new = middle + TIME_STEP * flags[i].astype(jnp.float32) * tendency
        if store:
            new_surface[i - 2] = new
        shift[i] = new - middle

    def widen(src, dst, i):
        here = src[i + 1]
        dst[i] = (CENTRE + 2.0) * here + (src[i] + src[i + 2]) + neighbours(here)

    all_layers = layers * n_depth
    profile = [
        (all_layers - (depth * layers + z)).astype(jnp.float32) / all_layers * SCALE for z in range(layers)
    ]
    zero = jnp.float32(0.0)
    top = jnp.where(has_up, zero, jnp.float32(SCALE))
    upper = jnp.where(has_up, jnp.float32(SCALE), zero)
    lower = jnp.where(has_down, jnp.float32(SCALE), zero)

    def narrow(v):
        return sum(v[:, k * 128:(k + 1) * 128] for k in range(width // 128))

    def sweep_twice(i, carry):
        here = once[i + 1, 0]
        earlier = None
        part = widest[i]
        acc = None
        for z in range(layers):
            later = once[i + 1, z + 1] if z < layers - 1 else None
            total = CENTRE * here + (once[i, z] + once[i + 2, z]) + neighbours(here)
            if earlier is not None:
                total = total + earlier
            if later is not None:
                total = total + later
            total = SCALE * total + profile[z] * part
            if z == 0:
                total = total + upper * prev[i + 2, 0] + top * (
                    (1.0 / SHARE + 2.0 / all_layers) * shift[i + 2]
                    - (1.0 + 2.0 / all_layers) * wide[i + 1])
            elif z == 1:
                total = total - (top * (1.0 / all_layers)) * shift[i + 2]
            elif z == layers - 1:
                total = total + lower * prev[i + 2, layers - 1]
            elif z < layers - 2:
                acc = total * total if acc is None else acc + total * total
            mesh_out[i, z] = total
            earlier, here = here, later
        squares[i] = narrow(acc)
        return carry

    def arrived(c):
        size = sum(last - first for first, last, sem in pieces if sem == c)

        @pl.when(has_up)
        def _():
            settled(above.at[slice(0, size)], down_recv.at[c])

        @pl.when(has_down)
        def _():
            settled(below.at[slice(0, size)], up_recv.at[c])

    arrived(0)

    for have, target in ((has_up, up), (has_down, down)):
        @pl.when(have)
        def _():
            pl.semaphore_signal(relay_sem, inc=1, device_id=target, device_id_type=MESH)

    corners = []
    for number, (ref, near, depth_from) in enumerate(((above, 1, has_up), (below, 0, has_down))):
        for side, (src, dst, goes, comes, target) in enumerate((
            (rows, 0, has_right, has_left, right),
            (1, rows + 1, has_left, has_right, left),
        )):
            copy = remote(
                ref.at[src, near], ref.at[dst, near],
                corner_send.at[2 * number + side], corner_recv.at[2 * number + side], target)
            goes, comes = jnp.logical_and(goes, depth_from), jnp.logical_and(comes, depth_from)
            corners.append((copy, goes, comes))

            @pl.when(goes)
            def _():
                copy.start()

    def grouped(first, last, size, what):
        def some(g, carry):
            for k in range(size):
                what(first + g * size + k)
            return carry

        count = (last - first) // size
        if count:
            lax.fori_loop(0, count, some, 0)
        for i in range(first + count * size, last):
            what(i)

    grouped(3, rows + 1, 5, lambda i: advect(i, True))
    grouped(3, rows - 1, 5, lambda i: widen(shift, wide, i))
    grouped(3, rows - 3, 5, lambda i: widen(wide, widest, i))
    lax.fori_loop(3, rows - 3, sweep_twice, 0)

    @pl.when(has_left)
    def _():
        settled(edge_bytes, side_recv.at[0, 0])

    @pl.when(has_right)
    def _():
        settled(edge_bytes, side_recv.at[1, 0])

    for i in (0, 1, rows + 2, rows + 3):
        advect(i, False)
    for i in (2, rows + 1):
        advect(i, True)
    for i in (0, 1, 2, rows - 1, rows, rows + 1):
        widen(shift, wide, i)

    @pl.when(jnp.logical_not(has_left))
    def _():
        clear(wide.at[0])

    @pl.when(jnp.logical_not(has_right))
    def _():
        clear(wide.at[rows + 1])

    for i in (0, 1, 2, rows - 3, rows - 2, rows - 1):
        widen(wide, widest, i)

    even = jnp.logical_not(odd)
    far_side = jnp.logical_or(jnp.logical_and(odd, has_right), jnp.logical_and(even, has_left))

    def side_rows(at_left, kind):
        first = lax.select(at_left, 0, rows - 1)
        inward = lax.select(at_left, 1, -1)

        def wait():
            @pl.when(at_left)
            def _():
                to_right[kind].wait_recv()

            @pl.when(jnp.logical_not(at_left))
            def _():
                to_left[kind].wait_recv()

        return first, inward, wait

    def near_rows(at_left, have):
        first, inward, wait = side_rows(at_left, 4)
        pl.when(have)(wait)
        sweep_once(first + 1, 0)

        def body(k, carry):
            return sweep_twice(first + k * inward, 0)

        lax.fori_loop(1, 3, body, 0)

    def edge_row(at_left, have):
        first, inward, wait = side_rows(at_left, 5)

        @pl.when(have)
        def _():
            wait()
            sweep_once(first + 1 - inward, 0)

        sweep_twice(first, 0)

    near_rows(odd, True)
    edge_row(odd, True)
    near_rows(even, far_side)
    send_layers(held, slice(3, None))

    def finish(first, last):
        parts, values = {}, []
        for i in range(first, last):
            acc = None
            for ref, near, far, outer, inner in ((above, 1, 0, 0, 1), (below, 0, 1, layers - 1, layers - 2)):
                here = ref[i + 1, near]
                around = ref[i, near] + ref[i + 2, near] + neighbours(here)
                edge = mesh_out[i, outer] + SCALE * (2.0 * CENTRE * here + 2.0 * around + ref[i + 1, far])
                next_in = mesh_out[i, inner] + SCALE * here
                values += [(i, outer, edge), (i, inner, next_in)]
                both = edge * edge + next_in * next_in
                acc = both if acc is None else acc + both
            parts[i] = squares[i] + narrow(acc)
        for i, z, value in values:
            mesh_out[i, z] = value
        for i, value in parts.items():
            squares[i] = value

    def middle():
        arrived(2)
        finish(FIRST - 1, rows - 5)

    arrived(1)
    for first in range(1, FIRST - 1, 4):
        finish(first, min(first + 4, FIRST - 1))
    pl.when(even)(middle)
    edge_row(even, far_side)

    for copy, goes, comes in corners:
        @pl.when(comes)
        def _():
            copy.wait_recv()

    finish(0, 1)
    pl.when(odd)(middle)
    arrived(3)
    finish(rows - 5, rows - 3)
    arrived(4)
    finish(rows - 3, rows)

    pl.semaphore_wait(relay_sem, has_up.astype(jnp.int32) + has_down.astype(jnp.int32))
    totals[depth] = jnp.sum(squares[...], axis=1)
    for k in sorted(range(1, n_depth), key=lambda k: abs(2 * k - n_depth)):
        target = lax.rem(depth + k, n_depth)
        copy = remote(totals.at[depth], totals.at[depth], sum_sem.at[0], sum_sem.at[1], {"depth": target})
        copy.start()
    everyone_else = totals.at[slice(0, n_depth - 1)]
    settled(everyone_else, sum_sem.at[1])

    for have, sem in ((has_down, z_send.at[0]), (has_up, z_send.at[1])):
        @pl.when(have)
        def _():
            settled(prev.at[own, slice(0, 2)], sem)

    for have, row in ((has_right, 0), (has_left, 1)):
        @pl.when(have)
        def _():
            settled(edge_bytes, side_send.at[row, 0])
            settled(prev.at[slice(0, 2)], side_send.at[row, 1])

    for copy, goes, comes in corners:
        @pl.when(goes)
        def _():
            copy.wait_send()

    settled(everyone_else, sum_sem.at[0])


def store_kernel(rows, width, mesh_in, surface_in, totals, mesh_out, surface_out, norm_out, norm, sem):
    copies = []
    for s in range(SUB):
        cols = slice(s * width, (s + 1) * width)
        copies.append(pltpu.make_async_copy(mesh_in.at[:, :, s, :], mesh_out.at[:, :, cols], sem.at[0]))
        copies.append(pltpu.make_async_copy(surface_in.at[:, s, :], surface_out.at[:, cols], sem.at[1]))
    for copy in copies:
        copy.start()
    total = totals[0]
    for k in range(1, totals.shape[0]):
        total = total + totals[k]
    nodes = mesh_in.shape[1] * totals.shape[0] * SUB * width
    root = jnp.sqrt(jnp.sum(total, axis=1, keepdims=True) / nodes)
    spot = lax.broadcasted_iota(jnp.int32, (rows, 128), 0) == lax.broadcasted_iota(jnp.int32, (rows, 128), 1)
    norm[...] = jnp.sum(jnp.where(spot, root, 0.0), axis=0)[:rows]
    last = pltpu.make_async_copy(norm, norm_out, sem.at[2])
    last.start()
    last.wait()
    for ref, k in ((mesh_in, 0), (surface_in, 1)):
        pltpu.make_async_copy(ref, ref, sem.at[k]).wait()


def solution(mesh):
    n_lat, n_depth = mesh.shape["lat"], mesh.shape["depth"]

    def per_device(surface, velocity, block_map, free_flags, block_rates, previous):
        rows, layers, columns = previous.shape
        width = columns // SUB
        f32 = jnp.float32

        def vmem(*shape, dtype=f32):
            return pltpu.VMEM(shape, dtype)

        def kernel(*refs):
            relax_kernel(rows, layers, width, n_lat, n_depth, *refs)

        hbm = pl.BlockSpec(memory_space=pl.ANY)
        inside = pl.BlockSpec(memory_space=pltpu.VMEM)
        dma = pltpu.SemaphoreType.DMA
        new_surface, field, norm = pl.pallas_call(
            kernel,
            out_shape=(
                jax.ShapeDtypeStruct((rows, SUB, width), f32),
                jax.ShapeDtypeStruct((rows, layers, SUB, width), f32),
                jax.ShapeDtypeStruct((n_depth, rows, 128), f32),
            ),
            in_specs=[hbm] * 6,
            out_specs=(inside, inside, inside),
            scratch_shapes=[
                vmem(rows + 4, layers, SUB, width),
                vmem(rows + 2, layers, SUB, width),
                vmem(rows + 2, 2, SUB, width),
                vmem(rows + 2, 2, SUB, width),
                vmem(rows + 6, SUB, width),
                vmem(2, rows + 4, SUB, width),
                vmem(rows + 4, SUB, width, dtype=jnp.int32),
                vmem(rows + 4, SUB, width, dtype=jnp.int32),
                pltpu.SMEM((16,), f32),
                vmem(rows + 4, SUB, width),
                vmem(rows + 2, SUB, width),
                vmem(rows, SUB, width),
                vmem(rows, SUB, 128),
                dma((4,)),
                dma((2,)), dma((5,)), dma((5,)),
                dma((2, 2)), dma((2, 3)),
                dma((4,)), dma((4,)),
                dma((2,)),
                pltpu.SemaphoreType.REGULAR,
            ],
            compiler_params=pltpu.CompilerParams(
                collective_id=0, has_side_effects=True, vmem_limit_bytes=VMEM_LIMIT
            ),
            name="relax",
        )(*(
            pltpu.with_memory_space_constraint(value, pltpu.HBM)
            for value in (surface, velocity, block_map, free_flags, block_rates, previous)
        ))

        def store(*refs):
            store_kernel(rows, width, *refs)

        field, new_surface, norm = pl.pallas_call(
            store,
            out_shape=(
                jax.ShapeDtypeStruct(previous.shape, f32),
                jax.ShapeDtypeStruct(surface.shape, f32),
                jax.ShapeDtypeStruct((rows,), f32),
            ),
            in_specs=[inside, inside, inside],
            out_specs=(hbm, hbm, hbm),
            scratch_shapes=[vmem(rows), dma((3,))],
            compiler_params=pltpu.CompilerParams(vmem_limit_bytes=1024 * 1024),
            name="store",
        )(field, new_surface, norm)
        return new_surface, field, norm

    return jax.shard_map(
        per_device,
        mesh=mesh,
        in_specs=(
            P("lat", None), P(None, "lat", None), P("lat", None), P("lat", None), P(),
            P("lat", "depth", None),
        ),
        out_specs=(P("lat", None), P("lat", "depth", None), P("lat")),
        check_vma=False,
    )


VMEM_LIMIT = 40 * 1024 * 1024
```

```python
import jax
import jax.numpy as jnp
from jax import lax
from jax.experimental import pallas as pl
from jax.experimental.pallas import tpu as pltpu
from jax.sharding import PartitionSpec as P

MESH = pl.DeviceIdType.MESH
TIME_STEP = 0.5
RELAX_WEIGHT = 0.8
KEEP = 1.0 - RELAX_WEIGHT
SHARE = RELAX_WEIGHT / 6.0
CENTRE = KEEP / SHARE
SCALE = SHARE * SHARE
SUB = 8
FIRST = 9


def iotas(width):
    lane = lax.broadcasted_iota(jnp.int32, (SUB, 128), 1)
    sub = lax.broadcasted_iota(jnp.int32, (SUB, 128), 0)
    return lane, sub


def before(v, masks):
    width = v.shape[-1]
    rolled = pltpu.roll(v, 1, 1)
    first = rolled[:, :128]
    carried = pltpu.roll(first, 1, 0)
    first = jnp.where(masks[0], jnp.where(masks[1], 0.0, carried), first)
    return jnp.concatenate([first, rolled[:, 128:]], axis=1)


def after(v, masks):
    width = v.shape[-1]
    rolled = pltpu.roll(v, width - 1, 1)
    last = rolled[:, width - 128:]
    carried = pltpu.roll(last, SUB - 1, 0)
    last = jnp.where(masks[2], jnp.where(masks[3], 0.0, carried), last)
    return jnp.concatenate([rolled[:, : width - 128], last], axis=1)


def relax_kernel(
    rows, layers, width, n_lat, n_depth,
    surface, velocity, block_map, free_flags, block_rates, previous,
    new_surface, mesh_out, totals,
    prev, once, above, below, surf, vel, bmap, flags, rates,
    shift, wide, widest, squares,
    load_sem, z_send, up_recv, down_recv, side_send, side_recv,
    corner_send, corner_recv, sum_sem, relay_sem,
):
    lat = lax.axis_index("lat")
    depth = lax.axis_index("depth")
    has_left, has_right = lat > 0, lat < n_lat - 1
    has_up, has_down = depth > 0, depth < n_depth - 1
    left, right = {"lat": lat - 1}, {"lat": lat + 1}
    up, down = {"depth": depth - 1}, {"depth": depth + 1}

    barrier = pltpu.get_barrier_semaphore()
    around = ((has_up, up), (has_down, down), (has_left, left), (has_right, right))
    for have, target in around:
        @pl.when(have)
        def _():
            pl.semaphore_signal(barrier, inc=1, device_id=target, device_id_type=MESH)

    def settled(ref, sem):
        pltpu.make_async_copy(ref, ref, sem).wait()

    def load(sem, pairs):
        for src, dst in pairs:
            pltpu.make_async_copy(src, dst, sem).start()

    pieces = [
        (0, 1, 0), (rows - 1, rows, 0), (1, FIRST, 1), (FIRST, rows - 4, 2),
        (rows - 4, rows - 2, 3), (rows - 2, rows - 1, 4),
    ]

    cols = [slice(s * width, (s + 1) * width) for s in range(SUB)]
    own = slice(2, 2 + rows)
    load(load_sem.at[0], [
        (previous.at[:, part, cols[s]], prev.at[own, part, s, :])
        for part in (slice(layers - 2, layers), slice(0, 2)) for s in range(SUB)
    ])
    load(load_sem.at[1],
         [(surface.at[:, cols[s]], surf.at[slice(3, 3 + rows), s, :]) for s in range(SUB)]
         + [(velocity.at[:, :, cols[s]], vel.at[:, own, s, :]) for s in range(SUB)]
         + [(block_map.at[:, cols[s]], bmap.at[own, s, :]) for s in range(SUB)]
         + [(free_flags.at[:, cols[s]], flags.at[own, s, :]) for s in range(SUB)])
    load(load_sem.at[2], [
        (previous.at[:, part, cols[s]], prev.at[own, part, s, :])
        for part in (slice(2, SUB), slice(layers - SUB, layers - 2)) for s in range(SUB)
    ])
    rates_copy = pltpu.make_async_copy(block_rates, rates, load_sem.at[3])
    rates_copy.start()

    def clear(ref):
        ref[...] = jnp.zeros(ref.shape, ref.dtype)

    @pl.when(jnp.logical_not(has_up))
    def _():
        clear(above)

    @pl.when(jnp.logical_not(has_down))
    def _():
        clear(below)

    for have, near, far, at in (
        (has_left, slice(0, 2), slice(0, 3), 0),
        (has_right, slice(rows + 2, rows + 4), slice(rows + 3, rows + 6), rows + 1),
    ):
        @pl.when(jnp.logical_not(have))
        def _():
            clear(prev.at[near])
            clear(surf.at[far])
            clear(vel.at[:, near])
            clear(bmap.at[near])
            clear(flags.at[near])
            clear(above.at[at])
            clear(below.at[at])
            clear(once.at[at])

    pl.semaphore_wait(barrier, sum(have.astype(jnp.int32) for have, _ in around))

    def remote(src, dst, send, recv, target):
        return pltpu.make_async_remote_copy(
            src_ref=src, dst_ref=dst, send_sem=send, recv_sem=recv,
            device_id=target, device_id_type=MESH,
        )

    last_two, first_two = slice(layers - 2, layers), slice(0, 2)
    to_down, to_up = [], []
    for first, last, c in pieces:
        mine, theirs = slice(2 + first, 2 + last), slice(1 + first, 1 + last)
        to_down.append(remote(prev.at[mine, last_two], above.at[theirs], z_send.at[0], down_recv.at[c], down))
        to_up.append(remote(prev.at[mine, first_two], below.at[theirs], z_send.at[1], up_recv.at[c], up))

    settled(prev.at[own, slice(0, 4)], load_sem.at[0])

    def send_layers(turn, part):
        @pl.when(jnp.logical_and(has_down, turn))
        def _():
            for copy in to_down[part]:
                copy.start()

        @pl.when(jnp.logical_and(has_up, turn))
        def _():
            for copy in to_up[part]:
                copy.start()

    odd = lax.rem(lat, 2) == 1
    half = n_lat // 2
    late = jnp.logical_or(lat == 1, lat == half - 1)
    held = jnp.logical_or(jnp.logical_and(odd, jnp.logical_not(late)), lat == 0)
    send_layers(True, slice(0, 3))
    send_layers(jnp.logical_not(held), slice(3, None))

    def sides(mine3, theirs3, mine2, theirs2, near, far, row, target):
        return [
            remote(surf.at[mine3], surf.at[theirs3], side_send.at[row, 0], side_recv.at[row, 0], target),
            remote(vel.at[:, mine2], vel.at[:, theirs2], side_send.at[row, 0], side_recv.at[row, 0], target),
            remote(bmap.at[mine2], bmap.at[theirs2], side_send.at[row, 0], side_recv.at[row, 0], target),
            remote(flags.at[mine2], flags.at[theirs2], side_send.at[row, 0], side_recv.at[row, 0], target),
            remote(prev.at[near[0]], prev.at[near[1]], side_send.at[row, 1], side_recv.at[row, 1], target),
            remote(prev.at[far[0]], prev.at[far[1]], side_send.at[row, 1], side_recv.at[row, 2], target),
        ]

    edge_bytes = surf.at[slice(0, 3 + 4 * 2)]

    to_right = sides(slice(rows, rows + 3), slice(0, 3), slice(rows, rows + 2), slice(0, 2),
                     (rows + 1, 1), (rows, 0), 0, right)
    to_left = sides(slice(3, 6), slice(rows + 3, rows + 6), slice(2, 4), slice(rows + 2, rows + 4),
                    (2, rows + 2), (3, rows + 3), 1, left)

    settled(prev.at[own, slice(0, 5)], load_sem.at[1])
    rates_copy.wait()

    @pl.when(has_right)
    def _():
        for copy in to_right[:4]:
            copy.start()

    @pl.when(has_left)
    def _():
        for copy in to_left[:4]:
            copy.start()

    settled(prev.at[own, slice(2, layers - 2)], load_sem.at[2])

    @pl.when(has_right)
    def _():
        for copy in to_right[4:]:
            copy.start()

    @pl.when(has_left)
    def _():
        for copy in to_left[4:]:
            copy.start()

    lane, sub = iotas(width)
    masks = (lane == 0, sub == 0, lane == 127, sub == SUB - 1)

    def neighbours(v):
        return before(v, masks) + after(v, masks)

    def sweep_once(i, carry):
        here = prev[i + 1, 0]
        earlier = None
        for z in range(layers):
            later = prev[i + 1, z + 1] if z < layers - 1 else None
            total = CENTRE * here + (prev[i, z] + prev[i + 2, z]) + neighbours(here)
            if earlier is not None:
                total = total + earlier
            if later is not None:
                total = total + later
            once[i, z] = total
            earlier, here = here, later
        return carry

    lax.fori_loop(2, rows, sweep_once, 0)

    rate = [rates[k] for k in range(16)]

    def lookup(index):
        level = rate
        for bit in range(4):
            odd = (index & (1 << bit)) != 0
            level = [jnp.where(odd, level[2 * k + 1], level[2 * k]) for k in range(len(level) // 2)]
        return level[0]

    def advect(i, store):
        low, middle, high = surf[i], surf[i + 1], surf[i + 2]
        west, east = before(middle, masks), after(middle, masks)
        grad_rows = (high - low) * 0.5
        grad_cols = (east - west) * 0.5
        laplace = high + low + east + west - 4.0 * middle
        tendency = -vel[0, i] * grad_rows - vel[1, i] * grad_cols + lookup(bmap[i]) * laplace
        new = middle + TIME_STEP * flags[i].astype(jnp.float32) * tendency
        if store:
            new_surface[i - 2] = new
        shift[i] = new - middle

    def widen(src, dst, i):
        here = src[i + 1]
        dst[i] = (CENTRE + 2.0) * here + (src[i] + src[i + 2]) + neighbours(here)

    all_layers = layers * n_depth
    profile = [
        (all_layers - (depth * layers + z)).astype(jnp.float32) / all_layers * SCALE for z in range(layers)
    ]
    zero = jnp.float32(0.0)
    top = jnp.where(has_up, zero, jnp.float32(SCALE))
    upper = jnp.where(has_up, jnp.float32(SCALE), zero)
    lower = jnp.where(has_down, jnp.float32(SCALE), zero)

    def narrow(v):
        return sum(v[:, k * 128:(k + 1) * 128] for k in range(width // 128))

    def sweep_twice(i, carry):
        here = once[i + 1, 0]
        earlier = None
        part = widest[i]
        acc = None
        for z in range(layers):
            later = once[i + 1, z + 1] if z < layers - 1 else None
            total = CENTRE * here + (once[i, z] + once[i + 2, z]) + neighbours(here)
            if earlier is not None:
                total = total + earlier
            if later is not None:
                total = total + later
            total = SCALE * total + profile[z] * part
            if z == 0:
                total = total + upper * prev[i + 2, 0] + top * (
                    (1.0 / SHARE + 2.0 / all_layers) * shift[i + 2]
                    - (1.0 + 2.0 / all_layers) * wide[i + 1])
            elif z == 1:
                total = total - (top * (1.0 / all_layers)) * shift[i + 2]
            elif z == layers - 1:
                total = total + lower * prev[i + 2, layers - 1]
            elif z < layers - 2:
                acc = total * total if acc is None else acc + total * total
            mesh_out[i, z] = total
            earlier, here = here, later
        squares[i] = narrow(acc)
        return carry

    def arrived(c):
        size = sum(last - first for first, last, sem in pieces if sem == c)

        @pl.when(has_up)
        def _():
            settled(above.at[slice(0, size)], down_recv.at[c])

        @pl.when(has_down)
        def _():
            settled(below.at[slice(0, size)], up_recv.at[c])

    arrived(0)

    for have, target in ((has_up, up), (has_down, down)):
        @pl.when(have)
        def _():
            pl.semaphore_signal(relay_sem, inc=1, device_id=target, device_id_type=MESH)

    corners = []
    for number, (ref, near, depth_from) in enumerate(((above, 1, has_up), (below, 0, has_down))):
        for side, (src, dst, goes, comes, target) in enumerate((
            (rows, 0, has_right, has_left, right),
            (1, rows + 1, has_left, has_right, left),
        )):
            copy = remote(
                ref.at[src, near], ref.at[dst, near],
                corner_send.at[2 * number + side], corner_recv.at[2 * number + side], target)
            goes, comes = jnp.logical_and(goes, depth_from), jnp.logical_and(comes, depth_from)
            corners.append((copy, goes, comes))

            @pl.when(goes)
            def _():
                copy.start()

    def grouped(first, last, size, what):
        def some(g, carry):
            for k in range(size):
                what(first + g * size + k)
            return carry

        count = (last - first) // size
        if count:
            lax.fori_loop(0, count, some, 0)
        for i in range(first + count * size, last):
            what(i)

    grouped(3, rows + 1, 5, lambda i: advect(i, True))
    grouped(3, rows - 1, 5, lambda i: widen(shift, wide, i))
    grouped(3, rows - 3, 5, lambda i: widen(wide, widest, i))
    lax.fori_loop(3, rows - 3, sweep_twice, 0)

    @pl.when(has_left)
    def _():
        settled(edge_bytes, side_recv.at[0, 0])

    @pl.when(has_right)
    def _():
        settled(edge_bytes, side_recv.at[1, 0])

    for i in (0, 1, rows + 2, rows + 3):
        advect(i, False)
    for i in (2, rows + 1):
        advect(i, True)
    for i in (0, 1, 2, rows - 1, rows, rows + 1):
        widen(shift, wide, i)

    @pl.when(jnp.logical_not(has_left))
    def _():
        clear(wide.at[0])

    @pl.when(jnp.logical_not(has_right))
    def _():
        clear(wide.at[rows + 1])

    for i in (0, 1, 2, rows - 3, rows - 2, rows - 1):
        widen(wide, widest, i)

    even = jnp.logical_not(odd)
    far_side = jnp.logical_or(jnp.logical_and(odd, has_right), jnp.logical_and(even, has_left))

    def side_rows(at_left, kind):
        first = lax.select(at_left, 0, rows - 1)
        inward = lax.select(at_left, 1, -1)

        def wait():
            @pl.when(at_left)
            def _():
                to_right[kind].wait_recv()

            @pl.when(jnp.logical_not(at_left))
            def _():
                to_left[kind].wait_recv()

        return first, inward, wait

    def near_rows(at_left, have):
        first, inward, wait = side_rows(at_left, 4)
        pl.when(have)(wait)
        sweep_once(first + 1, 0)

        def body(k, carry):
            return sweep_twice(first + k * inward, 0)

        lax.fori_loop(1, 3, body, 0)

    def edge_row(at_left, have):
        first, inward, wait = side_rows(at_left, 5)

        @pl.when(have)
        def _():
            wait()
            sweep_once(first + 1 - inward, 0)

        sweep_twice(first, 0)

    near_rows(odd, True)
    edge_row(odd, True)
    send_layers(held, slice(3, None))
    near_rows(even, far_side)

    def finish(first, last):
        parts, values = {}, []
        for i in range(first, last):
            acc = None
            for ref, near, far, outer, inner in ((above, 1, 0, 0, 1), (below, 0, 1, layers - 1, layers - 2)):
                here = ref[i + 1, near]
                around = ref[i, near] + ref[i + 2, near] + neighbours(here)
                edge = mesh_out[i, outer] + SCALE * (2.0 * CENTRE * here + 2.0 * around + ref[i + 1, far])
                next_in = mesh_out[i, inner] + SCALE * here
                values += [(i, outer, edge), (i, inner, next_in)]
                both = edge * edge + next_in * next_in
                acc = both if acc is None else acc + both
            parts[i] = squares[i] + narrow(acc)
        for i, z, value in values:
            mesh_out[i, z] = value
        for i, value in parts.items():
            squares[i] = value

    def middle():
        arrived(2)
        finish(FIRST - 1, rows - 5)

    arrived(1)
    for first in range(1, FIRST - 1, 4):
        finish(first, min(first + 4, FIRST - 1))
    pl.when(even)(middle)
    edge_row(even, far_side)

    for copy, goes, comes in corners:
        @pl.when(comes)
        def _():
            copy.wait_recv()

    finish(0, 1)
    pl.when(odd)(middle)
    arrived(3)
    finish(rows - 5, rows - 3)
    arrived(4)
    finish(rows - 3, rows)

    pl.semaphore_wait(relay_sem, has_up.astype(jnp.int32) + has_down.astype(jnp.int32))
    totals[depth] = jnp.sum(squares[...], axis=1)
    for k in sorted(range(1, n_depth), key=lambda k: abs(2 * k - n_depth)):
        target = lax.rem(depth + k, n_depth)
        copy = remote(totals.at[depth], totals.at[depth], sum_sem.at[0], sum_sem.at[1], {"depth": target})
        copy.start()
    everyone_else = totals.at[slice(0, n_depth - 1)]
    settled(everyone_else, sum_sem.at[1])

    for have, sem in ((has_down, z_send.at[0]), (has_up, z_send.at[1])):
        @pl.when(have)
        def _():
            settled(prev.at[own, slice(0, 2)], sem)

    for have, row in ((has_right, 0), (has_left, 1)):
        @pl.when(have)
        def _():
            settled(edge_bytes, side_send.at[row, 0])
            settled(prev.at[slice(0, 2)], side_send.at[row, 1])

    for copy, goes, comes in corners:
        @pl.when(goes)
        def _():
            copy.wait_send()

    settled(everyone_else, sum_sem.at[0])


def store_kernel(rows, width, mesh_in, surface_in, totals, mesh_out, surface_out, norm_out, norm, sem):
    copies = []
    for s in range(SUB):
        cols = slice(s * width, (s + 1) * width)
        copies.append(pltpu.make_async_copy(mesh_in.at[:, :, s, :], mesh_out.at[:, :, cols], sem.at[0]))
        copies.append(pltpu.make_async_copy(surface_in.at[:, s, :], surface_out.at[:, cols], sem.at[1]))
    for copy in copies:
        copy.start()
    total = totals[0]
    for k in range(1, totals.shape[0]):
        total = total + totals[k]
    nodes = mesh_in.shape[1] * totals.shape[0] * SUB * width
    root = jnp.sqrt(jnp.sum(total, axis=1, keepdims=True) / nodes)
    spot = lax.broadcasted_iota(jnp.int32, (rows, 128), 0) == lax.broadcasted_iota(jnp.int32, (rows, 128), 1)
    norm[...] = jnp.sum(jnp.where(spot, root, 0.0), axis=0)[:rows]
    last = pltpu.make_async_copy(norm, norm_out, sem.at[2])
    last.start()
    last.wait()
    for ref, k in ((mesh_in, 0), (surface_in, 1)):
        pltpu.make_async_copy(ref, ref, sem.at[k]).wait()


def solution(mesh):
    n_lat, n_depth = mesh.shape["lat"], mesh.shape["depth"]

    def per_device(surface, velocity, block_map, free_flags, block_rates, previous):
        rows, layers, columns = previous.shape
        width = columns // SUB
        f32 = jnp.float32

        def vmem(*shape, dtype=f32):
            return pltpu.VMEM(shape, dtype)

        def kernel(*refs):
            relax_kernel(rows, layers, width, n_lat, n_depth, *refs)

        hbm = pl.BlockSpec(memory_space=pl.ANY)
        inside = pl.BlockSpec(memory_space=pltpu.VMEM)
        dma = pltpu.SemaphoreType.DMA
        new_surface, field, norm = pl.pallas_call(
            kernel,
            out_shape=(
                jax.ShapeDtypeStruct((rows, SUB, width), f32),
                jax.ShapeDtypeStruct((rows, layers, SUB, width), f32),
                jax.ShapeDtypeStruct((n_depth, rows, 128), f32),
            ),
            in_specs=[hbm] * 6,
            out_specs=(inside, inside, inside),
            scratch_shapes=[
                vmem(rows + 4, layers, SUB, width),
                vmem(rows + 2, layers, SUB, width),
                vmem(rows + 2, 2, SUB, width),
                vmem(rows + 2, 2, SUB, width),
                vmem(rows + 6, SUB, width),
                vmem(2, rows + 4, SUB, width),
                vmem(rows + 4, SUB, width, dtype=jnp.int32),
                vmem(rows + 4, SUB, width, dtype=jnp.int32),
                pltpu.SMEM((16,), f32),
                vmem(rows + 4, SUB, width),
                vmem(rows + 2, SUB, width),
                vmem(rows, SUB, width),
                vmem(rows, SUB, 128),
                dma((4,)),
                dma((2,)), dma((5,)), dma((5,)),
                dma((2, 2)), dma((2, 3)),
                dma((4,)), dma((4,)),
                dma((2,)),
                pltpu.SemaphoreType.REGULAR,
            ],
            compiler_params=pltpu.CompilerParams(
                collective_id=0, has_side_effects=True, vmem_limit_bytes=VMEM_LIMIT
            ),
            name="relax",
        )(*(
            pltpu.with_memory_space_constraint(value, pltpu.HBM)
            for value in (surface, velocity, block_map, free_flags, block_rates, previous)
        ))

        def store(*refs):
            store_kernel(rows, width, *refs)

        field, new_surface, norm = pl.pallas_call(
            store,
            out_shape=(
                jax.ShapeDtypeStruct(previous.shape, f32),
                jax.ShapeDtypeStruct(surface.shape, f32),
                jax.ShapeDtypeStruct((rows,), f32),
            ),
            in_specs=[inside, inside, inside],
            out_specs=(hbm, hbm, hbm),
            scratch_shapes=[vmem(rows), dma((3,))],
            compiler_params=pltpu.CompilerParams(vmem_limit_bytes=1024 * 1024),
            name="store",
        )(field, new_surface, norm)
        return new_surface, field, norm

    return jax.shard_map(
        per_device,
        mesh=mesh,
        in_specs=(
            P("lat", None), P(None, "lat", None), P("lat", None), P("lat", None), P(),
            P("lat", "depth", None),
        ),
        out_specs=(P("lat", None), P("lat", "depth", None), P("lat")),
        check_vma=False,
    )


VMEM_LIMIT = 40 * 1024 * 1024
```

```python
import jax
import jax.numpy as jnp
from jax import lax
from jax.experimental import pallas as pl
from jax.experimental.pallas import tpu as pltpu
from jax.sharding import PartitionSpec as P

MESH = pl.DeviceIdType.MESH
TIME_STEP = 0.5
RELAX_WEIGHT = 0.8
KEEP = 1.0 - RELAX_WEIGHT
SHARE = RELAX_WEIGHT / 6.0
CENTRE = KEEP / SHARE
SCALE = SHARE * SHARE
SUB = 8
FIRST = 10


def iotas(width):
    lane = lax.broadcasted_iota(jnp.int32, (SUB, 128), 1)
    sub = lax.broadcasted_iota(jnp.int32, (SUB, 128), 0)
    return lane, sub


def before(v, masks):
    width = v.shape[-1]
    rolled = pltpu.roll(v, 1, 1)
    first = rolled[:, :128]
    carried = pltpu.roll(first, 1, 0)
    first = jnp.where(masks[0], jnp.where(masks[1], 0.0, carried), first)
    return jnp.concatenate([first, rolled[:, 128:]], axis=1)


def after(v, masks):
    width = v.shape[-1]
    rolled = pltpu.roll(v, width - 1, 1)
    last = rolled[:, width - 128:]
    carried = pltpu.roll(last, SUB - 1, 0)
    last = jnp.where(masks[2], jnp.where(masks[3], 0.0, carried), last)
    return jnp.concatenate([rolled[:, : width - 128], last], axis=1)


def relax_kernel(
    rows, layers, width, n_lat, n_depth,
    surface, velocity, block_map, free_flags, block_rates, previous,
    new_surface, mesh_out, totals,
    prev, once, above, below, surf, vel, bmap, flags, rates,
    shift, wide, widest, squares,
    load_sem, z_send, up_recv, down_recv, side_send, side_recv,
    corner_send, corner_recv, sum_sem, relay_sem,
):
    lat = lax.axis_index("lat")
    depth = lax.axis_index("depth")
    has_left, has_right = lat > 0, lat < n_lat - 1
    has_up, has_down = depth > 0, depth < n_depth - 1
    left, right = {"lat": lat - 1}, {"lat": lat + 1}
    up, down = {"depth": depth - 1}, {"depth": depth + 1}

    barrier = pltpu.get_barrier_semaphore()
    around = ((has_up, up), (has_down, down), (has_left, left), (has_right, right))
    for have, target in around:
        @pl.when(have)
        def _():
            pl.semaphore_signal(barrier, inc=1, device_id=target, device_id_type=MESH)

    def settled(ref, sem):
        pltpu.make_async_copy(ref, ref, sem).wait()

    def load(sem, pairs):
        for src, dst in pairs:
            pltpu.make_async_copy(src, dst, sem).start()

    pieces = [
        (0, 1, 0), (rows - 1, rows, 0), (1, FIRST, 1), (FIRST, rows - 4, 2),
        (rows - 4, rows - 2, 3), (rows - 2, rows - 1, 4),
    ]

    cols = [slice(s * width, (s + 1) * width) for s in range(SUB)]
    own = slice(2, 2 + rows)
    load(load_sem.at[0], [
        (previous.at[:, part, cols[s]], prev.at[own, part, s, :])
        for part in (slice(layers - 2, layers), slice(0, 2)) for s in range(SUB)
    ])
    load(load_sem.at[1],
         [(surface.at[:, cols[s]], surf.at[slice(3, 3 + rows), s, :]) for s in range(SUB)]
         + [(velocity.at[:, :, cols[s]], vel.at[:, own, s, :]) for s in range(SUB)]
         + [(block_map.at[:, cols[s]], bmap.at[own, s, :]) for s in range(SUB)]
         + [(free_flags.at[:, cols[s]], flags.at[own, s, :]) for s in range(SUB)])
    load(load_sem.at[2], [
        (previous.at[:, part, cols[s]], prev.at[own, part, s, :])
        for part in (slice(2, SUB), slice(layers - SUB, layers - 2)) for s in range(SUB)
    ])
    rates_copy = pltpu.make_async_copy(block_rates, rates, load_sem.at[3])
    rates_copy.start()

    def clear(ref):
        ref[...] = jnp.zeros(ref.shape, ref.dtype)

    @pl.when(jnp.logical_not(has_up))
    def _():
        clear(above)

    @pl.when(jnp.logical_not(has_down))
    def _():
        clear(below)

    for have, near, far, at in (
        (has_left, slice(0, 2), slice(0, 3), 0),
        (has_right, slice(rows + 2, rows + 4), slice(rows + 3, rows + 6), rows + 1),
    ):
        @pl.when(jnp.logical_not(have))
        def _():
            clear(prev.at[near])
            clear(surf.at[far])
            clear(vel.at[:, near])
            clear(bmap.at[near])
            clear(flags.at[near])
            clear(above.at[at])
            clear(below.at[at])
            clear(once.at[at])

    pl.semaphore_wait(barrier, sum(have.astype(jnp.int32) for have, _ in around))

    def remote(src, dst, send, recv, target):
        return pltpu.make_async_remote_copy(
            src_ref=src, dst_ref=dst, send_sem=send, recv_sem=recv,
            device_id=target, device_id_type=MESH,
        )

    last_two, first_two = slice(layers - 2, layers), slice(0, 2)
    to_down, to_up = [], []
    for first, last, c in pieces:
        mine, theirs = slice(2 + first, 2 + last), slice(1 + first, 1 + last)
        to_down.append(remote(prev.at[mine, last_two], above.at[theirs], z_send.at[0], down_recv.at[c], down))
        to_up.append(remote(prev.at[mine, first_two], below.at[theirs], z_send.at[1], up_recv.at[c], up))

    settled(prev.at[own, slice(0, 4)], load_sem.at[0])

    def send_layers(turn, part):
        @pl.when(jnp.logical_and(has_down, turn))
        def _():
            for copy in to_down[part]:
                copy.start()

        @pl.when(jnp.logical_and(has_up, turn))
        def _():
            for copy in to_up[part]:
                copy.start()

    odd = lax.rem(lat, 2) == 1
    half = n_lat // 2
    late = jnp.logical_or(lat == 1, lat == half - 1)
    held = jnp.logical_or(jnp.logical_and(odd, jnp.logical_not(late)), lat == 0)
    send_layers(True, slice(0, 3))
    send_layers(jnp.logical_not(held), slice(3, None))

    def sides(mine3, theirs3, mine2, theirs2, near, far, row, target):
        return [
            remote(surf.at[mine3], surf.at[theirs3], side_send.at[row, 0], side_recv.at[row, 0], target),
            remote(vel.at[:, mine2], vel.at[:, theirs2], side_send.at[row, 0], side_recv.at[row, 0], target),
            remote(bmap.at[mine2], bmap.at[theirs2], side_send.at[row, 0], side_recv.at[row, 0], target),
            remote(flags.at[mine2], flags.at[theirs2], side_send.at[row, 0], side_recv.at[row, 0], target),
            remote(prev.at[near[0]], prev.at[near[1]], side_send.at[row, 1], side_recv.at[row, 1], target),
            remote(prev.at[far[0]], prev.at[far[1]], side_send.at[row, 1], side_recv.at[row, 2], target),
        ]

    edge_bytes = surf.at[slice(0, 3 + 4 * 2)]

    to_right = sides(slice(rows, rows + 3), slice(0, 3), slice(rows, rows + 2), slice(0, 2),
                     (rows + 1, 1), (rows, 0), 0, right)
    to_left = sides(slice(3, 6), slice(rows + 3, rows + 6), slice(2, 4), slice(rows + 2, rows + 4),
                    (2, rows + 2), (3, rows + 3), 1, left)

    settled(prev.at[own, slice(0, 5)], load_sem.at[1])
    rates_copy.wait()

    @pl.when(has_right)
    def _():
        for copy in to_right[:4]:
            copy.start()

    @pl.when(has_left)
    def _():
        for copy in to_left[:4]:
            copy.start()

    settled(prev.at[own, slice(2, layers - 2)], load_sem.at[2])

    @pl.when(has_right)
    def _():
        for copy in to_right[4:]:
            copy.start()

    @pl.when(has_left)
    def _():
        for copy in to_left[4:]:
            copy.start()

    lane, sub = iotas(width)
    masks = (lane == 0, sub == 0, lane == 127, sub == SUB - 1)

    def neighbours(v):
        return before(v, masks) + after(v, masks)

    def sweep_once(i, carry):
        here = prev[i + 1, 0]
        earlier = None
        for z in range(layers):
            later = prev[i + 1, z + 1] if z < layers - 1 else None
            total = CENTRE * here + (prev[i, z] + prev[i + 2, z]) + neighbours(here)
            if earlier is not None:
                total = total + earlier
            if later is not None:
                total = total + later
            once[i, z] = total
            earlier, here = here, later
        return carry

    lax.fori_loop(2, rows, sweep_once, 0)

    rate = [rates[k] for k in range(16)]

    def lookup(index):
        level = rate
        for bit in range(4):
            odd = (index & (1 << bit)) != 0
            level = [jnp.where(odd, level[2 * k + 1], level[2 * k]) for k in range(len(level) // 2)]
        return level[0]

    def advect(i, store):
        low, middle, high = surf[i], surf[i + 1], surf[i + 2]
        west, east = before(middle, masks), after(middle, masks)
        grad_rows = (high - low) * 0.5
        grad_cols = (east - west) * 0.5
        laplace = high + low + east + west - 4.0 * middle
        tendency = -vel[0, i] * grad_rows - vel[1, i] * grad_cols + lookup(bmap[i]) * laplace
        new = middle + TIME_STEP * flags[i].astype(jnp.float32) * tendency
        if store:
            new_surface[i - 2] = new
        shift[i] = new - middle

    def widen(src, dst, i):
        here = src[i + 1]
        dst[i] = (CENTRE + 2.0) * here + (src[i] + src[i + 2]) + neighbours(here)

    all_layers = layers * n_depth
    profile = [
        (all_layers - (depth * layers + z)).astype(jnp.float32) / all_layers * SCALE for z in range(layers)
    ]
    zero = jnp.float32(0.0)
    top = jnp.where(has_up, zero, jnp.float32(SCALE))
    upper = jnp.where(has_up, jnp.float32(SCALE), zero)
    lower = jnp.where(has_down, jnp.float32(SCALE), zero)

    def narrow(v):
        return sum(v[:, k * 128:(k + 1) * 128] for k in range(width // 128))

    def sweep_twice(i, carry):
        here = once[i + 1, 0]
        earlier = None
        part = widest[i]
        acc = None
        for z in range(layers):
            later = once[i + 1, z + 1] if z < layers - 1 else None
            total = CENTRE * here + (once[i, z] + once[i + 2, z]) + neighbours(here)
            if earlier is not None:
                total = total + earlier
            if later is not None:
                total = total + later
            total = SCALE * total + profile[z] * part
            if z == 0:
                total = total + upper * prev[i + 2, 0] + top * (
                    (1.0 / SHARE + 2.0 / all_layers) * shift[i + 2]
                    - (1.0 + 2.0 / all_layers) * wide[i + 1])
            elif z == 1:
                total = total - (top * (1.0 / all_layers)) * shift[i + 2]
            elif z == layers - 1:
                total = total + lower * prev[i + 2, layers - 1]
            elif z < layers - 2:
                acc = total * total if acc is None else acc + total * total
            mesh_out[i, z] = total
            earlier, here = here, later
        squares[i] = narrow(acc)
        return carry

    def arrived(c):
        size = sum(last - first for first, last, sem in pieces if sem == c)

        @pl.when(has_up)
        def _():
            settled(above.at[slice(0, size)], down_recv.at[c])

        @pl.when(has_down)
        def _():
            settled(below.at[slice(0, size)], up_recv.at[c])

    arrived(0)

    for have, target in ((has_up, up), (has_down, down)):
        @pl.when(have)
        def _():
            pl.semaphore_signal(relay_sem, inc=1, device_id=target, device_id_type=MESH)

    corners = []
    for number, (ref, near, depth_from) in enumerate(((above, 1, has_up), (below, 0, has_down))):
        for side, (src, dst, goes, comes, target) in enumerate((
            (rows, 0, has_right, has_left, right),
            (1, rows + 1, has_left, has_right, left),
        )):
            copy = remote(
                ref.at[src, near], ref.at[dst, near],
                corner_send.at[2 * number + side], corner_recv.at[2 * number + side], target)
            goes, comes = jnp.logical_and(goes, depth_from), jnp.logical_and(comes, depth_from)
            corners.append((copy, goes, comes))

            @pl.when(goes)
            def _():
                copy.start()

    def grouped(first, last, size, what):
        def some(g, carry):
            for k in range(size):
                what(first + g * size + k)
            return carry

        count = (last - first) // size
        if count:
            lax.fori_loop(0, count, some, 0)
        for i in range(first + count * size, last):
            what(i)

    grouped(3, rows + 1, 5, lambda i: advect(i, True))
    grouped(3, rows - 1, 5, lambda i: widen(shift, wide, i))
    grouped(3, rows - 3, 5, lambda i: widen(wide, widest, i))
    lax.fori_loop(3, rows - 3, sweep_twice, 0)

    @pl.when(has_left)
    def _():
        settled(edge_bytes, side_recv.at[0, 0])

    @pl.when(has_right)
    def _():
        settled(edge_bytes, side_recv.at[1, 0])

    for i in (0, 1, rows + 2, rows + 3):
        advect(i, False)
    for i in (2, rows + 1):
        advect(i, True)
    for i in (0, 1, 2, rows - 1, rows, rows + 1):
        widen(shift, wide, i)

    @pl.when(jnp.logical_not(has_left))
    def _():
        clear(wide.at[0])

    @pl.when(jnp.logical_not(has_right))
    def _():
        clear(wide.at[rows + 1])

    for i in (0, 1, 2, rows - 3, rows - 2, rows - 1):
        widen(wide, widest, i)

    even = jnp.logical_not(odd)
    far_side = jnp.logical_or(jnp.logical_and(odd, has_right), jnp.logical_and(even, has_left))

    def side_rows(at_left, kind):
        first = lax.select(at_left, 0, rows - 1)
        inward = lax.select(at_left, 1, -1)

        def wait():
            @pl.when(at_left)
            def _():
                to_right[kind].wait_recv()

            @pl.when(jnp.logical_not(at_left))
            def _():
                to_left[kind].wait_recv()

        return first, inward, wait

    def near_rows(at_left, have):
        first, inward, wait = side_rows(at_left, 4)
        pl.when(have)(wait)
        sweep_once(first + 1, 0)

        def body(k, carry):
            return sweep_twice(first + k * inward, 0)

        lax.fori_loop(1, 3, body, 0)

    def edge_row(at_left, have):
        first, inward, wait = side_rows(at_left, 5)

        @pl.when(have)
        def _():
            wait()
            sweep_once(first + 1 - inward, 0)

        sweep_twice(first, 0)

    near_rows(odd, True)
    edge_row(odd, True)
    turn = lax.rem(lat, 8) == 7
    send_layers(jnp.logical_and(held, turn), slice(3, None))
    near_rows(even, far_side)
    send_layers(jnp.logical_and(held, jnp.logical_not(turn)), slice(3, None))

    def finish(first, last):
        parts, values = {}, []
        for i in range(first, last):
            acc = None
            for ref, near, far, outer, inner in ((above, 1, 0, 0, 1), (below, 0, 1, layers - 1, layers - 2)):
                here = ref[i + 1, near]
                around = ref[i, near] + ref[i + 2, near] + neighbours(here)
                edge = mesh_out[i, outer] + SCALE * (2.0 * CENTRE * here + 2.0 * around + ref[i + 1, far])
                next_in = mesh_out[i, inner] + SCALE * here
                values += [(i, outer, edge), (i, inner, next_in)]
                both = edge * edge + next_in * next_in
                acc = both if acc is None else acc + both
            parts[i] = squares[i] + narrow(acc)
        for i, z, value in values:
            mesh_out[i, z] = value
        for i, value in parts.items():
            squares[i] = value

    def middle():
        arrived(2)
        finish(FIRST - 1, rows - 5)

    arrived(1)
    for first in range(1, FIRST - 1, 4):
        finish(first, min(first + 4, FIRST - 1))
    pl.when(even)(middle)
    edge_row(even, far_side)

    for copy, goes, comes in corners:
        @pl.when(comes)
        def _():
            copy.wait_recv()

    finish(0, 1)
    pl.when(odd)(middle)
    arrived(3)
    finish(rows - 5, rows - 3)
    arrived(4)
    finish(rows - 3, rows)

    pl.semaphore_wait(relay_sem, has_up.astype(jnp.int32) + has_down.astype(jnp.int32))
    totals[depth] = jnp.sum(squares[...], axis=1)
    for k in sorted(range(1, n_depth), key=lambda k: abs(2 * k - n_depth)):
        target = lax.rem(depth + k, n_depth)
        copy = remote(totals.at[depth], totals.at[depth], sum_sem.at[0], sum_sem.at[1], {"depth": target})
        copy.start()
    everyone_else = totals.at[slice(0, n_depth - 1)]
    settled(everyone_else, sum_sem.at[1])

    for have, sem in ((has_down, z_send.at[0]), (has_up, z_send.at[1])):
        @pl.when(have)
        def _():
            settled(prev.at[own, slice(0, 2)], sem)

    for have, row in ((has_right, 0), (has_left, 1)):
        @pl.when(have)
        def _():
            settled(edge_bytes, side_send.at[row, 0])
            settled(prev.at[slice(0, 2)], side_send.at[row, 1])

    for copy, goes, comes in corners:
        @pl.when(goes)
        def _():
            copy.wait_send()

    settled(everyone_else, sum_sem.at[0])


def store_kernel(rows, width, mesh_in, surface_in, totals, mesh_out, surface_out, norm_out, norm, sem):
    copies = []
    for s in range(SUB):
        cols = slice(s * width, (s + 1) * width)
        copies.append(pltpu.make_async_copy(mesh_in.at[:, :, s, :], mesh_out.at[:, :, cols], sem.at[0]))
        copies.append(pltpu.make_async_copy(surface_in.at[:, s, :], surface_out.at[:, cols], sem.at[1]))
    for copy in copies:
        copy.start()
    total = totals[0]
    for k in range(1, totals.shape[0]):
        total = total + totals[k]
    nodes = mesh_in.shape[1] * totals.shape[0] * SUB * width
    root = jnp.sqrt(jnp.sum(total, axis=1, keepdims=True) / nodes)
    spot = lax.broadcasted_iota(jnp.int32, (rows, 128), 0) == lax.broadcasted_iota(jnp.int32, (rows, 128), 1)
    norm[...] = jnp.sum(jnp.where(spot, root, 0.0), axis=0)[:rows]
    last = pltpu.make_async_copy(norm, norm_out, sem.at[2])
    last.start()
    last.wait()
    for ref, k in ((mesh_in, 0), (surface_in, 1)):
        pltpu.make_async_copy(ref, ref, sem.at[k]).wait()


def solution(mesh):
    n_lat, n_depth = mesh.shape["lat"], mesh.shape["depth"]

    def per_device(surface, velocity, block_map, free_flags, block_rates, previous):
        rows, layers, columns = previous.shape
        width = columns // SUB
        f32 = jnp.float32

        def vmem(*shape, dtype=f32):
            return pltpu.VMEM(shape, dtype)

        def kernel(*refs):
            relax_kernel(rows, layers, width, n_lat, n_depth, *refs)

        hbm = pl.BlockSpec(memory_space=pl.ANY)
        inside = pl.BlockSpec(memory_space=pltpu.VMEM)
        dma = pltpu.SemaphoreType.DMA
        new_surface, field, norm = pl.pallas_call(
            kernel,
            out_shape=(
                jax.ShapeDtypeStruct((rows, SUB, width), f32),
                jax.ShapeDtypeStruct((rows, layers, SUB, width), f32),
                jax.ShapeDtypeStruct((n_depth, rows, 128), f32),
            ),
            in_specs=[hbm] * 6,
            out_specs=(inside, inside, inside),
            scratch_shapes=[
                vmem(rows + 4, layers, SUB, width),
                vmem(rows + 2, layers, SUB, width),
                vmem(rows + 2, 2, SUB, width),
                vmem(rows + 2, 2, SUB, width),
                vmem(rows + 6, SUB, width),
                vmem(2, rows + 4, SUB, width),
                vmem(rows + 4, SUB, width, dtype=jnp.int32),
                vmem(rows + 4, SUB, width, dtype=jnp.int32),
                pltpu.SMEM((16,), f32),
                vmem(rows + 4, SUB, width),
                vmem(rows + 2, SUB, width),
                vmem(rows, SUB, width),
                vmem(rows, SUB, 128),
                dma((4,)),
                dma((2,)), dma((5,)), dma((5,)),
                dma((2, 2)), dma((2, 3)),
                dma((4,)), dma((4,)),
                dma((2,)),
                pltpu.SemaphoreType.REGULAR,
            ],
            compiler_params=pltpu.CompilerParams(
                collective_id=0, has_side_effects=True, vmem_limit_bytes=VMEM_LIMIT
            ),
            name="relax",
        )(*(
            pltpu.with_memory_space_constraint(value, pltpu.HBM)
            for value in (surface, velocity, block_map, free_flags, block_rates, previous)
        ))

        def store(*refs):
            store_kernel(rows, width, *refs)

        field, new_surface, norm = pl.pallas_call(
            store,
            out_shape=(
                jax.ShapeDtypeStruct(previous.shape, f32),
                jax.ShapeDtypeStruct(surface.shape, f32),
                jax.ShapeDtypeStruct((rows,), f32),
            ),
            in_specs=[inside, inside, inside],
            out_specs=(hbm, hbm, hbm),
            scratch_shapes=[vmem(rows), dma((3,))],
            compiler_params=pltpu.CompilerParams(vmem_limit_bytes=1024 * 1024),
            name="store",
        )(field, new_surface, norm)
        return new_surface, field, norm

    return jax.shard_map(
        per_device,
        mesh=mesh,
        in_specs=(
            P("lat", None), P(None, "lat", None), P("lat", None), P("lat", None), P(),
            P("lat", "depth", None),
        ),
        out_specs=(P("lat", None), P("lat", "depth", None), P("lat")),
        check_vma=False,
    )


VMEM_LIMIT = 40 * 1024 * 1024
```
